32 devices in a mesh: dp: 8 (over z, y), tp: 4 (over x, core).
Axes of the slice: x: 2, y: 2, z: 4, core: 2. Of those that a mesh axis runs over, the one named last changes fastest.
Arguments:
- hidden: bfloat16 [64, 256, 1024], P('dp')
- table: bfloat16 [50688, 1024], P('tp')
- labels: int32 [64, 256], P('dp')
- loss_mask: int32 [64, 256], P('dp')
- ln_gain: bfloat16 [1024], replicated
- ln_bias: bfloat16 [1024], replicated
Outputs:
- output 1: float32 [], replicated
- output 2: bfloat16 [64, 256, 1024], P('dp')
- output 3: float32 [50688, 1024], P('tp')
- output 4: float32 [1024], replicated
- output 5: float32 [1024], replicated
All inputs are finite; a program needn't handle non-finite values.
Results may differ from the reference program's by a relative error of at most 0.001.
Values sent between devices are 32-bit elements.
A program may use at most 1 GiB of HBM per device.

```python
import jax
import jax.numpy as jnp
from jax import lax

GROUP_BATCH = 8
DP_GROUPS = 8
SEQ_LEN = 256
MODEL_WIDTH = 1024
VOCAB_SIZE = 50257
VOCAB_PAD = 50688
BATCH_SIZE = DP_GROUPS * GROUP_BATCH
LN_EPS = 1e-5


def draw_targets(base_key):
    k_lab, k_grp, k_len, k_pre = jax.random.split(base_key, 4)
    labels = jax.random.randint(k_lab, (BATCH_SIZE, SEQ_LEN), 0, VOCAB_SIZE, dtype=jnp.int32)
    labels = labels.at[0, 0].set(0).at[0, 1].set(VOCAB_SIZE - 1)
    group_top = jax.random.randint(k_grp, (DP_GROUPS,), SEQ_LEN // 8, SEQ_LEN + 1, dtype=jnp.int32)
    seq_top = jnp.repeat(group_top, GROUP_BATCH)
    span_len = seq_top - seq_top // 2 + 1
    lengths = seq_top // 2 + jax.random.randint(k_len, (BATCH_SIZE,), 0, 1 << 20, dtype=jnp.int32) % span_len
    prefix = jax.random.randint(k_pre, (BATCH_SIZE,), 1, SEQ_LEN // 8 + 1, dtype=jnp.int32)
    lengths = jnp.maximum(lengths, prefix + 1)
    positions = jnp.arange(SEQ_LEN, dtype=jnp.int32)[None, :]
    loss_mask = ((positions >= prefix[:, None]) & (positions < lengths[:, None])).astype(jnp.int32)
    return labels, loss_mask


def setup_inputs(seed: int = 0) -> dict:
    base_key = jax.random.key(seed)
    k_hid, k_tab, k_gain, k_bias, k_tgt = jax.random.split(base_key, 5)
    hidden = jax.random.normal(k_hid, (BATCH_SIZE, SEQ_LEN, MODEL_WIDTH), jnp.float32)
    live_rows = (jnp.arange(VOCAB_PAD) < VOCAB_SIZE)[:, None]
    table = jax.random.normal(k_tab, (VOCAB_PAD, MODEL_WIDTH), jnp.float32) * (2.0 * MODEL_WIDTH ** -0.5)
    table = jnp.where(live_rows, table, 0.0)
    ln_gain = 1.0 + 0.3 * jax.random.normal(k_gain, (MODEL_WIDTH,), jnp.float32)
    ln_bias = 0.3 * jax.random.normal(k_bias, (MODEL_WIDTH,), jnp.float32)
    labels, loss_mask = draw_targets(k_tgt)
    return dict(hidden=hidden.astype(jnp.bfloat16), table=table.astype(jnp.bfloat16), labels=labels, loss_mask=loss_mask, ln_gain=ln_gain.astype(jnp.bfloat16), ln_bias=ln_bias.astype(jnp.bfloat16))


def reference(hidden, table, labels, loss_mask, ln_gain, ln_bias):
    count = jnp.sum(loss_mask).astype(jnp.float32)
    gain32 = ln_gain.astype(jnp.float32)
    bias32 = ln_bias.astype(jnp.float32)
    vocab_ids = jnp.arange(VOCAB_PAD)
    valid_cols = (vocab_ids < VOCAB_SIZE)[None, :]

    def one_seq(carry, inputs):
        grad_table, loss_sum = carry
        h_seq, lab_seq, mask_seq = inputs
        h32 = h_seq.astype(jnp.float32)
        mean = jnp.mean(h32, axis=-1, keepdims=True)
        centred = h32 - mean
        variance = jnp.mean(centred * centred, axis=-1, keepdims=True)
        inv_std = lax.rsqrt(variance + LN_EPS)
        x_hat = centred * inv_std
        x_norm = (x_hat * gain32 + bias32).astype(jnp.bfloat16)
        logits = jnp.dot(x_norm, table.T, preferred_element_type=jnp.float32)
        logits = jnp.where(valid_cols, logits, -jnp.inf)
        top = jnp.max(logits, axis=-1, keepdims=True)
        log_norm = top[:, 0] + jnp.log(jnp.sum(jnp.exp(logits - top), axis=-1))
        one_hot = vocab_ids[None, :] == lab_seq[:, None]
        target = jnp.sum(jnp.where(one_hot, logits, 0.0), axis=-1)
        weight = mask_seq.astype(jnp.float32)
        loss_sum = loss_sum + jnp.sum(weight * (log_norm - target))
        prob_vals = jnp.exp(logits - log_norm[:, None])
        grad_logits = ((prob_vals - one_hot.astype(jnp.float32)) * (weight / count)[:, None]).astype(jnp.bfloat16)
        grad_x = jnp.dot(grad_logits, table, preferred_element_type=jnp.float32)
        grad_table = grad_table + jnp.dot(grad_logits.T, x_norm, preferred_element_type=jnp.float32)
        grad_hat = grad_x * gain32
        mean_grad = jnp.mean(grad_hat, axis=-1, keepdims=True)
        mean_proj = jnp.mean(grad_hat * x_hat, axis=-1, keepdims=True)
        grad_h = (inv_std * (grad_hat - mean_grad - x_hat * mean_proj)).astype(jnp.bfloat16)
        return (grad_table, loss_sum), (grad_h, jnp.sum(grad_x * x_hat, axis=0), jnp.sum(grad_x, axis=0))

    init = (jnp.zeros((VOCAB_PAD, MODEL_WIDTH), jnp.float32), jnp.zeros((), jnp.float32))
    (grad_table, loss_sum), (grad_hidden, gain_parts, bias_parts) = lax.scan(one_seq, init, (hidden, labels, loss_mask))
    return loss_sum / count, grad_hidden, grad_table, jnp.sum(gain_parts, axis=0), jnp.sum(bias_parts, axis=0)
```

```python
import functools

import jax
import jax.numpy as jnp
from jax import lax
from jax.experimental import pallas as pl
from jax.experimental.pallas import tpu as pltpu
from jax.sharding import PartitionSpec as P

LN_EPS = 1e-5
VOCAB = 50257
Z = 4
Y = 2
CHUNKS = 33
MESH = pl.DeviceIdType.MESH


def chain_kernel(chunks, part, out, red, loc, red_send, red_recv, bc_send, bc_recv, y_send, y_recv, loc_sem, own_sem):
    rows = red.shape[2]
    half = part.shape[0]
    dp = lax.axis_index('dp')
    y = dp % Y
    z = dp // Y
    mate = dp + 1 - 2 * y
    place = (Z - 1 - z, z)
    onward = (dp - Y, dp + Y)
    back = (dp + Y, dp - Y)

    barrier = pltpu.get_barrier_semaphore()
    pl.semaphore_signal(barrier, inc=1, device_id={'dp': mate}, device_id_type=MESH)

    @pl.when(z > 0)
    def _():
        pl.semaphore_signal(barrier, inc=1, device_id={'dp': dp - Y}, device_id_type=MESH)

    @pl.when(z < Z - 1)
    def _():
        pl.semaphore_signal(barrier, inc=1, device_id={'dp': dp + Y}, device_id_type=MESH)

    inner = jnp.where((z > 0) & (z < Z - 1), 1, 0)
    pl.semaphore_wait(barrier, 2 + inner)

    def part_rows(x, c):
        return part.at[pl.ds(x * (half // 2) + c * rows, rows)]

    def out_rows(side, x, c):
        return out.at[pl.ds(side * half + x * (half // 2) + c * rows, rows)]

    def fetch(x, c):
        return pltpu.make_async_copy(part_rows(x, c), loc.at[x, c], loc_sem.at[x, c])

    def reduce_copy(x, c, src):
        return pltpu.make_async_remote_copy(
            src_ref=src, dst_ref=red.at[x, c], send_sem=red_send.at[x, c], recv_sem=red_recv.at[x, c],
            device_id={'dp': onward[x]}, device_id_type=MESH)

    def spread_copy(x, c, src):
        return pltpu.make_async_remote_copy(
            src_ref=src, dst_ref=out_rows(y, x, c), send_sem=bc_send.at[x], recv_sem=bc_recv.at[x, c],
            device_id={'dp': back[x]}, device_id_type=MESH)

    def mate_copy(x, c, src):
        return pltpu.make_async_remote_copy(
            src_ref=src, dst_ref=out_rows(y, x, c), send_sem=y_send.at[x], recv_sem=y_recv.at[x],
            device_id={'dp': mate}, device_id_type=MESH)

    def own_copy(x, c):
        return pltpu.make_async_copy(red.at[x, c], out_rows(y, x, c), own_sem.at[x])

    def begin(c, carry):
        for x in range(2):
            @pl.when(place[x] > 0)
            def _():
                fetch(x, c).start()
        return carry

    lax.fori_loop(0, chunks, begin, 0)

    def add(x, c):
        reduce_copy(x, c, red.at[x, c]).wait_recv()
        fetch(x, c).wait()
        red[x, c] = red[x, c] + loc[x, c]

    def step(s, carry):
        for x in range(2):
            p = place[x]
            c = s - p
            here = (c >= 0) & (c < chunks)

            @pl.when(here & (p == 0))
            def _():
                reduce_copy(x, c, part_rows(x, c)).start()

            @pl.when(here & (p > 0) & (p < Z - 1))
            def _():
                add(x, c)
                reduce_copy(x, c, red.at[x, c]).start()

            @pl.when(here & (p < Z - 1) & (c >= 2))
            def _():
                reduce_copy(x, c - 2, red.at[x, c - 2]).wait_send()

            @pl.when(here & (p == Z - 1))
            def _():
                add(x, c)
                spread_copy(x, c, red.at[x, c]).start()
                mate_copy(x, c, red.at[x, c]).start()
                own_copy(x, c).start()

        for x in range(2):
            p = place[x]
            c = s - 2 * (Z - 1) + p

            @pl.when((c >= 0) & (c < chunks) & (p < Z - 1))
            def _():
                spread_copy(x, c, out_rows(y, x, c)).wait_recv()

                @pl.when(p > 0)
                def _():
                    spread_copy(x, c, out_rows(y, x, c)).start()

                mate_copy(x, c, out_rows(y, x, c)).start()
        return carry

    lax.fori_loop(0, chunks + 2 * (Z - 1), step, 0)

    for x in range(2):
        p = place[x]
        mine = out.at[pl.ds(y * half + x * (half // 2), half // 2)]
        theirs = out.at[pl.ds((1 - y) * half + x * (half // 2), half // 2)]

        @pl.when(p < Z - 1)
        def _():
            reduce_copy(x, chunks - 2, red.at[x, chunks - 2]).wait_send()
            reduce_copy(x, chunks - 1, red.at[x, chunks - 1]).wait_send()

        @pl.when(p > 0)
        def _():
            pltpu.make_async_copy(mine, mine, bc_send.at[x]).wait()

        @pl.when(p == Z - 1)
        def _():
            pltpu.make_async_copy(mine, mine, own_sem.at[x]).wait()

        pltpu.make_async_copy(mine, mine, y_send.at[x]).wait()
        pltpu.make_async_copy(theirs, theirs, y_recv.at[x]).wait()


def chain_all_reduce(part, chunks=CHUNKS):
    half, width = part.shape
    rows = half // (2 * chunks)
    assert rows * 2 * chunks == half and rows % 8 == 0
    dma = pltpu.SemaphoreType.DMA
    return pl.pallas_call(
        functools.partial(chain_kernel, chunks),
        out_shape=jax.ShapeDtypeStruct((Y * half, width), jnp.float32),
        in_specs=[pl.BlockSpec(memory_space=pl.ANY)],
        out_specs=pl.BlockSpec(memory_space=pl.ANY),
        scratch_shapes=[
            pltpu.VMEM((2, chunks, rows, width), jnp.float32),
            pltpu.VMEM((2, chunks, rows, width), jnp.float32),
            dma((2, chunks)), dma((2, chunks)),
            dma((2,)), dma((2, chunks)),
            dma((2,)), dma((2,)),
            dma((2, chunks)), dma((2,)),
        ],
        compiler_params=pltpu.CompilerParams(
            collective_id=0, has_side_effects=True, vmem_limit_bytes=60 * 1024 * 1024),
        cost_estimate=pl.CostEstimate(flops=4 * half * width, bytes_accessed=12 * half * width, transcendentals=0),
    )(part)


def norm_stats(hidden):
    h32 = hidden.astype(jnp.float32)
    mean = jnp.mean(h32, axis=-1, keepdims=True)
    centred = h32 - mean
    variance = jnp.mean(centred * centred, axis=-1, keepdims=True)
    inv_std = lax.rsqrt(variance + LN_EPS)
    return centred * inv_std, inv_std


def norm_backward(grad_x, x_hat, inv_std, ln_gain):
    grad_hat = grad_x * ln_gain.astype(jnp.float32)
    mean_grad = jnp.mean(grad_hat, axis=-1, keepdims=True)
    mean_proj = jnp.mean(grad_hat * x_hat, axis=-1, keepdims=True)
    return (inv_std * (grad_hat - mean_grad - x_hat * mean_proj)).astype(jnp.bfloat16)


def solution(mesh):
    n_dp = mesh.shape['dp']
    n_tp = mesh.shape['tp']
    to_mate = [(i, i ^ 1) for i in range(n_dp)]
    to_core = [(i, i ^ 1) for i in range(n_tp)]

    def device_step(hidden, table, labels, loss_mask, ln_gain, ln_bias):
        batch, seq, width = hidden.shape
        tokens = batch * seq
        shard = table.shape[0]
        half = shard // Y
        dp = lax.axis_index('dp')
        tp = lax.axis_index('tp')
        y = dp % Y
        core = tp % 2
        gain = ln_gain.astype(jnp.float32)
        bias = ln_bias.astype(jnp.float32)

        x_hat, inv_std = norm_stats(hidden.reshape(tokens, width))
        ids = jnp.stack([labels.reshape(tokens), loss_mask.reshape(tokens)])
        ids_mate = lax.ppermute(ids, 'dp', to_mate)

        piece = lax.dynamic_slice(x_hat, (core * (tokens // 2), 0), (tokens // 2, width))
        got = lax.ppermute(piece, 'dp', to_mate)
        got2 = lax.ppermute(got, 'tp', to_core)
        first = jnp.where(core == 0, got, got2)
        second = jnp.where(core == 0, got2, got)
        hat_mate = jnp.concatenate([first, second])

        def pair(own, mate):
            return jnp.where(y == 0, jnp.stack([own, mate]), jnp.stack([mate, own]))

        hat_all = pair(x_hat, hat_mate).reshape(Y * tokens, width)
        x_all = (hat_all * gain + bias).astype(jnp.bfloat16)
        ids_all = pair(ids, ids_mate)
        labels_all = ids_all[:, 0].reshape(Y * tokens)
        mask_all = ids_all[:, 1].reshape(Y * tokens)

        rows = lax.dynamic_slice(table, (y * half, 0), (half, width))
        first_row = tp * shard + y * half
        logits = lax.dot_general(x_all, rows, (((1,), (1,)), ((), ())), preferred_element_type=jnp.float32)
        row_ids = first_row + lax.broadcasted_iota(jnp.int32, (1, half), 1)
        logits = jnp.where(row_ids < VOCAB, logits, -jnp.inf)
        one_hot = row_ids == labels_all[:, None]
        top = jnp.maximum(jnp.max(logits, axis=-1), jnp.finfo(jnp.float32).min)
        exp_sum = jnp.sum(jnp.exp(logits - top[:, None]), axis=-1)
        target = jnp.sum(jnp.where(one_hot, logits, 0.0), axis=-1)

        def merge(stats):
            best = jnp.max(stats[:, 0], axis=0)
            total = jnp.sum(stats[:, 1] * jnp.exp(stats[:, 0] - best), axis=0)
            return jnp.stack([best, total, jnp.sum(stats[:, 2], axis=0)])

        stats = merge(lax.all_gather(jnp.stack([top, exp_sum, target]), 'tp'))
        stats = merge(jnp.stack([stats, lax.ppermute(stats, 'dp', to_mate)]))
        log_norm = stats[0] + jnp.log(stats[1])

        weight = mask_all.astype(jnp.float32)
        own_weight = loss_mask.reshape(tokens).astype(jnp.float32)
        count = lax.psum(jnp.sum(own_weight), 'dp')
        scale = weight / count
        grad_logits = ((jnp.exp(logits - log_norm[:, None]) - one_hot.astype(jnp.float32)) * scale[:, None]).astype(jnp.bfloat16)
        part_table = lax.dot_general(grad_logits, x_all, (((0,), (0,)), ((), ())), preferred_element_type=jnp.float32)
        part_x = lax.dot_general(grad_logits, rows, (((1,), (0,)), ((), ())), preferred_element_type=jnp.float32)

        quarter = tokens // n_tp
        part_x = part_x.reshape(Y, n_tp, quarter, width)
        mixed = lax.psum_scatter(part_x, 'tp', scatter_dimension=1, tiled=False)
        mine = lax.dynamic_index_in_dim(mixed, y, 0, keepdims=False)
        other = lax.dynamic_index_in_dim(mixed, 1 - y, 0, keepdims=False)
        grad_quarter = mine + lax.ppermute(other, 'dp', to_mate)
        grad_x = lax.all_gather(grad_quarter, 'tp', tiled=True)

        grad_table = chain_all_reduce(part_table)

        grad_hidden = norm_backward(grad_x, x_hat, inv_std, ln_gain).reshape(batch, seq, width)
        own_norm = lax.dynamic_slice(log_norm - stats[2], (y * tokens,), (tokens,))
        sums = jnp.stack([jnp.sum(grad_x * x_hat, axis=0), jnp.sum(grad_x, axis=0)])
        lost = jnp.sum(own_weight * own_norm)
        sums, lost = lax.psum((sums, lost), 'dp')
        return lost / count, grad_hidden, grad_table, sums[0], sums[1]

    specs_in = (P('dp', None, None), P('tp', None), P('dp', None), P('dp', None), P(None), P(None))
    specs_out = (P(), P('dp', None, None), P('tp', None), P(None), P(None))
    return jax.shard_map(device_step, mesh=mesh, in_specs=specs_in, out_specs=specs_out, check_vma=False)
```

```python
import functools

import jax
import jax.numpy as jnp
from jax import lax
from jax.experimental import pallas as pl
from jax.experimental.pallas import tpu as pltpu
from jax.sharding import PartitionSpec as P

LN_EPS = 1e-5
VOCAB = 50257
Z = 4
Y = 2
CHUNKS = 33
SLOTS = 8
TILE = 512
MESH = pl.DeviceIdType.MESH


def unit_at(i):
    return 1 + i // 2 + (i // 2 + i % 2) // 2


def has_unit(i, units):
    return ((i % 2 == 1) | (i // 2 % 2 == 1)) & (unit_at(i) < units)


def last_tick(units):
    return max(i for i in range(1, 4 * units) if has_unit(i, units))


def backward_kernel(
        chunks, table, x, x_t, lse, scale, label,
        out, part, dx, target,
        red, loc, q_t, rows_buf, more_buf, stage, dx_t, from_core, from_x, dx_q,
        red_send, red_recv, credit, bc_send, bc_recv, y_send, y_recv, loc_sem, own_sem, part_sem, rows_sem, more_sem,
        core_sem, x_sem, share_send, share_recv):
    size = red.shape[2]
    half = part.shape[0]
    unit = 2 * size
    tokens = x.shape[0]
    own = tokens // Y
    width = x.shape[1]
    quarter = dx.shape[1]
    dp = lax.axis_index('dp')
    tp = lax.axis_index('tp')
    y = dp % Y
    z = dp // Y
    core = tp % 2
    mate = dp + 1 - 2 * y
    partner = tp + 1 - 2 * core
    beside = tp + 2 - 4 * (tp // 2)
    across = beside + 1 - 2 * core
    place = (Z - 1 - z, z)
    onward = (dp - Y, dp + Y)
    back = (dp + Y, dp - Y)

    barrier = pltpu.get_barrier_semaphore()
    pl.semaphore_signal(barrier, inc=1, device_id={'dp': mate}, device_id_type=MESH)
    for other in (partner, beside, across):
        pl.semaphore_signal(barrier, inc=1, device_id={'tp': other}, device_id_type=MESH)

    @pl.when(z > 0)
    def _():
        pl.semaphore_signal(barrier, inc=1, device_id={'dp': dp - Y}, device_id_type=MESH)

    @pl.when(z < Z - 1)
    def _():
        pl.semaphore_signal(barrier, inc=1, device_id={'dp': dp + Y}, device_id_type=MESH)

    inner = jnp.where((z > 0) & (z < Z - 1), 1, 0)

    def part_rows(h, c):
        return part.at[pl.ds(h * (half // 2) + c * size, size)]

    def out_rows(side, h, c):
        return out.at[pl.ds(side * half + h * (half // 2) + c * size, size)]

    def fetch(h, c):
        return pltpu.make_async_copy(part_rows(h, c), loc.at[h, c % 2], loc_sem.at[h, c % 2])

    def reduce_copy(h, c, src):
        slot = c % SLOTS
        return pltpu.make_async_remote_copy(
            src_ref=src, dst_ref=red.at[h, slot], send_sem=red_send.at[h, slot], recv_sem=red_recv.at[h, slot],
            device_id={'dp': onward[h]}, device_id_type=MESH)

    def spread_copy(h, c):
        return pltpu.make_async_remote_copy(
            src_ref=out_rows(y, h, c), dst_ref=out_rows(y, h, c), send_sem=bc_send.at[h], recv_sem=bc_recv.at[h, c],
            device_id={'dp': back[h]}, device_id_type=MESH)

    def mate_copy(h, c):
        return pltpu.make_async_remote_copy(
            src_ref=out_rows(y, h, c), dst_ref=out_rows(y, h, c), send_sem=y_send.at[h], recv_sem=y_recv.at[h],
            device_id={'dp': mate}, device_id_type=MESH)

    def own_copy(h, c):
        return pltpu.make_async_copy(red.at[h, c % SLOTS], out_rows(y, h, c), own_sem.at[h])

    def rows_copy(h, u):
        return pltpu.make_async_copy(
            table.at[pl.ds(y * half + h * (half // 2) + u * size, size)],
            rows_buf.at[u % 2, pl.ds(h * size, size)], rows_sem.at[u % 2, h])

    def more_copy(u):
        return pltpu.make_async_copy(
            table.at[pl.ds((1 - y) * half + u * unit, unit)], more_buf.at[u % 2], more_sem.at[u % 2])

    def part_copy(h, u):
        return pltpu.make_async_copy(stage.at[pl.ds(h * size, size)], part_rows(h, u), part_sem.at[h])

    shard_first = tp * Y * half
    steps_in_unit = lax.broadcasted_iota(jnp.int32, (unit, 1), 0)

    def grads(table_rows, row_ids, t):
        at = pl.ds(pl.multiple_of(t * TILE, TILE), TILE)
        logits = jnp.dot(table_rows, x_t[:, at], preferred_element_type=jnp.float32)
        hit = row_ids == label[:, at]
        probs = jnp.where(row_ids + shard_first < VOCAB, jnp.exp(logits - lse[:, at]), 0.0)
        q = ((probs - jnp.where(hit, 1.0, 0.0)) * scale[:, at]).astype(jnp.bfloat16)
        return q, jnp.where(hit, logits, 0.0)

    def add_dx(table_rows, q, t):
        dx_t[t] = dx_t[t] + lax.dot_general(
            table_rows, q, (((0,), (0,)), ((), ())), preferred_element_type=jnp.float32)

    def settle(u):
        for h in range(2):
            part_copy(h, u).wait()

    def compute(u):
        for h in range(2):
            rows_copy(h, u).wait()
        more_copy(u).wait()

        @pl.when(u + 1 < chunks)
        def _():
            for h in range(2):
                rows_copy(h, u + 1).start()
            more_copy(u + 1).start()

        slot = u % 2
        mine = y * half + u * size + steps_in_unit
        row_ids = jnp.where(steps_in_unit < size, mine, mine + (half // 2 - size))

        def main_tile(t, carry):
            q, hits = grads(rows_buf[slot], row_ids, t)
            at = pl.ds(pl.multiple_of(t * TILE, TILE), TILE)
            q_t[:, at] = q
            target[:, at] = target[:, at] + jnp.sum(hits, axis=0, keepdims=True)

            @pl.when(t < own // TILE)
            def _():
                add_dx(rows_buf[slot], q_t[:, at], t)
            return carry

        lax.fori_loop(0, tokens // TILE, main_tile, 0)

        def table_tile(n, carry):
            at = pl.ds(pl.multiple_of(n * 256, 256), 256)
            stage[:, at] = jnp.dot(q_t[...], x[:, at], preferred_element_type=jnp.float32)
            return carry

        lax.fori_loop(0, width // 256, table_tile, 0)
        for h in range(2):
            part_copy(h, u).start()

        theirs = (1 - y) * half + u * unit + steps_in_unit

        def more_tile(t, carry):
            q, _ = grads(more_buf[slot], theirs, t)
            add_dx(more_buf[slot], q, t)
            return carry

        lax.fori_loop(0, own // TILE, more_tile, 0)

    def send_reduced(h, c, src):
        @pl.when(c >= SLOTS)
        def _():
            pl.semaphore_wait(credit.at[h], 1)
        reduce_copy(h, c, src).start()

    def free_slot(h, c):
        @pl.when(c + SLOTS < chunks)
        def _():
            pl.semaphore_signal(credit.at[h], inc=1, device_id={'dp': back[h]}, device_id_type=MESH)

    def reduce_phase(s):
        for h in range(2):
            p = place[h]
            c = s - p
            here = (c >= 0) & (c < chunks)

            @pl.when(here & (p == 0))
            def _():
                @pl.when(c >= 2)
                def _():
                    reduce_copy(h, c - 2, part_rows(h, c - 2)).wait_send()
                send_reduced(h, c, part_rows(h, c))

            @pl.when(here & (p > 0))
            def _():
                slot = c % SLOTS
                reduce_copy(h, c, red.at[h, slot]).wait_recv()
                fetch(h, c).wait()
                red[h, slot] = red[h, slot] + loc[h, c % 2]

                @pl.when(p < Z - 1)
                def _():
                    @pl.when(c >= 2)
                    def _():
                        reduce_copy(h, c - 2, red.at[h, (c - 2) % SLOTS]).wait_send()
                        free_slot(h, c - 2)
                    send_reduced(h, c, red.at[h, slot])

                @pl.when(p == Z - 1)
                def _():
                    own_copy(h, c).start()

            @pl.when((p > 0) & (c >= -1) & (c + 1 < chunks))
            def _():
                fetch(h, c + 1).start()

    def spread_phase(s):
        for h in range(2):
            p = place[h]
            c = s - 2 * (Z - 1) + p

            @pl.when((c >= 0) & (c < chunks))
            def _():
                @pl.when(p == Z - 1)
                def _():
                    own_copy(h, c).wait()
                    free_slot(h, c)

                @pl.when(p < Z - 1)
                def _():
                    spread_copy(h, c).wait_recv()

                @pl.when(p > 0)
                def _():
                    spread_copy(h, c).start()

                mate_copy(h, c).start()

    def core_copy(i):
        return pltpu.make_async_remote_copy(
            src_ref=dx_t.at[2 * i + 1 - core], dst_ref=from_core.at[i], send_sem=core_sem.at[0, i],
            recv_sem=core_sem.at[1, i], device_id={'tp': partner}, device_id_type=MESH)

    def beside_copy():
        return pltpu.make_async_remote_copy(
            src_ref=dx_t.at[beside], dst_ref=from_x, send_sem=x_sem.at[0], recv_sem=x_sem.at[1],
            device_id={'tp': beside}, device_id_type=MESH)

    def share_copy(i, other):
        return pltpu.make_async_remote_copy(
            src_ref=dx_q, dst_ref=dx.at[tp], send_sem=share_send.at[i], recv_sem=share_recv.at[i],
            device_id={'tp': other}, device_id_type=MESH)

    def keep_copy():
        return pltpu.make_async_copy(dx_q, dx.at[tp], share_send.at[3])

    others = (partner, beside, across)
    block = 128

    def add_into(j, ref):
        def body(i, carry):
            at = pl.ds(pl.multiple_of(i * block, block), block)
            dx_t[j, at] = dx_t[j, at] + ref[at]
            return carry
        lax.fori_loop(0, width // block, body, 0)

    def dx_start():
        for i in range(2):
            core_copy(i).start()

    def dx_middle():
        for i in range(2):
            core_copy(i).wait_recv()
            add_into(2 * i + core, from_core.at[i])
        beside_copy().start()

    def dx_finish():
        beside_copy().wait_recv()
        add_into(tp, from_x)
        for i in range(width // block):
            at = pl.ds(i * block, block)
            dx_q[:, at] = dx_t[tp, at].T
        for i, other in enumerate(others):
            share_copy(i, other).start()
        keep_copy().start()

    def dx_end():
        for i in range(2):
            core_copy(i).wait_send()
        beside_copy().wait_send()
        for i, other in enumerate(others):
            share_copy(i, other).wait()
        keep_copy().wait()

    for h in range(2):
        rows_copy(h, 0).start()
    more_copy(0).start()
    target[...] = jnp.zeros_like(target)

    def clear(t, carry):
        dx_t[t] = jnp.zeros(dx_t.shape[1:], jnp.float32)
        return carry

    lax.fori_loop(0, own // TILE, clear, 0)
    pl.semaphore_wait(barrier, 5 + inner)

    done = last_tick(chunks)
    ticks = 1 + 2 * (chunks + 2 * (Z - 1))
    assert done + 9 < ticks

    def tick(i, carry):
        k = i // 2
        odd = i % 2 == 1
        earlier = jnp.maximum(i - 1, 1)

        @pl.when(i == 1)
        def _():
            settle(0)

        @pl.when(odd)
        def _():
            reduce_phase(k)

        @pl.when((i > 0) & (i % 2 == 0))
        def _():
            spread_phase(k - 1)

        @pl.when((i > 1) & has_unit(earlier, chunks))
        def _():
            settle(unit_at(earlier))

        @pl.when((i == 0) | has_unit(i, chunks))
        def _():
            compute(jnp.where(i == 0, 0, unit_at(i)))

        @pl.when(i == done + 1)
        def _():
            dx_start()

        @pl.when(i == done + 2)
        def _():
            dx_middle()

        @pl.when(i == done + 9)
        def _():
            dx_finish()
        return carry

    lax.fori_loop(0, ticks, tick, 0)

    for h in range(2):
        p = place[h]
        mine = out.at[pl.ds(y * half + h * (half // 2), half // 2)]
        theirs = out.at[pl.ds((1 - y) * half + h * (half // 2), half // 2)]

        @pl.when(p < Z - 1)
        def _():
            for c in (chunks - 2, chunks - 1):
                reduce_copy(h, c, red.at[h, c % SLOTS]).wait_send()

        @pl.when(p > 0)
        def _():
            pltpu.make_async_copy(mine, mine, bc_send.at[h]).wait()

        pltpu.make_async_copy(mine, mine, y_send.at[h]).wait()
        pltpu.make_async_copy(theirs, theirs, y_recv.at[h]).wait()
    dx_end()


def backward(table, x, x_t, lse, scale, label, n_tp, chunks):
    shard, width = table.shape
    half = shard // Y
    size = half // (2 * chunks)
    tokens = x.shape[0]
    quarter = tokens // Y // n_tp
    assert size * 2 * chunks == half and size % 16 == 0 and quarter == TILE
    f32 = jnp.float32
    dma = pltpu.SemaphoreType.DMA
    vmem = pl.BlockSpec(memory_space=pltpu.VMEM)
    hbm = pl.BlockSpec(memory_space=pl.ANY)
    flops = 2 * width * half * (2 * tokens + 3 * tokens // Y)
    return pl.pallas_call(
        functools.partial(backward_kernel, chunks),
        out_shape=(
            jax.ShapeDtypeStruct((shard, width), f32),
            jax.ShapeDtypeStruct((half, width), f32),
            jax.ShapeDtypeStruct((n_tp, quarter, width), f32),
            jax.ShapeDtypeStruct((1, tokens), f32)),
        in_specs=[hbm, vmem, vmem, vmem, vmem, vmem],
        out_specs=(hbm, hbm, hbm, vmem),
        scratch_shapes=[
            pltpu.VMEM((2, SLOTS, size, width), f32),
            pltpu.VMEM((2, 2, size, width), f32),
            pltpu.VMEM((2 * size, tokens), jnp.bfloat16),
            pltpu.VMEM((2, 2 * size, width), jnp.bfloat16),
            pltpu.VMEM((2, 2 * size, width), jnp.bfloat16),
            pltpu.VMEM((2 * size, width), f32),
            pltpu.VMEM((n_tp, width, quarter), f32),
            pltpu.VMEM((2, width, quarter), f32),
            pltpu.VMEM((width, quarter), f32),
            pltpu.VMEM((quarter, width), f32),
            dma((2, SLOTS)), dma((2, SLOTS)), pltpu.SemaphoreType.REGULAR((2,)),
            dma((2,)), dma((2, chunks)),
            dma((2,)), dma((2,)),
            dma((2, 2)), dma((2,)), dma((2,)), dma((2, 2)), dma((2,)),
            dma((2, 2)), dma((2,)), dma((4,)), dma((3,)),
        ],
        compiler_params=pltpu.CompilerParams(
            collective_id=0, has_side_effects=True, vmem_limit_bytes=62 * 1024 * 1024),
        cost_estimate=pl.CostEstimate(flops=flops, bytes_accessed=12 * half * width, transcendentals=half * tokens),
    )(table, x, x_t, lse, scale, label)


def norm_stats(hidden):
    h32 = hidden.astype(jnp.float32)
    mean = jnp.mean(h32, axis=-1, keepdims=True)
    centred = h32 - mean
    variance = jnp.mean(centred * centred, axis=-1, keepdims=True)
    inv_std = lax.rsqrt(variance + LN_EPS)
    return centred * inv_std, inv_std


def norm_backward(grad_x, x_hat, inv_std, ln_gain):
    grad_hat = grad_x * ln_gain.astype(jnp.float32)
    mean_grad = jnp.mean(grad_hat, axis=-1, keepdims=True)
    mean_proj = jnp.mean(grad_hat * x_hat, axis=-1, keepdims=True)
    return (inv_std * (grad_hat - mean_grad - x_hat * mean_proj)).astype(jnp.bfloat16)


def solution(mesh):
    n_dp = mesh.shape['dp']
    n_tp = mesh.shape['tp']
    to_mate = [(i, i ^ 1) for i in range(n_dp)]
    to_core = [(i, i ^ 1) for i in range(n_tp)]

    def device_step(hidden, table, labels, loss_mask, ln_gain, ln_bias):
        batch, seq, width = hidden.shape
        tokens = batch * seq
        shard = table.shape[0]
        tp = lax.axis_index('tp')
        core = tp % 2
        gain = ln_gain.astype(jnp.float32)
        bias = ln_bias.astype(jnp.float32)

        x_hat, inv_std = norm_stats(hidden.reshape(tokens, width))
        piece = lax.dynamic_slice(x_hat, (core * (tokens // 2), 0), (tokens // 2, width))
        got = lax.ppermute(piece, 'dp', to_mate)
        got2 = lax.ppermute(got, 'tp', to_core)
        ids = jnp.stack([labels.reshape(tokens), loss_mask.reshape(tokens)])
        ids_mate = lax.ppermute(ids, 'dp', to_mate)

        x = (x_hat * gain + bias).astype(jnp.bfloat16)
        logits = lax.dot_general(x, table, (((1,), (1,)), ((), ())), preferred_element_type=jnp.float32)
        row_ids = tp * shard + lax.broadcasted_iota(jnp.int32, (1, shard), 1)
        logits = jnp.where(row_ids < VOCAB, logits, -jnp.inf)
        top = jnp.maximum(jnp.max(logits, axis=-1), jnp.finfo(jnp.float32).min)
        exp_sum = jnp.sum(jnp.exp(logits - top[:, None]), axis=-1)
        stats = lax.all_gather(jnp.stack([top, exp_sum]), 'tp')
        best = jnp.max(stats[:, 0], axis=0)
        log_norm = best + jnp.log(jnp.sum(stats[:, 1] * jnp.exp(stats[:, 0] - best), axis=0))
        norm_mate = lax.ppermute(log_norm, 'dp', to_mate)

        mask = loss_mask.reshape(tokens).astype(jnp.float32)
        count = lax.psum(jnp.sum(mask), 'dp')

        first = jnp.where(core == 0, got, got2)
        second = jnp.where(core == 0, got2, got)
        x_mate = (jnp.concatenate([first, second]) * gain + bias).astype(jnp.bfloat16)
        x_all = jnp.concatenate([x, x_mate])
        lse = jnp.concatenate([log_norm, norm_mate])[None]
        label = jnp.concatenate([ids[0], ids_mate[0]])[None] - tp * shard
        weight = jnp.concatenate([mask, ids_mate[1].astype(jnp.float32)])[None]

        grad_table, _, grad_x, target = backward(table, x_all, x_all.T, lse, weight / count, label, n_tp, CHUNKS)

        grad_x = grad_x.reshape(tokens, width)
        grad_hidden = norm_backward(grad_x, x_hat, inv_std, ln_gain).reshape(batch, seq, width)
        sums = jnp.stack([jnp.sum(grad_x * x_hat, axis=0), jnp.sum(grad_x, axis=0)])
        lost = jnp.sum(mask * log_norm) / n_tp - jnp.sum(weight * target)
        sums, lost = lax.psum((sums / n_tp, lost), ('dp', 'tp'))
        return lost / count, grad_hidden, grad_table, sums[0], sums[1]

    specs_in = (P('dp', None, None), P('tp', None), P('dp', None), P('dp', None), P(None), P(None))
    specs_out = (P(), P('dp', None, None), P('tp', None), P(None), P(None))
    return jax.shard_map(device_step, mesh=mesh, in_specs=specs_in, out_specs=specs_out, check_vma=False)
```

```python
import functools

import jax
import jax.numpy as jnp
from jax import lax
from jax.experimental import pallas as pl
from jax.experimental.pallas import tpu as pltpu
from jax.sharding import PartitionSpec as P

LN_EPS = 1e-5
VOCAB = 50257
Z = 4
Y = 2
CHUNKS = 33
SLOTS = 8
TILE = 512
PIECES = 4
FORWARD_ROWS = 384
MESH = pl.DeviceIdType.MESH


def signal(barrier, **where):
    pl.semaphore_signal(barrier, inc=1, device_id=where, device_id_type=MESH)


def neighbours(tp):
    core = tp % 2
    partner = tp + 1 - 2 * core
    beside = tp + 2 - 4 * (tp // 2)
    return partner, beside, beside + 1 - 2 * core


def forward_kernel(
        n_dp, n_tp, table, hidden, gain, bias, mask,
        x_all, xt_all, lse, count, hat_q, inv_q,
        x_own, xt_own, send_q, got, x_mate, xt_mate, rows_buf, top, total, stats, counts, hat_buf,
        rows_sem, y_sem, beside_sem, core_sem, relay_sem, stat_send, stat_recv, count_send, count_recv, out_sem):
    own, width = hidden.shape
    shard = table.shape[0]
    size = rows_buf.shape[1]
    blocks = shard // size
    quarter = own // n_tp
    piece = quarter // PIECES
    dp = lax.axis_index('dp')
    tp = lax.axis_index('tp')
    mate = dp + 1 - 2 * (dp % Y)
    partner, beside, across = neighbours(tp)
    others = (partner, beside, across)
    dp_others = [lax.rem(dp + j, n_dp) for j in range(1, n_dp)]

    barrier = pltpu.get_barrier_semaphore()
    for other in dp_others:
        signal(barrier, dp=other)
    for other in others:
        signal(barrier, tp=other)
        signal(barrier, dp=mate, tp=other)

    def rows_copy(b):
        return pltpu.make_async_copy(table.at[pl.ds(b * size, size)], rows_buf.at[b % 2], rows_sem.at[b % 2])

    def remote(src, dst, sems, k, **where):
        return pltpu.make_async_remote_copy(
            src_ref=src, dst_ref=dst, send_sem=sems.at[0, k], recv_sem=sems.at[1, k],
            device_id=where, device_id_type=MESH)

    def got_piece(q, k):
        return got.at[q, pl.ds(k * piece, piece)]

    def y_copy(k):
        return remote(send_q.at[pl.ds(k * piece, piece)], got_piece(tp, k), y_sem, k, dp=mate)

    def beside_copy(k):
        return remote(got_piece(tp, k), got_piece(tp, k), beside_sem, k, tp=beside)

    def core_copy(k):
        return remote(got_piece(tp, k), got_piece(tp, k), core_sem, k, tp=partner)

    def relay_copy(k):
        return remote(got_piece(beside, k), got_piece(beside, k), relay_sem, k, tp=partner)

    def count_copy(j):
        return pltpu.make_async_remote_copy(
            src_ref=counts.at[dp], dst_ref=counts.at[dp], send_sem=count_send.at[j], recv_sem=count_recv.at[dp],
            device_id={'dp': dp_others[j]}, device_id_type=MESH)

    def count_arrival(j):
        other = dp_others[j]
        return pltpu.make_async_remote_copy(
            src_ref=counts.at[other], dst_ref=counts.at[other], send_sem=count_send.at[j], recv_sem=count_recv.at[other],
            device_id={'dp': other}, device_id_type=MESH)

    def normalize(at):
        h = hidden[at, :].astype(jnp.float32)
        mean = jnp.mean(h, axis=-1, keepdims=True)
        centred = h - mean
        variance = jnp.mean(centred * centred, axis=-1, keepdims=True)
        inv_std = lax.rsqrt(variance + LN_EPS)
        x_hat = centred * inv_std
        x = (x_hat * gain[...] + bias[...]).astype(jnp.bfloat16)
        wide = x.astype(jnp.float32)
        x_own[at, :] = x
        xt_own[:, at] = wide.T.astype(jnp.bfloat16)
        return x_hat, inv_std, wide

    def block_of(q, k):
        return pl.ds(pl.multiple_of(q * quarter + k * piece, piece), piece)

    def first_piece(k, carry):
        x_hat, inv_std, wide = normalize(block_of(tp, k))
        at = pl.ds(pl.multiple_of(k * piece, piece), piece)
        send_q[at, :] = wide
        hat_buf[at, :] = x_hat
        inv_q[at, :] = jnp.broadcast_to(inv_std, (piece, inv_q.shape[1]))

        @pl.when(k == 0)
        def _():
            pl.semaphore_wait(barrier, n_dp - 1 + 2 * len(others))
        y_copy(k).start()
        return carry

    rows_copy(0).start()
    lax.fori_loop(0, PIECES, first_piece, 0)

    def next_piece(j, carry):
        normalize(block_of(lax.rem(tp + 1 + j // PIECES, n_tp), j % PIECES))
        return carry

    lax.fori_loop(0, (n_tp - 1) * PIECES, next_piece, 0)
    own_outs = (
        pltpu.make_async_copy(x_own, x_all.at[pl.ds(0, own)], out_sem.at[0]),
        pltpu.make_async_copy(xt_own, xt_all.at[:, pl.ds(0, own)], out_sem.at[1]),
        pltpu.make_async_copy(hat_buf, hat_q, out_sem.at[2]))
    for copy in own_outs:
        copy.start()

    counts[dp] = jnp.full(counts.shape[1:], jnp.sum(mask[...]), jnp.float32)
    for j in range(n_dp - 1):
        count_copy(j).start()
    top[...] = jnp.full_like(top, jnp.finfo(jnp.float32).min)
    total[...] = jnp.zeros_like(total)

    def convert(q, k):
        wide = got[q, pl.ds(pl.multiple_of(k * piece, piece), piece)]
        at = block_of(q, k)
        x_mate[at, :] = wide.astype(jnp.bfloat16)
        xt_mate[:, at] = wide.T.astype(jnp.bfloat16)

    first_row = tp * shard

    def block(b, carry):
        rows_copy(b).wait()

        @pl.when(b + 1 < blocks)
        def _():
            rows_copy(b + 1).start()

        phase = b % 6

        @pl.when((phase == 0) & (b > 0) & (b <= 6 * PIECES))
        def _():
            k = jnp.maximum(b // 6 - 1, 0)
            y_copy(k).wait_recv()
            beside_copy(k).start()
            core_copy(k).start()
            convert(tp, k)

        @pl.when((phase == 2) & (b >= 14) & (b < 14 + 6 * PIECES))
        def _():
            k = jnp.maximum(b - 14, 0) // 6
            beside_copy(k).wait_recv()
            relay_copy(k).start()
            convert(beside, k)

        @pl.when((phase == 4) & (b >= 10) & (b < 10 + 6 * PIECES))
        def _():
            k = jnp.maximum(b - 10, 0) // 6
            core_copy(k).wait_recv()
            convert(partner, k)

        @pl.when((phase == 4) & (b >= 16) & (b < 10 + 6 * PIECES))
        def _():
            k = jnp.maximum(b - 16, 0) // 6
            relay_copy(k).wait_recv()
            convert(across, k)

        slot = b % 2
        row_ids = first_row + b * size + lax.broadcasted_iota(jnp.int32, (size, 1), 0)

        def tile(t, carry):
            at = pl.ds(pl.multiple_of(t * TILE, TILE), TILE)
            logits = jnp.dot(rows_buf[slot], xt_own[:, at], preferred_element_type=jnp.float32)
            logits = jnp.where(row_ids < VOCAB, logits, -jnp.inf).reshape(size // 8, 8, TILE)
            before = top[:, at]
            now = jnp.maximum(before, jnp.max(logits, axis=0))
            total[:, at] = total[:, at] * jnp.exp(before - now) + jnp.sum(jnp.exp(logits - now[None]), axis=0)
            top[:, at] = now
            return carry

        lax.fori_loop(0, own // TILE, tile, 0)
        return carry

    assert blocks > 8 + 6 * PIECES
    lax.fori_loop(0, blocks, block, 0)

    best = jnp.max(top[...], axis=0, keepdims=True)
    stats[0, tp, 0:1] = best
    stats[0, tp, 1:2] = jnp.sum(total[...] * jnp.exp(top[...] - best), axis=0, keepdims=True)

    def stat_copies():
        copies = []
        for i, other in enumerate(others):
            copies.append((0, i, {'tp': other}))
        copies.append((1, 3, {'dp': mate}))
        for i, other in enumerate(others):
            copies.append((1, 4 + i, {'dp': mate, 'tp': other}))
        return [pltpu.make_async_remote_copy(
            src_ref=stats.at[0, tp], dst_ref=stats.at[side, tp], send_sem=stat_send.at[i], recv_sem=stat_recv.at[side, tp],
            device_id=where, device_id_type=MESH) for side, i, where in copies]

    def stat_arrival(side, other):
        return pltpu.make_async_remote_copy(
            src_ref=stats.at[side, other], dst_ref=stats.at[side, other], send_sem=stat_send.at[0],
            recv_sem=stat_recv.at[side, other], device_id={'tp': other}, device_id_type=MESH)

    for copy in stat_copies():
        copy.start()
    last = PIECES - 1
    relay_copy(last).wait_recv()
    convert(across, last)
    mate_outs = (
        pltpu.make_async_copy(x_mate, x_all.at[pl.ds(own, own)], out_sem.at[3]),
        pltpu.make_async_copy(xt_mate, xt_all.at[:, pl.ds(own, own)], out_sem.at[4]))
    for copy in mate_outs:
        copy.start()
    for other in others:
        stat_arrival(0, other).wait_recv()
    for other in (tp,) + others:
        stat_arrival(1, other).wait_recv()
    for side in range(Y):
        tops = [stats[side, j, 0:1] for j in range(n_tp)]
        best = functools.reduce(jnp.maximum, tops)
        mass = sum(stats[side, j, 1:2] * jnp.exp(tops[j] - best) for j in range(n_tp))
        lse[:, side * own:(side + 1) * own] = best + jnp.log(mass)
    for j in range(n_dp - 1):
        count_arrival(j).wait_recv()
    count[...] = sum(counts[j] for j in range(n_dp))

    for k in range(PIECES):
        for copy in (y_copy(k), beside_copy(k), core_copy(k), relay_copy(k)):
            copy.wait_send()
    for copy in stat_copies():
        copy.wait_send()
    for j in range(n_dp - 1):
        count_copy(j).wait_send()
    for copy in own_outs + mate_outs:
        copy.wait()


def forward(table, hidden, gain, bias, mask, n_dp, n_tp):
    own, width = hidden.shape
    shard = table.shape[0]
    quarter = own // n_tp
    assert shard % FORWARD_ROWS == 0
    f32 = jnp.float32
    b16 = jnp.bfloat16
    dma = pltpu.SemaphoreType.DMA
    vmem = pl.BlockSpec(memory_space=pltpu.VMEM)
    hbm = pl.BlockSpec(memory_space=pl.ANY)
    lanes = 128
    return pl.pallas_call(
        functools.partial(forward_kernel, n_dp, n_tp),
        out_shape=(
            jax.ShapeDtypeStruct((Y * own, width), b16),
            jax.ShapeDtypeStruct((width, Y * own), b16),
            jax.ShapeDtypeStruct((1, Y * own), f32),
            jax.ShapeDtypeStruct((8, lanes), f32),
            jax.ShapeDtypeStruct((quarter, width), f32),
            jax.ShapeDtypeStruct((quarter, lanes), f32)),
        in_specs=[hbm, vmem, vmem, vmem, vmem],
        out_specs=(hbm, hbm, vmem, vmem, hbm, vmem),
        scratch_shapes=[
            pltpu.VMEM((own, width), b16), pltpu.VMEM((width, own), b16),
            pltpu.VMEM((quarter, width), f32), pltpu.VMEM((n_tp, quarter, width), f32),
            pltpu.VMEM((own, width), b16), pltpu.VMEM((width, own), b16),
            pltpu.VMEM((2, FORWARD_ROWS, width), b16),
            pltpu.VMEM((8, own), f32), pltpu.VMEM((8, own), f32),
            pltpu.VMEM((Y, n_tp, 2, own), f32), pltpu.VMEM((n_dp, 8, lanes), f32),
            pltpu.VMEM((quarter, width), f32),
            dma((2,)), dma((2, PIECES)), dma((2, PIECES)), dma((2, PIECES)), dma((2, PIECES)),
            dma((2 * n_tp - 1,)), dma((Y, n_tp)), dma((n_dp - 1,)), dma((n_dp,)), dma((5,)),
        ],
        compiler_params=pltpu.CompilerParams(
            collective_id=1, has_side_effects=True, vmem_limit_bytes=56 * 1024 * 1024),
        cost_estimate=pl.CostEstimate(
            flops=2 * own * shard * width, bytes_accessed=2 * shard * width, transcendentals=own * shard),
    )(table, hidden, gain, bias, mask)


EVERY = 4


def main_unit(i):
    k, odd = i // 2, i % 2
    return 1 + k + (k + EVERY - 2 + odd) // EVERY


def has_main(i, units):
    return ((i % 2 == 1) | (i // 2 % EVERY == 1)) & (main_unit(i) < units)


def last_main(units):
    return max(i for i in range(1, 4 * units) if has_main(i, units))


def more_unit(i, units):
    end = last_main(units)
    return jnp.where(i <= end, i // 2 - 1, jnp.maximum(i - end, 0) + end // 2 - 1)


def has_more(i, units):
    end = last_main(units)
    return (i > 0) & ((i > end) | (i % 2 == 0)) & (more_unit(i, units) < units)


def last_more(units):
    end = last_main(units)
    return end + units - end // 2


def backward_kernel(
        chunks, table, x, x_t, lse, weight, label, count, hat, inv, gain,
        out, part, dh, sums,
        red, loc, q_t, rows_buf, more_buf, stage, dx_t, from_core, from_x, dx_q, scale, target, levels, arrived,
        red_send, red_recv, credit, bc_send, bc_recv, y_send, y_recv, loc_sem, own_sem, part_sem, rows_sem, more_sem,
        core_sem, x_sem, share_send, share_recv, level_sem):
    size = red.shape[2]
    half = part.shape[0]
    unit = 2 * size
    tokens = x.shape[0]
    own = tokens // Y
    width = x.shape[1]
    quarter = dh.shape[1]
    n_tp = dh.shape[0]
    dp = lax.axis_index('dp')
    tp = lax.axis_index('tp')
    y = dp % Y
    z = dp // Y
    core = tp % 2
    mate = dp + 1 - 2 * y
    partner, beside, across = neighbours(tp)
    z_mate = dp + Y - 2 * Y * (z % 2)
    z_far = dp + 2 * Y - 4 * Y * (z // 2)
    place = (Z - 1 - z, z)
    onward = (dp - Y, dp + Y)
    back = (dp + Y, dp - Y)

    barrier = pltpu.get_barrier_semaphore()
    signal(barrier, dp=mate)
    signal(barrier, dp=z_far)
    for other in (partner, beside, across):
        signal(barrier, tp=other)

    @pl.when(z > 0)
    def _():
        signal(barrier, dp=dp - Y)

    @pl.when(z < Z - 1)
    def _():
        signal(barrier, dp=dp + Y)

    inner = jnp.where((z > 0) & (z < Z - 1), 1, 0)

    def part_rows(h, c):
        return part.at[pl.ds(h * (half // 2) + c * size, size)]

    def out_rows(side, h, c):
        return out.at[pl.ds(side * half + h * (half // 2) + c * size, size)]

    def fetch(h, c):
        return pltpu.make_async_copy(part_rows(h, c), loc.at[h, c % 2], loc_sem.at[h, c % 2])

    def reduce_copy(h, c, src):
        slot = c % SLOTS
        return pltpu.make_async_remote_copy(
            src_ref=src, dst_ref=red.at[h, slot], send_sem=red_send.at[h, slot], recv_sem=red_recv.at[h, slot],
            device_id={'dp': onward[h]}, device_id_type=MESH)

    def spread_copy(h, c):
        return pltpu.make_async_remote_copy(
            src_ref=out_rows(y, h, c), dst_ref=out_rows(y, h, c), send_sem=bc_send.at[h], recv_sem=bc_recv.at[h, c],
            device_id={'dp': back[h]}, device_id_type=MESH)

    def mate_copy(h, c):
        return pltpu.make_async_remote_copy(
            src_ref=out_rows(y, h, c), dst_ref=out_rows(y, h, c), send_sem=y_send.at[h], recv_sem=y_recv.at[h],
            device_id={'dp': mate}, device_id_type=MESH)

    def own_copy(h, c):
        return pltpu.make_async_copy(red.at[h, c % SLOTS], out_rows(y, h, c), own_sem.at[h])

    def rows_copy(h, u):
        return pltpu.make_async_copy(
            table.at[pl.ds(y * half + h * (half // 2) + u * size, size)],
            rows_buf.at[u % 2, pl.ds(h * size, size)], rows_sem.at[u % 2, h])

    def more_copy(u):
        return pltpu.make_async_copy(
            table.at[pl.ds((1 - y) * half + u * unit, unit)], more_buf.at[u % 2], more_sem.at[u % 2])

    def part_copy(h, u):
        return pltpu.make_async_copy(stage.at[pl.ds(h * size, size)], part_rows(h, u), part_sem.at[h])

    shard_first = tp * Y * half
    steps_in_unit = lax.broadcasted_iota(jnp.int32, (unit, 1), 0)

    def grads(table_rows, row_ids, t):
        at = pl.ds(pl.multiple_of(t * TILE, TILE), TILE)
        logits = jnp.dot(table_rows, x_t[:, at], preferred_element_type=jnp.float32)
        hit = row_ids == label[:, at]
        probs = jnp.where(row_ids + shard_first < VOCAB, jnp.exp(logits - lse[:, at]), 0.0)
        q = ((probs - jnp.where(hit, 1.0, 0.0)) * scale[:, at]).astype(jnp.bfloat16)
        return q, jnp.where(hit, logits, 0.0)

    def add_dx(table_rows, q, t):
        dx_t[t] = dx_t[t] + lax.dot_general(
            table_rows, q, (((0,), (0,)), ((), ())), preferred_element_type=jnp.float32)

    def settle(u):
        for h in range(2):
            part_copy(h, u).wait()

    def compute_main(u):
        for h in range(2):
            rows_copy(h, u).wait()

        @pl.when(u + 1 < chunks)
        def _():
            for h in range(2):
                rows_copy(h, u + 1).start()

        slot = u % 2
        mine = y * half + u * size + steps_in_unit
        row_ids = jnp.where(steps_in_unit < size, mine, mine + (half // 2 - size))

        def main_tile(t, carry):
            q, hits = grads(rows_buf[slot], row_ids, t)
            at = pl.ds(pl.multiple_of(t * TILE, TILE), TILE)
            q_t[:, at] = q
            target[:, at] = target[:, at] + jnp.sum(hits, axis=0, keepdims=True)

            @pl.when(t < own // TILE)
            def _():
                add_dx(rows_buf[slot], q_t[:, at], t)
            return carry

        lax.fori_loop(0, tokens // TILE, main_tile, 0)

        def table_tile(n, carry):
            at = pl.ds(pl.multiple_of(n * 256, 256), 256)
            stage[:, at] = jnp.dot(q_t[...], x[:, at], preferred_element_type=jnp.float32)
            return carry

        lax.fori_loop(0, width // 256, table_tile, 0)
        for h in range(2):
            part_copy(h, u).start()

    def compute_more(u):
        more_copy(u).wait()

        @pl.when(u + 1 < chunks)
        def _():
            more_copy(u + 1).start()

        slot = u % 2
        theirs = (1 - y) * half + u * unit + steps_in_unit

        def more_tile(t, carry):
            q, _ = grads(more_buf[slot], theirs, t)
            add_dx(more_buf[slot], q, t)
            return carry

        lax.fori_loop(0, own // TILE, more_tile, 0)

    def send_reduced(h, c, src):
        @pl.when(c >= SLOTS)
        def _():
            pl.semaphore_wait(credit.at[h], 1)
        reduce_copy(h, c, src).start()

    def free_slot(h, c):
        @pl.when(c + SLOTS < chunks)
        def _():
            pl.semaphore_signal(credit.at[h], inc=1, device_id={'dp': back[h]}, device_id_type=MESH)

    def reduce_phase(s):
        for h in range(2):
            p = place[h]
            c = s - p
            here = (c >= 0) & (c < chunks)

            @pl.when(here & (p == 0))
            def _():
                @pl.when(c >= 2)
                def _():
                    reduce_copy(h, c - 2, part_rows(h, c - 2)).wait_send()
                send_reduced(h, c, part_rows(h, c))

            @pl.when(here & (p > 0))
            def _():
                slot = c % SLOTS
                reduce_copy(h, c, red.at[h, slot]).wait_recv()
                fetch(h, c).wait()
                red[h, slot] = red[h, slot] + loc[h, c % 2]

                @pl.when(p < Z - 1)
                def _():
                    @pl.when(c >= 2)
                    def _():
                        reduce_copy(h, c - 2, red.at[h, (c - 2) % SLOTS]).wait_send()
                        free_slot(h, c - 2)
                    send_reduced(h, c, red.at[h, slot])

                @pl.when(p == Z - 1)
                def _():
                    own_copy(h, c).start()

            @pl.when((p > 0) & (c >= -1) & (c + 1 < chunks))
            def _():
                fetch(h, c + 1).start()

    def spread_phase(s):
        for h in range(2):
            p = place[h]
            c = s - 2 * (Z - 1) + p

            @pl.when((c >= 0) & (c < chunks))
            def _():
                @pl.when(p == Z - 1)
                def _():
                    own_copy(h, c).wait()
                    free_slot(h, c)

                @pl.when(p < Z - 1)
                def _():
                    spread_copy(h, c).wait_recv()

                @pl.when(p > 0)
                def _():
                    spread_copy(h, c).start()

                mate_copy(h, c).start()

    def core_copy(i):
        return pltpu.make_async_remote_copy(
            src_ref=dx_t.at[2 * i + 1 - core], dst_ref=from_core.at[i], send_sem=core_sem.at[0, i],
            recv_sem=core_sem.at[1, i], device_id={'tp': partner}, device_id_type=MESH)

    def beside_copy():
        return pltpu.make_async_remote_copy(
            src_ref=dx_t.at[beside], dst_ref=from_x, send_sem=x_sem.at[0], recv_sem=x_sem.at[1],
            device_id={'tp': beside}, device_id_type=MESH)

    def share_copy(i, other):
        return pltpu.make_async_remote_copy(
            src_ref=dx_q, dst_ref=dh.at[tp], send_sem=share_send.at[i], recv_sem=share_recv.at[i],
            device_id={'tp': other}, device_id_type=MESH)

    def keep_copy():
        return pltpu.make_async_copy(dx_q, dh.at[tp], share_send.at[3])

    others = (partner, beside, across)
    block = 128

    def add_into(j, ref):
        def body(i, carry):
            at = pl.ds(pl.multiple_of(i * block, block), block)
            dx_t[j, at] = dx_t[j, at] + ref[at]
            return carry
        lax.fori_loop(0, width // block, body, 0)

    def dx_start():
        for i in range(2):
            core_copy(i).start()

    def dx_middle():
        for i in range(2):
            core_copy(i).wait_recv()
            add_into(2 * i + core, from_core.at[i])
        beside_copy().start()

    def dx_finish():
        beside_copy().wait_recv()
        add_into(tp, from_x)
        for i in range(width // block):
            at = pl.ds(i * block, block)
            dx_q[:, at] = dx_t[tp, at].T

        levels[0] = jnp.zeros(levels.shape[1:], jnp.float32)
        own_loss = weight[:, :own] * lse[:, :own] * (1.0 / n_tp) - weight[:, :own] * target[:, :own]
        loss_part = own_loss - weight[:, own:] * target[:, own:]
        levels[0, 2:3] = sum(loss_part[:, i * width:(i + 1) * width] for i in range(own // width))
        count_block = min(64, quarter)

        def token_block(i, carry):
            at = pl.ds(pl.multiple_of(i * count_block, count_block), count_block)
            grad = dx_q[at, :]
            x_hat = hat[at, :]
            levels[0, 0:1] = levels[0, 0:1] + jnp.sum(grad * x_hat, axis=0, keepdims=True)
            levels[0, 1:2] = levels[0, 1:2] + jnp.sum(grad, axis=0, keepdims=True)
            grad_hat = grad * gain[...]
            mean_grad = jnp.mean(grad_hat, axis=-1, keepdims=True)
            mean_proj = jnp.mean(grad_hat * x_hat, axis=-1, keepdims=True)
            dx_q[at, :] = inv[at, 0:1] * (grad_hat - mean_grad - x_hat * mean_proj)
            return carry

        lax.fori_loop(0, quarter // count_block, token_block, 0)
        level_copy(0).start()
        for i, other in enumerate(others):
            share_copy(i, other).start()
        keep_copy().start()

    level_peers = ({'tp': beside}, {'tp': partner}, {'dp': mate}, {'dp': z_mate}, {'dp': z_far})

    def level_copy(i):
        return pltpu.make_async_remote_copy(
            src_ref=levels.at[i], dst_ref=arrived.at[i], send_sem=level_sem.at[0, i], recv_sem=level_sem.at[1, i],
            device_id=level_peers[i], device_id_type=MESH)

    def level_next(i):
        level_copy(i).wait_recv()
        if i + 1 < len(level_peers):
            levels[i + 1] = levels[i] + arrived[i]
            level_copy(i + 1).start()
        else:
            sums[...] = levels[i] + arrived[i]

    def dx_end():
        for i in range(2):
            core_copy(i).wait_send()
        beside_copy().wait_send()
        for i, other in enumerate(others):
            share_copy(i, other).wait()
        keep_copy().wait()
        for i in range(len(level_peers)):
            level_copy(i).wait_send()

    for h in range(2):
        rows_copy(h, 0).start()
    more_copy(0).start()
    target[...] = jnp.zeros_like(target)
    scale[...] = weight[...] / count[0:1, 0:1]

    def clear(t, carry):
        dx_t[t] = jnp.zeros(dx_t.shape[1:], jnp.float32)
        return carry

    lax.fori_loop(0, own // TILE, clear, 0)
    pl.semaphore_wait(barrier, 6 + inner)

    done = max(last_more(chunks), last_main(chunks))
    ticks = 1 + 2 * (chunks + 2 * (Z - 1))
    assert done + 18 < ticks

    def tick(i, carry):
        earlier = jnp.maximum(i - 1, 1)

        @pl.when(i == 1)
        def _():
            settle(0)

        @pl.when(i % 2 == 1)
        def _():
            reduce_phase(i // 2)

        @pl.when((i > 0) & (i % 2 == 0))
        def _():
            spread_phase(i // 2 - 1)

        @pl.when((i > 1) & has_main(earlier, chunks))
        def _():
            settle(main_unit(earlier))

        @pl.when((i == 0) | has_main(i, chunks))
        def _():
            compute_main(jnp.where(i == 0, 0, main_unit(i)))

        @pl.when(has_more(i, chunks))
        def _():
            compute_more(more_unit(i, chunks))

        events = ((1, dx_start), (2, dx_middle), (8, dx_finish), (9, lambda: level_next(0)), (10, lambda: level_next(1)),
                  (14, lambda: level_next(2)), (17, lambda: level_next(3)))
        for after, event in events:
            pl.when(i == done + after)(event)
        return carry

    lax.fori_loop(0, ticks, tick, 0)
    level_next(4)

    for h in range(2):
        p = place[h]
        mine = out.at[pl.ds(y * half + h * (half // 2), half // 2)]
        theirs = out.at[pl.ds((1 - y) * half + h * (half // 2), half // 2)]

        @pl.when(p < Z - 1)
        def _():
            for c in (chunks - 2, chunks - 1):
                reduce_copy(h, c, red.at[h, c % SLOTS]).wait_send()

        @pl.when(p > 0)
        def _():
            pltpu.make_async_copy(mine, mine, bc_send.at[h]).wait()

        pltpu.make_async_copy(mine, mine, y_send.at[h]).wait()
        pltpu.make_async_copy(theirs, theirs, y_recv.at[h]).wait()
    dx_end()


def backward(table, x, x_t, lse, weight, label, count, hat, inv, gain, n_tp, chunks):
    shard, width = table.shape
    half = shard // Y
    size = half // (2 * chunks)
    tokens = x.shape[0]
    quarter = tokens // Y // n_tp
    assert size * 2 * chunks == half and size % 16 == 0 and quarter == TILE
    f32 = jnp.float32
    dma = pltpu.SemaphoreType.DMA
    vmem = pl.BlockSpec(memory_space=pltpu.VMEM)
    hbm = pl.BlockSpec(memory_space=pl.ANY)
    flops = 2 * width * half * (2 * tokens + 3 * tokens // Y)
    return pl.pallas_call(
        functools.partial(backward_kernel, chunks),
        out_shape=(
            jax.ShapeDtypeStruct((shard, width), f32),
            jax.ShapeDtypeStruct((half, width), f32),
            jax.ShapeDtypeStruct((n_tp, quarter, width), f32),
            jax.ShapeDtypeStruct((8, width), f32)),
        in_specs=[hbm] + [vmem] * 9,
        out_specs=(hbm, hbm, hbm, vmem),
        scratch_shapes=[
            pltpu.VMEM((2, SLOTS, size, width), f32),
            pltpu.VMEM((2, 2, size, width), f32),
            pltpu.VMEM((2 * size, tokens), jnp.bfloat16),
            pltpu.VMEM((2, 2 * size, width), jnp.bfloat16),
            pltpu.VMEM((2, 2 * size, width), jnp.bfloat16),
            pltpu.VMEM((2 * size, width), f32),
            pltpu.VMEM((n_tp, width, quarter), f32),
            pltpu.VMEM((2, width, quarter), f32),
            pltpu.VMEM((width, quarter), f32),
            pltpu.VMEM((quarter, width), f32),
            pltpu.VMEM((1, tokens), f32), pltpu.VMEM((1, tokens), f32),
            pltpu.VMEM((5, 8, width), f32), pltpu.VMEM((5, 8, width), f32),
            dma((2, SLOTS)), dma((2, SLOTS)), pltpu.SemaphoreType.REGULAR((2,)),
            dma((2,)), dma((2, chunks)),
            dma((2,)), dma((2,)),
            dma((2, 2)), dma((2,)), dma((2,)), dma((2, 2)), dma((2,)),
            dma((2, 2)), dma((2,)), dma((4,)), dma((3,)), dma((2, 5)),
        ],
        compiler_params=pltpu.CompilerParams(
            collective_id=0, has_side_effects=True, vmem_limit_bytes=62 * 1024 * 1024),
        cost_estimate=pl.CostEstimate(flops=flops, bytes_accessed=12 * half * width, transcendentals=half * tokens),
    )(table, x, x_t, lse, weight, label, count, hat, inv, gain)


def solution(mesh):
    n_dp = mesh.shape['dp']
    n_tp = mesh.shape['tp']
    to_mate = [(i, i ^ 1) for i in range(n_dp)]

    def device_step(hidden, table, labels, loss_mask, ln_gain, ln_bias):
        batch, seq, width = hidden.shape
        tokens = batch * seq
        shard = table.shape[0]
        tp = lax.axis_index('tp')
        gain = ln_gain.astype(jnp.float32)[None]
        bias = ln_bias.astype(jnp.float32)[None]

        ids = jnp.stack([labels.reshape(tokens), loss_mask.reshape(tokens)])
        ids_all = jnp.concatenate([ids, lax.ppermute(ids, 'dp', to_mate)], axis=1)
        label = ids_all[0:1] - tp * shard
        weight = ids_all[1:2].astype(jnp.float32)
        mask = loss_mask.reshape(1, tokens).astype(jnp.float32)

        x, x_t, lse, count, hat, inv = forward(table, hidden.reshape(tokens, width), gain, bias, mask, n_dp, n_tp)
        grad_table, _, grad_hidden, sums = backward(table, x, x_t, lse, weight, label, count, hat, inv, gain, n_tp, CHUNKS)
        return (jnp.sum(sums[2]) / count[0, 0], grad_hidden.reshape(batch, seq, width).astype(jnp.bfloat16), grad_table,
                sums[0], sums[1])

    specs_in = (P('dp', None, None), P('tp', None), P('dp', None), P('dp', None), P(None), P(None))
    specs_out = (P(), P('dp', None, None), P('tp', None), P(None), P(None))
    return jax.shard_map(device_step, mesh=mesh, in_specs=specs_in, out_specs=specs_out, check_vma=False)
```

```python
import functools

import jax
import jax.numpy as jnp
from jax import lax
from jax.experimental import pallas as pl
from jax.experimental.pallas import tpu as pltpu
from jax.sharding import PartitionSpec as P

LN_EPS = 1e-5
VOCAB = 50257
Z = 4
Y = 2
UNITS = 33
PER_UNIT = 2
SLOTS = 12
TILE = 512
PIECES = 4
FORWARD_ROWS = 384
COLUMNS = 256
VMEM_BYTES = 67043328
MESH = pl.DeviceIdType.MESH


def signal(barrier, **where):
    pl.semaphore_signal(barrier, inc=1, device_id=where, device_id_type=MESH)


def remote(src, dst, send_sem, recv_sem, **where):
    return pltpu.make_async_remote_copy(
        src_ref=src, dst_ref=dst, send_sem=send_sem, recv_sem=recv_sem, device_id=where, device_id_type=MESH)


def neighbours(tp):
    core = tp % 2
    partner = tp + 1 - 2 * core
    beside = tp + 2 - 4 * (tp // 2)
    return partner, beside, beside + 1 - 2 * core


def tile_at(t):
    return slice(t * TILE, (t + 1) * TILE)


def aligned(start, size):
    return pl.ds(pl.multiple_of(start, size), size)


def head_kernel(
        n_dp, n_tp, table, hidden, gain, bias, labels, loss_mask,
        out, part, dh, sums,
        x, x_t, lse, scale, weight, label, target, hat, inv, send_q,
        got, block_buf, top, total, stats, counts, ids,
        red, loc, q_t, rows_buf, more_buf, stage, dx_t, from_core, from_x, levels, arrived,
        hidden_sem, block_sem, y_sem, beside_sem, core_sem, relay_sem, stat_send, stat_recv, count_send, count_recv,
        ids_sem,
        red_send, red_recv, credit, bc_send, bc_recv, mate_send, mate_recv, loc_sem, own_sem, part_sem, rows_sem, more_sem,
        swap_sem, cross_sem, share_send, share_recv, level_sem):
    own, width = hidden.shape
    tokens = Y * own
    shard = table.shape[0]
    half = shard // Y
    quarter = own // n_tp
    piece = quarter // PIECES
    batch, seq = labels.shape
    size = red.shape[2]
    chunks = half // (2 * size)
    strip = size * PER_UNIT
    units = chunks // PER_UNIT
    unit = 2 * strip
    block_rows = block_buf.shape[1]
    blocks = shard // block_rows
    last = PIECES - 1

    dp = lax.axis_index('dp')
    tp = lax.axis_index('tp')
    y = dp % Y
    z = dp // Y
    core = tp % 2
    mate = dp + 1 - 2 * y
    partner, beside, across = neighbours(tp)
    others = (partner, beside, across)
    dp_others = [lax.rem(dp + j, n_dp) for j in range(1, n_dp)]
    z_mate = dp + Y - 2 * Y * (z % 2)
    z_far = dp + 2 * Y - 4 * Y * (z // 2)
    place = (Z - 1 - z, z)
    onward = (dp - Y, dp + Y)
    back = (dp + Y, dp - Y)
    first_row = tp * shard

    barrier = pltpu.get_barrier_semaphore()
    for other in dp_others:
        signal(barrier, dp=other)
    for other in others:
        signal(barrier, tp=other)
        signal(barrier, dp=mate, tp=other)

    def hidden_copy(j):
        q = lax.rem(tp + j, n_tp)
        at = aligned(q * quarter, quarter)
        return pltpu.make_async_copy(hidden.at[at], x.at[at], hidden_sem.at[j])

    def block_copy(b):
        return pltpu.make_async_copy(
            table.at[pl.ds(b * block_rows, block_rows)], block_buf.at[b % 2], block_sem.at[b % 2])

    def got_piece(q, k):
        return got.at[q, pl.ds(k * piece, piece)]

    def y_copy(k):
        return remote(send_q.at[pl.ds(k * piece, piece)], got_piece(tp, k), y_sem.at[0, k], y_sem.at[1, k], dp=mate)

    def beside_copy(k):
        return remote(got_piece(tp, k), got_piece(tp, k), beside_sem.at[0, k], beside_sem.at[1, k], tp=beside)

    def core_copy(k):
        return remote(got_piece(tp, k), got_piece(tp, k), core_sem.at[0, k], core_sem.at[1, k], tp=partner)

    def relay_copy(k):
        return remote(got_piece(beside, k), got_piece(beside, k), relay_sem.at[0, k], relay_sem.at[1, k], tp=partner)

    def count_copy(j):
        return remote(counts.at[dp], counts.at[dp], count_send.at[j], count_recv.at[dp], dp=dp_others[j])

    def count_arrival(j):
        other = dp_others[j]
        return remote(counts.at[other], counts.at[other], count_send.at[j], count_recv.at[other], dp=other)

    def ids_copy(i):
        return remote((labels, loss_mask)[i], ids.at[i], ids_sem.at[0, i], ids_sem.at[1, i], dp=mate)

    def block_of(q, k):
        return aligned(q * quarter + k * piece, piece)

    def normalize(at):
        h = x[at, :].astype(jnp.float32)
        mean = jnp.mean(h, axis=-1, keepdims=True)
        centred = h - mean
        variance = jnp.mean(centred * centred, axis=-1, keepdims=True)
        inv_std = lax.rsqrt(variance + LN_EPS)
        x_hat = centred * inv_std
        normed = (x_hat * gain[...].astype(jnp.float32) + bias[...].astype(jnp.float32)).astype(jnp.bfloat16)
        wide = normed.astype(jnp.float32)
        x[at, :] = normed
        x_t[:, at] = wide.T.astype(jnp.bfloat16)
        return x_hat, inv_std, wide

    def first_piece(k, carry):
        x_hat, inv_std, wide = normalize(block_of(tp, k))
        at = aligned(k * piece, piece)
        send_q[at, :] = wide
        hat[at, :] = x_hat
        inv[at, :] = jnp.broadcast_to(inv_std, (piece, inv.shape[1]))

        @pl.when(k == 0)
        def _():
            pl.semaphore_wait(barrier, n_dp - 1 + 2 * len(others))
        y_copy(k).start()
        return carry

    def next_piece(j, carry):
        k = j % PIECES

        @pl.when(k == 0)
        def _():
            hidden_copy(1 + j // PIECES).wait()
        normalize(block_of(lax.rem(tp + 1 + j // PIECES, n_tp), k))
        return carry

    def convert(q, k):
        wide = got[q, aligned(k * piece, piece)]
        at = aligned(own + q * quarter + k * piece, piece)
        x[at, :] = wide.astype(jnp.bfloat16)
        x_t[:, at] = wide.T.astype(jnp.bfloat16)

    def block(b, carry):
        block_copy(b).wait()

        @pl.when(b + 1 < blocks)
        def _():
            block_copy(b + 1).start()

        phase = b % 6

        @pl.when((phase == 0) & (b > 0) & (b <= 6 * PIECES))
        def _():
            k = jnp.maximum(b // 6 - 1, 0)
            y_copy(k).wait_recv()
            beside_copy(k).start()
            core_copy(k).start()
            convert(tp, k)

        @pl.when((phase == 2) & (b >= 14) & (b < 14 + 6 * PIECES))
        def _():
            k = jnp.maximum(b - 14, 0) // 6
            beside_copy(k).wait_recv()
            relay_copy(k).start()
            convert(beside, k)

        @pl.when((phase == 4) & (b >= 10) & (b < 10 + 6 * PIECES))
        def _():
            k = jnp.maximum(b - 10, 0) // 6
            core_copy(k).wait_recv()
            convert(partner, k)

        @pl.when((phase == 4) & (b >= 16) & (b < 10 + 6 * PIECES))
        def _():
            k = jnp.maximum(b - 16, 0) // 6
            relay_copy(k).wait_recv()
            convert(across, k)

        slot = b % 2
        row_ids = first_row + b * block_rows + lax.broadcasted_iota(jnp.int32, (block_rows, 1), 0)
        for t in range(own // TILE):
            at = tile_at(t)
            logits = jnp.dot(block_buf[slot], x_t[:, at], preferred_element_type=jnp.float32)
            logits = jnp.where(row_ids < VOCAB, logits, -jnp.inf).reshape(block_rows // 8, 8, TILE)
            before = top[:, at]
            now = jnp.maximum(before, jnp.max(logits, axis=0))
            total[:, at] = total[:, at] * jnp.exp(before - now) + jnp.sum(jnp.exp(logits - now[None]), axis=0)
            top[:, at] = now
        return carry

    def stat_copies():
        where = [{'tp': other} for other in others] + [{'dp': mate}] + [{'dp': mate, 'tp': other} for other in others]
        return [remote(stats.at[0, tp], stats.at[int(i >= n_tp - 1), tp], stat_send.at[i], stat_recv.at[int(i >= n_tp - 1), tp],
                       **w) for i, w in enumerate(where)]

    def stat_arrival(side, other):
        return remote(stats.at[side, other], stats.at[side, other], stat_send.at[0], stat_recv.at[side, other], tp=partner)

    def part_rows(h, c):
        return part.at[pl.ds(h * (half // 2) + c * size, size)]

    def out_rows(side, h, c):
        return out.at[pl.ds(side * half + h * (half // 2) + c * size, size)]

    def fetch(h, c):
        return pltpu.make_async_copy(part_rows(h, c), loc.at[h, c % 2], loc_sem.at[h, c % 2])

    def reduce_copy(h, c, src):
        slot = c % SLOTS
        return remote(src, red.at[h, slot], red_send.at[h, slot], red_recv.at[h, slot], dp=onward[h])

    def spread_copy(h, c):
        return remote(out_rows(y, h, c), out_rows(y, h, c), bc_send.at[h], bc_recv.at[h, c], dp=back[h])

    def mate_copy(h, c):
        return remote(out_rows(y, h, c), out_rows(y, h, c), mate_send.at[h], mate_recv.at[h], dp=mate)

    def own_copy(h, c):
        return pltpu.make_async_copy(red.at[h, c % SLOTS], out_rows(y, h, c), own_sem.at[h])

    def rows_copy(h, u):
        return pltpu.make_async_copy(
            table.at[pl.ds(y * half + h * (half // 2) + u * strip, strip)],
            rows_buf.at[u % 2, pl.ds(h * strip, strip)], rows_sem.at[u % 2, h])

    def more_copy(u):
        return pltpu.make_async_copy(
            table.at[pl.ds((1 - y) * half + u * unit, unit)], more_buf.at[u % 2], more_sem.at[u % 2])

    def part_copy(h, u):
        return pltpu.make_async_copy(
            stage.at[pl.ds(h * strip, strip)], part.at[pl.ds(h * (half // 2) + u * strip, strip)], part_sem.at[h])

    unit_iota = lax.broadcasted_iota(jnp.int32, (unit, 1), 0)

    def grads(table_rows, row_ids, at):
        logits = jnp.dot(table_rows, x_t[:, at], preferred_element_type=jnp.float32)
        hit = row_ids == label[:, at]
        probs = jnp.where(row_ids + first_row < VOCAB, jnp.exp(logits - lse[:, at]), 0.0)
        q = ((probs - jnp.where(hit, 1.0, 0.0)) * scale[:, at]).astype(jnp.bfloat16)
        return q, jnp.where(hit, logits, 0.0)

    def add_dx(table_rows, q, t):
        dx_t[t] = dx_t[t] + lax.dot_general(
            table_rows, q, (((0,), (0,)), ((), ())), preferred_element_type=jnp.float32)

    def main_tile(u, t):
        slot = u % 2
        at = tile_at(t)
        mine = y * half + u * strip + unit_iota
        row_ids = jnp.where(unit_iota < strip, mine, mine + (half // 2 - strip))
        q, hits = grads(rows_buf[slot], row_ids, at)
        q_t[:, at] = q
        target[:, at] = target[:, at] + jnp.sum(hits, axis=0, keepdims=True)
        if t < own // TILE:
            add_dx(rows_buf[slot], q, t)

    def compute_own(u):
        for h in range(2):
            rows_copy(h, u).wait()

        @pl.when(u + 1 < units)
        def _():
            for h in range(2):
                rows_copy(h, u + 1).start()

        for t in range(own // TILE):
            main_tile(u, t)

    def compute_table(u):
        for t in range(own // TILE, tokens // TILE):
            main_tile(u, t)
        for n in range(width // COLUMNS):
            at = slice(n * COLUMNS, (n + 1) * COLUMNS)
            stage[:, at] = jnp.dot(q_t[...], x[:, at], preferred_element_type=jnp.float32)
        for h in range(2):
            part_copy(h, u).start()

    def compute_more(u):
        more_copy(u).wait()

        @pl.when(u + 1 < units)
        def _():
            more_copy(u + 1).start()

        slot = u % 2
        theirs = (1 - y) * half + u * unit + unit_iota
        for t in range(own // TILE):
            q, _ = grads(more_buf[slot], theirs, tile_at(t))
            add_dx(more_buf[slot], q, t)

    def settle(u):
        for h in range(2):
            part_copy(h, u).wait()

    def send_reduced(h, c, src):
        @pl.when(c >= SLOTS)
        def _():
            pl.semaphore_wait(credit.at[h], 1)
        reduce_copy(h, c, src).start()

    def free_slot(h, c):
        @pl.when(c + SLOTS < chunks)
        def _():
            pl.semaphore_signal(credit.at[h], inc=1, device_id={'dp': back[h]}, device_id_type=MESH)

    def reduce_phase(s):
        for h in range(2):
            p = place[h]
            c = s - p
            here = (c >= 0) & (c < chunks)

            @pl.when(here & (p == 0))
            def _():
                @pl.when(c >= 2)
                def _():
                    reduce_copy(h, c - 2, part_rows(h, c - 2)).wait_send()
                send_reduced(h, c, part_rows(h, c))

            @pl.when(here & (p > 0))
            def _():
                slot = c % SLOTS
                reduce_copy(h, c, red.at[h, slot]).wait_recv()
                fetch(h, c).wait()
                red[h, slot] = red[h, slot] + loc[h, c % 2]

                @pl.when(p < Z - 1)
                def _():
                    @pl.when(c >= 2)
                    def _():
                        reduce_copy(h, c - 2, red.at[h, (c - 2) % SLOTS]).wait_send()
                        free_slot(h, c - 2)
                    send_reduced(h, c, red.at[h, slot])

                @pl.when(p == Z - 1)
                def _():
                    own_copy(h, c).start()

            @pl.when((p > 0) & (c >= -1) & (c + 1 < chunks))
            def _():
                fetch(h, c + 1).start()

    def spread_phase(s):
        for h in range(2):
            p = place[h]
            c = s - 2 * (Z - 1) + p

            @pl.when((c >= 0) & (c < chunks))
            def _():
                @pl.when(p == Z - 1)
                def _():
                    own_copy(h, c).wait()
                    free_slot(h, c)

                @pl.when(p < Z - 1)
                def _():
                    spread_copy(h, c).wait_recv()

                @pl.when(p > 0)
                def _():
                    spread_copy(h, c).start()

                mate_copy(h, c).start()

    def swap_copy(i):
        return remote(dx_t.at[2 * i + 1 - core], from_core.at[i], swap_sem.at[0, i], swap_sem.at[1, i], tp=partner)

    def cross_copy():
        return remote(dx_t.at[beside], from_x, cross_sem.at[0], cross_sem.at[1], tp=beside)

    def share_copy(i):
        return remote(send_q, dh.at[tp], share_send.at[i], share_recv.at[i], tp=others[i])

    def keep_copy():
        return pltpu.make_async_copy(send_q, dh.at[tp], share_send.at[n_tp - 1])

    slab = 128

    def add_into(j, ref):
        def body(i, carry):
            at = aligned(i * slab, slab)
            dx_t[j, at] = dx_t[j, at] + ref[at]
            return carry
        lax.fori_loop(0, width // slab, body, 0)

    def dx_start():
        for i in range(2):
            swap_copy(i).start()

    def dx_middle():
        for i in range(2):
            swap_copy(i).wait_recv()
            add_into(2 * i + core, from_core.at[i])
        cross_copy().start()

    def dx_finish():
        cross_copy().wait_recv()
        add_into(tp, from_x)
        for i in range(width // slab):
            at = pl.ds(i * slab, slab)
            send_q[:, at] = dx_t[tp, at].T

        levels[0] = jnp.zeros(levels.shape[1:], jnp.float32)
        own_loss = weight[:, :own] * lse[:, :own] * (1.0 / n_tp) - weight[:, :own] * target[:, :own]
        loss_part = own_loss - weight[:, own:] * target[:, own:]
        levels[0, 2:3] = sum(loss_part[:, i * width:(i + 1) * width] for i in range(own // width))
        step = min(64, quarter)

        def token_block(i, carry):
            at = aligned(i * step, step)
            grad = send_q[at, :]
            x_hat = hat[at, :]
            levels[0, 0:1] = levels[0, 0:1] + jnp.sum(grad * x_hat, axis=0, keepdims=True)
            levels[0, 1:2] = levels[0, 1:2] + jnp.sum(grad, axis=0, keepdims=True)
            grad_hat = grad * gain[...].astype(jnp.float32)
            mean_grad = jnp.mean(grad_hat, axis=-1, keepdims=True)
            mean_proj = jnp.mean(grad_hat * x_hat, axis=-1, keepdims=True)
            send_q[at, :] = inv[at, 0:1] * (grad_hat - mean_grad - x_hat * mean_proj)
            return carry

        lax.fori_loop(0, quarter // step, token_block, 0)
        level_copy(0).start()
        for i in range(len(others)):
            share_copy(i).start()
        keep_copy().start()

    level_peers = ({'tp': beside}, {'tp': partner}, {'dp': mate}, {'dp': z_mate}, {'dp': z_far})

    def level_copy(i):
        return remote(levels.at[i], arrived.at[i], level_sem.at[0, i], level_sem.at[1, i], **level_peers[i])

    def level_next(i):
        level_copy(i).wait_recv()
        merged = levels[i] + arrived[i]
        if i + 1 < len(level_peers):
            levels[i + 1] = merged
            level_copy(i + 1).start()
        else:
            sums[...] = merged
            sums[2:3] = jnp.broadcast_to(jnp.sum(merged[2:3], axis=-1, keepdims=True) / tokens_counted(), (1, width))

    def tokens_counted():
        return sum(counts[j, 0:1, 0:1] for j in range(n_dp))

    for j in range(n_tp):
        hidden_copy(j).start()
    block_copy(0).start()
    for h in range(2):
        rows_copy(h, 0).start()
    more_copy(0).start()
    hidden_copy(0).wait()
    lax.fori_loop(0, PIECES, first_piece, 0)
    for i in range(2):
        ids_copy(i).start()
    counts[dp] = jnp.full(counts.shape[1:], jnp.sum(loss_mask[...].astype(jnp.float32)), jnp.float32)
    for j in range(n_dp - 1):
        count_copy(j).start()
    lax.fori_loop(0, (n_tp - 1) * PIECES, next_piece, 0)

    top[...] = jnp.full_like(top, jnp.finfo(jnp.float32).min)
    total[...] = jnp.zeros_like(total)
    target[...] = jnp.zeros_like(target)

    def clear(t, carry):
        dx_t[t] = jnp.zeros(dx_t.shape[1:], jnp.float32)
        return carry

    lax.fori_loop(0, own // TILE, clear, 0)
    assert blocks > 8 + 6 * PIECES
    lax.fori_loop(0, blocks, block, 0)

    best = jnp.max(top[...], axis=0, keepdims=True)
    stats[0, tp, 0:1] = best
    stats[0, tp, 1:2] = jnp.sum(total[...] * jnp.exp(top[...] - best), axis=0, keepdims=True)
    for copy in stat_copies():
        copy.start()

    relay_copy(last).wait_recv()
    convert(across, last)
    for i in range(2):
        ids_copy(i).wait()
    for j in range(n_dp - 1):
        count_arrival(j).wait_recv()
    for i in range(batch):
        for side, (rows_of, marks) in enumerate(((labels, loss_mask), (ids.at[0], ids.at[1]))):
            at = slice(side * own + i * seq, side * own + (i + 1) * seq)
            label[:, at] = rows_of[i:i + 1, :] - first_row
            weight[:, at] = marks[i:i + 1, :].astype(jnp.float32)
    scale[...] = weight[...] / tokens_counted()
    for k in range(PIECES):
        for copy in (y_copy(k), beside_copy(k), core_copy(k), relay_copy(k)):
            copy.wait_send()
    for j in range(n_dp - 1):
        count_copy(j).wait_send()
    for other in others:
        stat_arrival(0, other).wait_recv()
    for other in (tp,) + others:
        stat_arrival(1, other).wait_recv()
    for side in range(Y):
        tops = [stats[side, j, 0:1] for j in range(n_tp)]
        best = functools.reduce(jnp.maximum, tops)
        mass = sum(stats[side, j, 1:2] * jnp.exp(tops[j] - best) for j in range(n_tp))
        lse[:, side * own:(side + 1) * own] = best + jnp.log(mass)

    done = 3 * units - 1
    ticks = 2 + 2 * (chunks + 2 * (Z - 1))
    assert done + 36 < ticks

    def tick(i, carry):
        u = i // 3
        kind = i % 3

        @pl.when(i == 2)
        def _():
            settle(0)

        @pl.when((i >= 2) & (i % 2 == 0))
        def _():
            reduce_phase(jnp.maximum(i - 2, 0) // 2)

        @pl.when((i >= 2) & (i % 2 == 1))
        def _():
            spread_phase(jnp.maximum(i - 2, 0) // 2)

        @pl.when((i > 2) & (kind == 2) & (u < units))
        def _():
            settle(u)

        for j, compute in enumerate((compute_own, compute_table, compute_more)):
            pl.when((kind == j) & (u < units))(functools.partial(compute, u))

        events = ((1, dx_start), (4, dx_middle), (16, dx_finish), (18, lambda: level_next(0)), (20, lambda: level_next(1)),
                  (26, lambda: level_next(2)), (33, lambda: level_next(3)))
        for after, event in events:
            pl.when(i == done + after)(event)
        return carry

    lax.fori_loop(0, ticks, tick, 0)
    level_next(4)

    for h in range(2):
        p = place[h]
        mine = out.at[pl.ds(y * half + h * (half // 2), half // 2)]
        theirs = out.at[pl.ds((1 - y) * half + h * (half // 2), half // 2)]

        @pl.when(p < Z - 1)
        def _():
            for c in (chunks - 2, chunks - 1):
                reduce_copy(h, c, red.at[h, c % SLOTS]).wait_send()

        @pl.when(p > 0)
        def _():
            pltpu.make_async_copy(mine, mine, bc_send.at[h]).wait()

        pltpu.make_async_copy(mine, mine, mate_send.at[h]).wait()
        pltpu.make_async_copy(theirs, theirs, mate_recv.at[h]).wait()
    for copy in stat_copies():
        copy.wait_send()
    for i in range(2):
        swap_copy(i).wait_send()
    cross_copy().wait_send()
    for i in range(len(others)):
        share_copy(i).wait()
    keep_copy().wait()
    for i in range(len(level_peers)):
        level_copy(i).wait_send()


def head_step(table, hidden, gain, bias, labels, loss_mask, n_dp, n_tp):
    own, width = hidden.shape
    tokens = Y * own
    shard = table.shape[0]
    half = shard // Y
    size = half // (2 * UNITS * PER_UNIT)
    unit = 2 * size * PER_UNIT
    chunks = UNITS * PER_UNIT
    quarter = own // n_tp
    assert size * 2 * chunks == half and size % 8 == 0 and unit % 32 == 0 and quarter == TILE
    assert shard % FORWARD_ROWS == 0
    f32 = jnp.float32
    b16 = jnp.bfloat16
    i32 = jnp.int32
    lanes = 128
    dma = pltpu.SemaphoreType.DMA
    vmem = pl.BlockSpec(memory_space=pltpu.VMEM)
    hbm = pl.BlockSpec(memory_space=pl.ANY)
    flops = 2 * width * (own * shard + half * (2 * tokens + 3 * own))
    return pl.pallas_call(
        functools.partial(head_kernel, n_dp, n_tp),
        out_shape=(
            jax.ShapeDtypeStruct((shard, width), f32),
            jax.ShapeDtypeStruct((half, width), f32),
            jax.ShapeDtypeStruct((n_tp, quarter, width), f32),
            jax.ShapeDtypeStruct((8, width), f32)),
        in_specs=[hbm, hbm, vmem, vmem, vmem, vmem],
        out_specs=(hbm, hbm, hbm, vmem),
        scratch_shapes=[
            pltpu.VMEM((tokens, width), b16), pltpu.VMEM((width, tokens), b16),
            pltpu.VMEM((1, tokens), f32), pltpu.VMEM((1, tokens), f32), pltpu.VMEM((1, tokens), f32),
            pltpu.VMEM((1, tokens), i32), pltpu.VMEM((1, tokens), f32),
            pltpu.VMEM((quarter, width), f32), pltpu.VMEM((quarter, lanes), f32), pltpu.VMEM((quarter, width), f32),
            pltpu.VMEM((n_tp, quarter, width), f32), pltpu.VMEM((2, FORWARD_ROWS, width), b16),
            pltpu.VMEM((8, own), f32), pltpu.VMEM((8, own), f32),
            pltpu.VMEM((Y, n_tp, 2, own), f32), pltpu.VMEM((n_dp, 8, lanes), f32),
            pltpu.VMEM((2,) + labels.shape, i32),
            pltpu.VMEM((2, SLOTS, size, width), f32), pltpu.VMEM((2, 2, size, width), f32),
            pltpu.VMEM((unit, tokens), b16),
            pltpu.VMEM((2, unit, width), b16), pltpu.VMEM((2, unit, width), b16),
            pltpu.VMEM((unit, width), f32),
            pltpu.VMEM((n_tp, width, quarter), f32),
            pltpu.VMEM((2, width, quarter), f32), pltpu.VMEM((width, quarter), f32),
            pltpu.VMEM((5, 8, width), f32), pltpu.VMEM((5, 8, width), f32),
            dma((n_tp,)), dma((2,)), dma((2, PIECES)), dma((2, PIECES)), dma((2, PIECES)), dma((2, PIECES)),
            dma((2 * n_tp - 1,)), dma((Y, n_tp)), dma((n_dp - 1,)), dma((n_dp,)),
            dma((2, 2)),
            dma((2, SLOTS)), dma((2, SLOTS)), pltpu.SemaphoreType.REGULAR((2,)),
            dma((2,)), dma((2, chunks)), dma((2,)), dma((2,)),
            dma((2, 2)), dma((2,)), dma((2,)), dma((2, 2)), dma((2,)),
            dma((2, 2)), dma((2,)), dma((n_tp,)), dma((n_tp - 1,)), dma((2, 5)),
        ],
        compiler_params=pltpu.CompilerParams(
            collective_id=0, has_side_effects=True, vmem_limit_bytes=VMEM_BYTES),
        cost_estimate=pl.CostEstimate(flops=flops, bytes_accessed=12 * half * width, transcendentals=half * tokens),
    )(table, hidden, gain, bias, labels, loss_mask)


def solution(mesh):
    n_dp = mesh.shape['dp']
    n_tp = mesh.shape['tp']

    def device_step(hidden, table, labels, loss_mask, ln_gain, ln_bias):
        batch, seq, width = hidden.shape
        grad_table, _, grad_hidden, sums = head_step(
            table, hidden.reshape(batch * seq, width), ln_gain[None], ln_bias[None], labels, loss_mask, n_dp, n_tp)
        return sums[2, 0], grad_hidden.reshape(batch, seq, width).astype(jnp.bfloat16), grad_table, sums[0], sums[1]

    specs_in = (P('dp', None, None), P('tp', None), P('dp', None), P('dp', None), P(None), P(None))
    specs_out = (P(), P('dp', None, None), P('tp', None), P(None), P(None))
    return jax.shard_map(device_step, mesh=mesh, in_specs=specs_in, out_specs=specs_out, check_vma=False)
```

```python
import functools

import jax
import jax.numpy as jnp
from jax import lax
from jax.experimental import pallas as pl
from jax.experimental.pallas import tpu as pltpu
from jax.sharding import PartitionSpec as P

LN_EPS = 1e-5
VOCAB = 50257
Z = 4
Y = 2
UNITS = 33
PER_UNIT = 3
SLOTS = 16
TILE = 512
PIECES = 4
FORWARD_ROWS = 384
COLUMNS = 256
VMEM_BYTES = 67043328
MESH = pl.DeviceIdType.MESH


def signal(barrier, **where):
    pl.semaphore_signal(barrier, inc=1, device_id=where, device_id_type=MESH)


def remote(src, dst, send_sem, recv_sem, **where):
    return pltpu.make_async_remote_copy(
        src_ref=src, dst_ref=dst, send_sem=send_sem, recv_sem=recv_sem, device_id=where, device_id_type=MESH)


def neighbours(tp):
    core = tp % 2
    partner = tp + 1 - 2 * core
    beside = tp + 2 - 4 * (tp // 2)
    return partner, beside, beside + 1 - 2 * core


def tile_at(t):
    return slice(t * TILE, (t + 1) * TILE)


def aligned(start, size):
    return pl.ds(pl.multiple_of(start, size), size)


def head_kernel(
        n_dp, n_tp, table, hidden, gain, bias, labels, loss_mask,
        out, part, dh, sums,
        x, x_t, lse, scale, weight, label, target, hat, inv, send_q,
        got, block_buf, held, top, total, stats, counts, ids,
        red, loc, q_t, rows_buf, more_buf, stage, dx_t, from_core, from_x, levels, arrived,
        hidden_sem, block_sem, y_sem, beside_sem, core_sem, relay_sem, stat_send, stat_recv, count_send, count_recv,
        ids_sem,
        red_send, red_recv, credit, bc_send, bc_recv, mate_send, mate_recv, loc_sem, own_sem, part_sem, rows_sem, more_sem,
        swap_sem, cross_sem, share_send, share_recv, level_sem):
    own, width = hidden.shape
    tokens = Y * own
    shard = table.shape[0]
    half = shard // Y
    quarter = own // n_tp
    piece = quarter // PIECES
    batch, seq = labels.shape
    size = red.shape[2]
    chunks = half // (2 * size)
    strip = size * PER_UNIT
    units = chunks // PER_UNIT
    unit = 2 * strip
    block_rows = block_buf.shape[1]
    blocks = shard // block_rows
    last = PIECES - 1
    own_tiles, all_tiles, columns = own // TILE, tokens // TILE, width // COLUMNS

    dp = lax.axis_index('dp')
    tp = lax.axis_index('tp')
    y = dp % Y
    z = dp // Y
    core = tp % 2
    mate = dp + 1 - 2 * y
    partner, beside, across = neighbours(tp)
    others = (partner, beside, across)
    dp_others = [lax.rem(dp + j, n_dp) for j in range(1, n_dp)]
    z_mate = dp + Y - 2 * Y * (z % 2)
    z_far = dp + 2 * Y - 4 * Y * (z // 2)
    place = (Z - 1 - z, z)
    onward = (dp - Y, dp + Y)
    back = (dp + Y, dp - Y)
    first_row = tp * shard

    barrier = pltpu.get_barrier_semaphore()
    for other in dp_others:
        signal(barrier, dp=other)
    for other in others:
        signal(barrier, tp=other)
        signal(barrier, dp=mate, tp=other)

    def hidden_copy(j):
        q = lax.rem(tp + j, n_tp)
        at = aligned(q * quarter, quarter)
        return pltpu.make_async_copy(hidden.at[at], x.at[at], hidden_sem.at[j])

    def block_copy(b):
        return pltpu.make_async_copy(
            table.at[pl.ds(b * block_rows, block_rows)], block_buf.at[b % 2], block_sem.at[b % 2])

    def got_piece(q, k):
        return got.at[q, pl.ds(k * piece, piece)]

    def y_copy(k):
        return remote(send_q.at[pl.ds(k * piece, piece)], got_piece(tp, k), y_sem.at[0, k], y_sem.at[1, k], dp=mate)

    def beside_copy(k):
        return remote(got_piece(tp, k), got_piece(tp, k), beside_sem.at[0, k], beside_sem.at[1, k], tp=beside)

    def core_copy(k):
        return remote(got_piece(tp, k), got_piece(tp, k), core_sem.at[0, k], core_sem.at[1, k], tp=partner)

    def relay_copy(k):
        return remote(got_piece(beside, k), got_piece(beside, k), relay_sem.at[0, k], relay_sem.at[1, k], tp=partner)

    def count_copy(j):
        return remote(counts.at[dp], counts.at[dp], count_send.at[j], count_recv.at[dp], dp=dp_others[j])

    def count_arrival(j):
        other = dp_others[j]
        return remote(counts.at[other], counts.at[other], count_send.at[j], count_recv.at[other], dp=other)

    def ids_copy(i):
        return remote((labels, loss_mask)[i], ids.at[i], ids_sem.at[0, i], ids_sem.at[1, i], dp=mate)

    def row_of(ref):
        return ref[...].astype(jnp.float32)[None, :]

    def block_of(q, k):
        return aligned(q * quarter + k * piece, piece)

    def normalize(at):
        h = x[at, :].astype(jnp.float32)
        mean = jnp.mean(h, axis=-1, keepdims=True)
        centred = h - mean
        variance = jnp.mean(centred * centred, axis=-1, keepdims=True)
        inv_std = lax.rsqrt(variance + LN_EPS)
        x_hat = centred * inv_std
        normed = (x_hat * row_of(gain) + row_of(bias)).astype(jnp.bfloat16)
        wide = normed.astype(jnp.float32)
        x[at, :] = normed
        x_t[:, at] = wide.T.astype(jnp.bfloat16)
        return x_hat, inv_std, wide

    def first_piece(k, carry):
        x_hat, inv_std, wide = normalize(block_of(tp, k))
        at = aligned(k * piece, piece)
        send_q[at, :] = wide
        hat[at, :] = x_hat
        inv[at, :] = jnp.broadcast_to(inv_std, (piece, inv.shape[1]))

        @pl.when(k == 0)
        def _():
            pl.semaphore_wait(barrier, n_dp - 1 + 2 * len(others))
        y_copy(k).start()
        return carry

    def next_piece(j, carry):
        k = j % PIECES

        @pl.when(k == 0)
        def _():
            hidden_copy(1 + j // PIECES).wait()
        normalize(block_of(lax.rem(tp + 1 + j // PIECES, n_tp), k))
        return carry

    def convert(q, k):
        wide = got[q, aligned(k * piece, piece)]
        at = aligned(own + q * quarter + k * piece, piece)
        x[at, :] = wide.astype(jnp.bfloat16)
        x_t[:, at] = wide.T.astype(jnp.bfloat16)

    def fold(logits, at):
        logits = logits.reshape(block_rows // 8, 8, TILE)
        before = top[:, at]
        now = jnp.maximum(before, jnp.max(logits, axis=0))
        total[:, at] = total[:, at] * jnp.exp(before - now) + jnp.sum(jnp.exp(logits - now[None]), axis=0)
        top[:, at] = now

    def block(b, carry):
        block_copy(b).wait()

        @pl.when(b + 1 < blocks)
        def _():
            block_copy(b + 1).start()

        phase = b % 6

        @pl.when((phase == 0) & (b > 0) & (b <= 6 * PIECES))
        def _():
            k = jnp.maximum(b // 6 - 1, 0)
            y_copy(k).wait_recv()
            beside_copy(k).start()
            core_copy(k).start()
            convert(tp, k)

        @pl.when((phase == 2) & (b >= 14) & (b < 14 + 6 * PIECES))
        def _():
            k = jnp.maximum(b - 14, 0) // 6
            beside_copy(k).wait_recv()
            relay_copy(k).start()
            convert(beside, k)

        @pl.when((phase == 4) & (b >= 10) & (b < 10 + 6 * PIECES))
        def _():
            k = jnp.maximum(b - 10, 0) // 6
            core_copy(k).wait_recv()
            convert(partner, k)

        @pl.when((phase == 4) & (b >= 16) & (b < 10 + 6 * PIECES))
        def _():
            k = jnp.maximum(b - 16, 0) // 6
            relay_copy(k).wait_recv()
            convert(across, k)

        slot = b % 2
        row_ids = first_row + b * block_rows + lax.broadcasted_iota(jnp.int32, (block_rows, 1), 0)
        fold(held[...], tile_at(own_tiles - 1))
        for t in range(own_tiles):
            at = tile_at(t)
            logits = jnp.dot(block_buf[slot], x_t[:, at], preferred_element_type=jnp.float32)
            logits = jnp.where(row_ids < VOCAB, logits, -jnp.inf)
            if t + 1 < own_tiles:
                fold(logits, at)
            else:
                held[...] = logits
        return carry

    def stat_copies():
        where = [{'tp': other} for other in others] + [{'dp': mate}] + [{'dp': mate, 'tp': other} for other in others]
        return [remote(stats.at[0, tp], stats.at[int(i >= n_tp - 1), tp], stat_send.at[i], stat_recv.at[int(i >= n_tp - 1), tp],
                       **w) for i, w in enumerate(where)]

    def stat_arrival(side, other):
        return remote(stats.at[side, other], stats.at[side, other], stat_send.at[0], stat_recv.at[side, other], tp=partner)

    def part_rows(h, c):
        return part.at[pl.ds(h * (half // 2) + c * size, size)]

    def out_rows(side, h, c):
        return out.at[pl.ds(side * half + h * (half // 2) + c * size, size)]

    def fetch(h, c):
        return pltpu.make_async_copy(part_rows(h, c), loc.at[h, c % 2], loc_sem.at[h, c % 2])

    def reduce_copy(h, c, src):
        slot = c % SLOTS
        return remote(src, red.at[h, slot], red_send.at[h, slot], red_recv.at[h, slot], dp=onward[h])

    def spread_copy(h, c):
        return remote(out_rows(y, h, c), out_rows(y, h, c), bc_send.at[h], bc_recv.at[h, c], dp=back[h])

    def mate_copy(h, c):
        return remote(out_rows(y, h, c), out_rows(y, h, c), mate_send.at[h], mate_recv.at[h], dp=mate)

    def own_copy(h, c):
        return pltpu.make_async_copy(red.at[h, c % SLOTS], out_rows(y, h, c), own_sem.at[h])

    def rows_copy(h, u):
        return pltpu.make_async_copy(
            table.at[pl.ds(y * half + h * (half // 2) + u * strip, strip)],
            rows_buf.at[u % 2, pl.ds(h * strip, strip)], rows_sem.at[u % 2, h])

    def more_copy(u):
        return pltpu.make_async_copy(
            table.at[pl.ds((1 - y) * half + u * unit, unit)], more_buf.at[u % 2], more_sem.at[u % 2])

    def part_copy(h, u):
        return pltpu.make_async_copy(
            stage.at[pl.ds(h * strip, strip)], part.at[pl.ds(h * (half // 2) + u * strip, strip)], part_sem.at[h])

    unit_iota = lax.broadcasted_iota(jnp.int32, (unit, 1), 0)

    def grads(table_rows, row_ids, at):
        logits = jnp.dot(table_rows, x_t[:, at], preferred_element_type=jnp.float32)
        hit = row_ids == label[:, at]
        probs = jnp.where(row_ids + first_row < VOCAB, jnp.exp(logits - lse[:, at]), 0.0)
        q = ((probs - jnp.where(hit, 1.0, 0.0)) * scale[:, at]).astype(jnp.bfloat16)
        return q, jnp.where(hit, logits, 0.0)

    def add_dx(table_rows, q, t):
        dx_t[t] = dx_t[t] + lax.dot_general(
            table_rows, q, (((0,), (0,)), ((), ())), preferred_element_type=jnp.float32)

    def main_tile(u, t):
        slot = u % 2
        at = tile_at(t)
        mine = y * half + u * strip + unit_iota
        row_ids = jnp.where(unit_iota < strip, mine, mine + (half // 2 - strip))
        q, hits = grads(rows_buf[slot], row_ids, at)
        q_t[:, at] = q
        target[:, at] = target[:, at] + jnp.sum(hits, axis=0, keepdims=True)
        if t < own // TILE:
            add_dx(rows_buf[slot], q, t)

    def table_tile(n):
        at = slice(n * COLUMNS, (n + 1) * COLUMNS)
        stage[:, at] = jnp.dot(q_t[...], x[:, at], preferred_element_type=jnp.float32)

    def more_tile(u, t):
        theirs = (1 - y) * half + u * unit + unit_iota
        q, _ = grads(more_buf[u % 2], theirs, tile_at(t))
        add_dx(more_buf[u % 2], q, t)

    few = (all_tiles - own_tiles) // 4

    def compute_0(u):
        for h in range(2):
            rows_copy(h, u).wait()

        @pl.when(u + 1 < units)
        def _():
            for h in range(2):
                rows_copy(h, u + 1).start()

        for t in list(range(own_tiles // 2)) + list(range(own_tiles, own_tiles + few)):
            main_tile(u, t)

    def compute_1(u):
        for t in list(range(own_tiles // 2, own_tiles)) + list(range(own_tiles + few, own_tiles + 2 * few)):
            main_tile(u, t)

    def compute_2(u):
        for t in range(own_tiles + 2 * few, all_tiles):
            main_tile(u, t)
        for n in range(columns - 1):
            table_tile(n)

    def compute_3(u):
        more_copy(u).wait()

        @pl.when(u + 1 < units)
        def _():
            more_copy(u + 1).start()

        table_tile(columns - 1)
        for h in range(2):
            part_copy(h, u).start()
        for t in range(own_tiles // 2):
            more_tile(u, t)

    def compute_4(u):
        for t in range(own_tiles // 2, own_tiles):
            more_tile(u, t)

    def settle(u):
        for h in range(2):
            part_copy(h, u).wait()

    def send_reduced(h, c, src):
        @pl.when(c >= SLOTS)
        def _():
            pl.semaphore_wait(credit.at[h], 1)
        reduce_copy(h, c, src).start()

    def free_slot(h, c):
        @pl.when(c + SLOTS < chunks)
        def _():
            pl.semaphore_signal(credit.at[h], inc=1, device_id={'dp': back[h]}, device_id_type=MESH)

    def reduce_phase(s):
        for h in range(2):
            p = place[h]
            c = s - p
            here = (c >= 0) & (c < chunks)

            @pl.when(here & (p == 0))
            def _():
                @pl.when(c >= 2)
                def _():
                    reduce_copy(h, c - 2, part_rows(h, c - 2)).wait_send()
                send_reduced(h, c, part_rows(h, c))

            @pl.when(here & (p > 0))
            def _():
                slot = c % SLOTS
                reduce_copy(h, c, red.at[h, slot]).wait_recv()
                fetch(h, c).wait()
                red[h, slot] = red[h, slot] + loc[h, c % 2]

                @pl.when(p < Z - 1)
                def _():
                    @pl.when(c >= 2)
                    def _():
                        reduce_copy(h, c - 2, red.at[h, (c - 2) % SLOTS]).wait_send()
                        free_slot(h, c - 2)
                    send_reduced(h, c, red.at[h, slot])

                @pl.when(p == Z - 1)
                def _():
                    own_copy(h, c).start()

            @pl.when((p > 0) & (c >= -1) & (c + 1 < chunks))
            def _():
                fetch(h, c + 1).start()

    def spread_phase(s):
        for h in range(2):
            p = place[h]
            c = s - 2 * (Z - 1) + p

            @pl.when((c >= 0) & (c < chunks))
            def _():
                @pl.when(p == Z - 1)
                def _():
                    own_copy(h, c).wait()
                    free_slot(h, c)

                @pl.when(p < Z - 1)
                def _():
                    spread_copy(h, c).wait_recv()

                @pl.when(p > 0)
                def _():
                    spread_copy(h, c).start()

                mate_copy(h, c).start()

    def swap_copy(i):
        return remote(dx_t.at[2 * i + 1 - core], from_core.at[i], swap_sem.at[0, i], swap_sem.at[1, i], tp=partner)

    def cross_copy():
        return remote(dx_t.at[beside], from_x, cross_sem.at[0], cross_sem.at[1], tp=beside)

    def share_copy(i):
        return remote(send_q, got.at[tp], share_send.at[i], share_recv.at[i], tp=others[i])

    def pass_copy():
        return remote(got.at[beside], got.at[beside], share_send.at[2], share_recv.at[2], tp=partner)

    def round_dh(q, ref):
        at = aligned(q * quarter, quarter)
        x[at, :] = ref.astype(jnp.bfloat16)

    def dh_relay():
        share_copy(1).wait_recv()
        pass_copy().start()
        round_dh(beside, got[beside])
        share_copy(0).wait_recv()
        round_dh(partner, got[partner])
        round_dh(tp, send_q[...])

    def dh_copy():
        return pltpu.make_async_copy(x.at[pl.ds(0, own)], dh, hidden_sem.at[0])

    def dh_finish():
        pass_copy().wait_recv()
        round_dh(across, got[across])
        dh_copy().start()

    slab = 128

    def add_into(j, ref):
        def body(i, carry):
            at = aligned(i * slab, slab)
            dx_t[j, at] = dx_t[j, at] + ref[at]
            return carry
        lax.fori_loop(0, width // slab, body, 0)

    def dx_start():
        for i in range(2):
            swap_copy(i).start()

    def dx_middle():
        for i in range(2):
            swap_copy(i).wait_recv()
            add_into(2 * i + core, from_core.at[i])
        cross_copy().start()

    def dx_finish():
        cross_copy().wait_recv()
        add_into(tp, from_x)
        for i in range(width // slab):
            at = pl.ds(i * slab, slab)
            send_q[:, at] = dx_t[tp, at].T

        levels[0] = jnp.zeros(levels.shape[1:], jnp.float32)
        own_loss = weight[:, :own] * lse[:, :own] * (1.0 / n_tp) - weight[:, :own] * target[:, :own]
        loss_part = own_loss - weight[:, own:] * target[:, own:]
        levels[0, 2:3] = sum(loss_part[:, i * width:(i + 1) * width] for i in range(own // width))
        step = min(64, quarter)

        def token_block(i, carry):
            at = aligned(i * step, step)
            grad = send_q[at, :]
            x_hat = hat[at, :]
            levels[0, 0:1] = levels[0, 0:1] + jnp.sum(grad * x_hat, axis=0, keepdims=True)
            levels[0, 1:2] = levels[0, 1:2] + jnp.sum(grad, axis=0, keepdims=True)
            grad_hat = grad * row_of(gain)
            mean_grad = jnp.mean(grad_hat, axis=-1, keepdims=True)
            mean_proj = jnp.mean(grad_hat * x_hat, axis=-1, keepdims=True)
            send_q[at, :] = inv[at, 0:1] * (grad_hat - mean_grad - x_hat * mean_proj)
            return carry

        lax.fori_loop(0, quarter // step, token_block, 0)
        level_copy(0).start()
        for i in range(2):
            share_copy(i).start()

    level_peers = ({'tp': beside}, {'tp': partner}, {'dp': mate}, {'dp': z_mate}, {'dp': z_far})

    def level_copy(i):
        return remote(levels.at[i], arrived.at[i], level_sem.at[0, i], level_sem.at[1, i], **level_peers[i])

    def level_next(i):
        level_copy(i).wait_recv()
        merged = levels[i] + arrived[i]
        if i + 1 < len(level_peers):
            levels[i + 1] = merged
            level_copy(i + 1).start()
        else:
            sums[...] = merged
            sums[2:3] = jnp.broadcast_to(jnp.sum(merged[2:3], axis=-1, keepdims=True) / tokens_counted(), (1, width))

    def tokens_counted():
        return sum(counts[j, 0:1, 0:1] for j in range(n_dp))

    for j in range(n_tp):
        hidden_copy(j).start()
    block_copy(0).start()
    for h in range(2):
        rows_copy(h, 0).start()
    more_copy(0).start()
    hidden_copy(0).wait()
    lax.fori_loop(0, PIECES, first_piece, 0)
    for i in range(2):
        ids_copy(i).start()
    counts[dp] = jnp.full(counts.shape[1:], jnp.sum(loss_mask[...].astype(jnp.float32)), jnp.float32)
    for j in range(n_dp - 1):
        count_copy(j).start()
    lax.fori_loop(0, (n_tp - 1) * PIECES, next_piece, 0)

    top[...] = jnp.full_like(top, jnp.finfo(jnp.float32).min)
    total[...] = jnp.zeros_like(total)
    held[...] = jnp.full_like(held, -jnp.inf)
    target[...] = jnp.zeros_like(target)

    def clear(t, carry):
        dx_t[t] = jnp.zeros(dx_t.shape[1:], jnp.float32)
        return carry

    lax.fori_loop(0, own // TILE, clear, 0)
    assert blocks > 8 + 6 * PIECES
    lax.fori_loop(0, blocks, block, 0)
    fold(held[...], tile_at(own_tiles - 1))

    best = jnp.max(top[...], axis=0, keepdims=True)
    stats[0, tp, 0:1] = best
    stats[0, tp, 1:2] = jnp.sum(total[...] * jnp.exp(top[...] - best), axis=0, keepdims=True)
    for copy in stat_copies():
        copy.start()

    relay_copy(last).wait_recv()
    convert(across, last)
    for i in range(2):
        ids_copy(i).wait()
    for j in range(n_dp - 1):
        count_arrival(j).wait_recv()
    for i in range(batch):
        for side, (rows_of, marks) in enumerate(((labels, loss_mask), (ids.at[0], ids.at[1]))):
            at = slice(side * own + i * seq, side * own + (i + 1) * seq)
            label[:, at] = rows_of[i:i + 1, :] - first_row
            weight[:, at] = marks[i:i + 1, :].astype(jnp.float32)
    scale[...] = weight[...] / tokens_counted()
    for k in range(PIECES):
        for copy in (y_copy(k), beside_copy(k), core_copy(k), relay_copy(k)):
            copy.wait_send()
    for j in range(n_dp - 1):
        count_copy(j).wait_send()
    for other in others:
        stat_arrival(0, other).wait_recv()
    for other in (tp,) + others:
        stat_arrival(1, other).wait_recv()
    for side in range(Y):
        tops = [stats[side, j, 0:1] for j in range(n_tp)]
        best = functools.reduce(jnp.maximum, tops)
        mass = sum(stats[side, j, 1:2] * jnp.exp(tops[j] - best) for j in range(n_tp))
        lse[:, side * own:(side + 1) * own] = best + jnp.log(mass)

    computes = (compute_0, compute_1, compute_2, compute_3, compute_4)
    beats = len(computes)
    start = beats - 1
    done = beats * units - 1
    ticks = start + 2 * (chunks + 2 * (Z - 1))
    assert done + 38 < ticks

    def tick(i, carry):
        u = i // beats
        kind = i % beats
        since = jnp.maximum(i - start, 0)

        @pl.when(i == start)
        def _():
            settle(0)

        @pl.when((i >= start) & (since % 2 == 0))
        def _():
            reduce_phase(since // 2)

        @pl.when((i >= start) & (since % 2 == 1))
        def _():
            spread_phase(since // 2)

        @pl.when((i > start) & (kind == beats - 1) & (u < units))
        def _():
            settle(u)

        for j, compute in enumerate(computes):
            pl.when((kind == j) & (u < units))(functools.partial(compute, u))

        events = ((1, dx_start), (5, dx_middle), (22, dx_finish), (24, lambda: level_next(0)), (26, lambda: level_next(1)),
                  (33, lambda: level_next(2)), (37, lambda: level_next(3)), (38, dh_relay))
        for after, event in events:
            pl.when(i == done + after)(event)
        return carry

    lax.fori_loop(0, ticks, tick, 0)
    level_next(4)
    dh_finish()

    for h in range(2):
        p = place[h]
        mine = out.at[pl.ds(y * half + h * (half // 2), half // 2)]
        theirs = out.at[pl.ds((1 - y) * half + h * (half // 2), half // 2)]

        @pl.when(p < Z - 1)
        def _():
            for c in (chunks - 2, chunks - 1):
                reduce_copy(h, c, red.at[h, c % SLOTS]).wait_send()

        @pl.when(p > 0)
        def _():
            pltpu.make_async_copy(mine, mine, bc_send.at[h]).wait()

        pltpu.make_async_copy(mine, mine, mate_send.at[h]).wait()
        pltpu.make_async_copy(theirs, theirs, mate_recv.at[h]).wait()
    for copy in stat_copies():
        copy.wait_send()
    for i in range(2):
        swap_copy(i).wait_send()
    cross_copy().wait_send()
    for i in range(2):
        share_copy(i).wait_send()
    pass_copy().wait_send()
    dh_copy().wait()
    for i in range(len(level_peers)):
        level_copy(i).wait_send()


def head_step(table, hidden, gain, bias, labels, loss_mask, n_dp, n_tp):
    own, width = hidden.shape
    tokens = Y * own
    shard = table.shape[0]
    half = shard // Y
    size = half // (2 * UNITS * PER_UNIT)
    unit = 2 * size * PER_UNIT
    chunks = UNITS * PER_UNIT
    quarter = own // n_tp
    assert size * 2 * chunks == half and size % 8 == 0 and unit % 32 == 0 and quarter == TILE
    assert shard % FORWARD_ROWS == 0
    f32 = jnp.float32
    b16 = jnp.bfloat16
    i32 = jnp.int32
    lanes = 128
    dma = pltpu.SemaphoreType.DMA
    vmem = pl.BlockSpec(memory_space=pltpu.VMEM)
    hbm = pl.BlockSpec(memory_space=pl.ANY)
    flops = 2 * width * (own * shard + half * (2 * tokens + 3 * own))
    return pl.pallas_call(
        functools.partial(head_kernel, n_dp, n_tp),
        out_shape=(
            jax.ShapeDtypeStruct((shard, width), f32),
            jax.ShapeDtypeStruct((half, width), f32),
            jax.ShapeDtypeStruct((own, width), b16),
            jax.ShapeDtypeStruct((8, width), f32)),
        in_specs=[hbm, hbm, vmem, vmem, vmem, vmem],
        out_specs=(hbm, hbm, hbm, vmem),
        scratch_shapes=[
            pltpu.VMEM((tokens, width), b16), pltpu.VMEM((width, tokens), b16),
            pltpu.VMEM((1, tokens), f32), pltpu.VMEM((1, tokens), f32), pltpu.VMEM((1, tokens), f32),
            pltpu.VMEM((1, tokens), i32), pltpu.VMEM((1, tokens), f32),
            pltpu.VMEM((quarter, width), f32), pltpu.VMEM((quarter, lanes), f32), pltpu.VMEM((quarter, width), f32),
            pltpu.VMEM((n_tp, quarter, width), f32), pltpu.VMEM((2, FORWARD_ROWS, width), b16),
            pltpu.VMEM((FORWARD_ROWS, TILE), f32),
            pltpu.VMEM((8, own), f32), pltpu.VMEM((8, own), f32),
            pltpu.VMEM((Y, n_tp, 2, own), f32), pltpu.VMEM((n_dp, 8, lanes), f32),
            pltpu.VMEM((2,) + labels.shape, i32),
            pltpu.VMEM((2, SLOTS, size, width), f32), pltpu.VMEM((2, 2, size, width), f32),
            pltpu.VMEM((unit, tokens), b16),
            pltpu.VMEM((2, unit, width), b16), pltpu.VMEM((2, unit, width), b16),
            pltpu.VMEM((unit, width), f32),
            pltpu.VMEM((n_tp, width, quarter), f32),
            pltpu.VMEM((2, width, quarter), f32), pltpu.VMEM((width, quarter), f32),
            pltpu.VMEM((5, 8, width), f32), pltpu.VMEM((5, 8, width), f32),
            dma((n_tp,)), dma((2,)), dma((2, PIECES)), dma((2, PIECES)), dma((2, PIECES)), dma((2, PIECES)),
            dma((2 * n_tp - 1,)), dma((Y, n_tp)), dma((n_dp - 1,)), dma((n_dp,)),
            dma((2, 2)),
            dma((2, SLOTS)), dma((2, SLOTS)), pltpu.SemaphoreType.REGULAR((2,)),
            dma((2,)), dma((2, chunks)), dma((2,)), dma((2,)),
            dma((2, 2)), dma((2,)), dma((2,)), dma((2, 2)), dma((2,)),
            dma((2, 2)), dma((2,)), dma((3,)), dma((3,)), dma((2, 5)),
        ],
        compiler_params=pltpu.CompilerParams(
            collective_id=0, has_side_effects=True, vmem_limit_bytes=VMEM_BYTES),
        cost_estimate=pl.CostEstimate(flops=flops, bytes_accessed=12 * half * width, transcendentals=half * tokens),
    )(table, hidden, gain, bias, labels, loss_mask)


def solution(mesh):
    n_dp = mesh.shape['dp']
    n_tp = mesh.shape['tp']

    def device_step(hidden, table, labels, loss_mask, ln_gain, ln_bias):
        batch, seq, width = hidden.shape
        grad_table, _, grad_hidden, sums = head_step(
            table, hidden.reshape(batch * seq, width), ln_gain, ln_bias, labels, loss_mask, n_dp, n_tp)
        return sums[2, 0], grad_hidden.reshape(batch, seq, width), grad_table, sums[0], sums[1]

    specs_in = (P('dp', None, None), P('tp', None), P('dp', None), P('dp', None), P(None), P(None))
    specs_out = (P(), P('dp', None, None), P('tp', None), P(None), P(None))
    return jax.shard_map(device_step, mesh=mesh, in_specs=specs_in, out_specs=specs_out, check_vma=False)
```

```python
import functools

import jax
import jax.numpy as jnp
from jax import lax
from jax.experimental import pallas as pl
from jax.experimental.pallas import tpu as pltpu
from jax.sharding import PartitionSpec as P

LN_EPS = 1e-5
VOCAB = 50257
Z = 4
Y = 2
UNITS = 33
PER_UNIT = 3
SLOTS = 16
TILE = 512
PIECES = 4
FORWARD_ROWS = 704
PLACE_ROWS = 264
PLACE_SLOTS = 12
COLUMNS = 256
VMEM_BYTES = 67043328
MESH = pl.DeviceIdType.MESH


def signal(barrier, **where):
    pl.semaphore_signal(barrier, inc=1, device_id=where, device_id_type=MESH)


def remote(src, dst, send_sem, recv_sem, **where):
    return pltpu.make_async_remote_copy(
        src_ref=src, dst_ref=dst, send_sem=send_sem, recv_sem=recv_sem, device_id=where, device_id_type=MESH)


def neighbours(tp):
    core = tp % 2
    partner = tp + 1 - 2 * core
    beside = tp + 2 - 4 * (tp // 2)
    return partner, beside, beside + 1 - 2 * core


def tile_at(t):
    return slice(t * TILE, (t + 1) * TILE)


def aligned(start, size):
    return pl.ds(pl.multiple_of(start, size), size)


def head_kernel(
        n_dp, n_tp, table, hidden, gain, bias, labels, loss_mask,
        out, part, dh, sums,
        x, x_t, lse, scale, weight, label, target, hat, inv, send_q,
        got, block_buf, held, top, total, stats, counts, ids,
        red, loc, q_t, rows_buf, more_buf, stage, dx_t, from_core, from_x, levels, arrived,
        hidden_sem, block_sem, y_sem, beside_sem, core_sem, relay_sem, stat_send, stat_recv, count_send, count_recv,
        ids_sem,
        red_send, red_recv, credit, bc_send, bc_recv, mate_send, mate_recv, loc_sem, own_sem, part_sem, rows_sem, more_sem,
        swap_sem, cross_sem, share_send, share_recv, level_sem):
    own, width = hidden.shape
    tokens = Y * own
    shard = table.shape[0]
    half = shard // Y
    quarter = own // n_tp
    piece = quarter // PIECES
    batch, seq = labels.shape
    size = red.shape[2]
    chunks = half // (2 * size)
    strip = size * PER_UNIT
    units = chunks // PER_UNIT
    unit = 2 * strip
    block_rows = block_buf.shape[1]
    blocks = shard // block_rows
    last = PIECES - 1
    own_tiles, all_tiles, columns = own // TILE, tokens // TILE, width // COLUMNS

    dp = lax.axis_index('dp')
    tp = lax.axis_index('tp')
    y = dp % Y
    z = dp // Y
    core = tp % 2
    mate = dp + 1 - 2 * y
    partner, beside, across = neighbours(tp)
    others = (partner, beside, across)
    dp_others = [lax.rem(dp + j, n_dp) for j in range(1, n_dp)]
    z_mate = dp + Y - 2 * Y * (z % 2)
    z_far = dp + 2 * Y - 4 * Y * (z // 2)
    place = (Z - 1 - z, z)
    onward = (dp - Y, dp + Y)
    back = (dp + Y, dp - Y)
    first_row = tp * shard

    barrier = pltpu.get_barrier_semaphore()
    for other in dp_others:
        signal(barrier, dp=other)
    for other in others:
        signal(barrier, tp=other)
        signal(barrier, dp=mate, tp=other)

    def hidden_copy(j):
        q = lax.rem(tp + j, n_tp)
        at = aligned(q * quarter, quarter)
        return pltpu.make_async_copy(hidden.at[at], x.at[at], hidden_sem.at[j])

    def block_copy(b):
        return pltpu.make_async_copy(
            table.at[pl.ds(b * block_rows, block_rows)], block_buf.at[b % 2], block_sem.at[b % 2])

    def got_piece(q, k):
        return got.at[q, pl.ds(k * piece, piece)]

    def y_copy(k):
        return remote(send_q.at[pl.ds(k * piece, piece)], got_piece(tp, k), y_sem.at[0, k], y_sem.at[1, k], dp=mate)

    def beside_copy(k):
        return remote(got_piece(tp, k), got_piece(tp, k), beside_sem.at[0, k], beside_sem.at[1, k], tp=beside)

    def core_copy(k):
        return remote(got_piece(tp, k), got_piece(tp, k), core_sem.at[0, k], core_sem.at[1, k], tp=partner)

    def relay_copy(k):
        return remote(got_piece(beside, k), got_piece(beside, k), relay_sem.at[0, k], relay_sem.at[1, k], tp=partner)

    def count_copy(j):
        return remote(counts.at[dp], counts.at[dp], count_send.at[j], count_recv.at[dp], dp=dp_others[j])

    def count_arrival(j):
        other = dp_others[j]
        return remote(counts.at[other], counts.at[other], count_send.at[j], count_recv.at[other], dp=other)

    def ids_copy(i):
        return remote((labels, loss_mask)[i], ids.at[i], ids_sem.at[0, i], ids_sem.at[1, i], dp=mate)

    def row_of(ref):
        return ref[...].astype(jnp.float32)[None, :]

    def block_of(q, k):
        return aligned(q * quarter + k * piece, piece)

    def normalize(at):
        h = x[at, :].astype(jnp.float32)
        mean = jnp.mean(h, axis=-1, keepdims=True)
        centred = h - mean
        variance = jnp.mean(centred * centred, axis=-1, keepdims=True)
        inv_std = lax.rsqrt(variance + LN_EPS)
        x_hat = centred * inv_std
        normed = (x_hat * row_of(gain) + row_of(bias)).astype(jnp.bfloat16)
        wide = normed.astype(jnp.float32)
        x[at, :] = normed
        x_t[:, at] = wide.T.astype(jnp.bfloat16)
        return x_hat, inv_std, wide

    def first_piece(k, carry):
        x_hat, inv_std, wide = normalize(block_of(tp, k))
        at = aligned(k * piece, piece)
        send_q[at, :] = wide
        hat[at, :] = x_hat
        inv[at, :] = jnp.broadcast_to(inv_std, (piece, inv.shape[1]))
        return carry

    def next_piece(j, carry):
        k = j % PIECES

        @pl.when(k == 0)
        def _():
            hidden_copy(1 + j // PIECES).wait()
        normalize(block_of(lax.rem(tp + 1 + j // PIECES, n_tp), k))
        return carry

    def convert(q, k):
        wide = got[q, aligned(k * piece, piece)]
        at = aligned(own + q * quarter + k * piece, piece)
        x[at, :] = wide.astype(jnp.bfloat16)
        x_t[:, at] = wide.T.astype(jnp.bfloat16)

    def fold(logits, at):
        logits = logits.reshape(block_rows // 8, 8, TILE)
        before = top[:, at]
        now = jnp.maximum(before, jnp.max(logits, axis=0))
        total[:, at] = total[:, at] * jnp.exp(before - now) + jnp.sum(jnp.exp(logits - now[None]), axis=0)
        top[:, at] = now

    def block(b, carry):
        block_copy(b).wait()

        @pl.when(b + 1 < blocks)
        def _():
            block_copy(b + 1).start()

        def every_third(first, count):
            d = b - first
            return (d >= 0) & (d < 3 * count) & (jnp.maximum(d, 0) % 3 == 0), jnp.maximum(d, 0) // 3

        due, k_y = every_third(4, PIECES)

        @pl.when(due)
        def _():
            y_copy(k_y).wait_recv()
            beside_copy(k_y).start()
            core_copy(k_y).start()
            convert(tp, k_y)

        due, k_core = every_third(5, PIECES)

        @pl.when(due)
        def _():
            core_copy(k_core).wait_recv()
            convert(partner, k_core)

        due, k_x = every_third(8, PIECES)

        @pl.when(due)
        def _():
            beside_copy(k_x).wait_recv()
            relay_copy(k_x).start()
            convert(beside, k_x)

        due, k_relay = every_third(9, PIECES - 1)

        @pl.when(due)
        def _():
            relay_copy(k_relay).wait_recv()
            convert(across, k_relay)

        slot = b % 2
        row_ids = first_row + b * block_rows + lax.broadcasted_iota(jnp.int32, (block_rows, 1), 0)
        fold(held[...], tile_at(own_tiles - 1))
        for t in range(own_tiles):
            at = tile_at(t)
            logits = jnp.dot(block_buf[slot], x_t[:, at], preferred_element_type=jnp.float32)
            logits = jnp.where(row_ids < VOCAB, logits, -jnp.inf)
            if t + 1 < own_tiles:
                fold(logits, at)
            else:
                held[...] = logits
        return carry

    def stat_copies():
        where = [{'tp': other} for other in others] + [{'dp': mate}] + [{'dp': mate, 'tp': other} for other in others]
        return [remote(stats.at[0, tp], stats.at[int(i >= n_tp - 1), tp], stat_send.at[i], stat_recv.at[int(i >= n_tp - 1), tp],
                       **w) for i, w in enumerate(where)]

    def stat_arrival(side, other):
        return remote(stats.at[side, other], stats.at[side, other], stat_send.at[0], stat_recv.at[side, other], tp=partner)

    def part_rows(h, c):
        return part.at[pl.ds(h * (half // 2) + c * size, size)]

    def out_rows(side, h, c):
        return out.at[pl.ds(side * half + h * (half // 2) + c * size, size)]

    def fetch(h, c):
        return pltpu.make_async_copy(part_rows(h, c), loc.at[h, c % 2], loc_sem.at[h, c % 2])

    def reduce_copy(h, c, src):
        slot = c % SLOTS
        return remote(src, red.at[h, slot], red_send.at[h, slot], red_recv.at[h, slot], dp=onward[h])

    def spread_copy(h, c):
        return remote(out_rows(y, h, c), out_rows(y, h, c), bc_send.at[h], bc_recv.at[h, c], dp=back[h])

    def mate_copy(h, c):
        return remote(out_rows(y, h, c), out_rows(y, h, c), mate_send.at[h], mate_recv.at[h], dp=mate)

    def own_copy(h, c):
        return pltpu.make_async_copy(red.at[h, c % SLOTS], out_rows(y, h, c), own_sem.at[h])

    def rows_copy(h, u):
        return pltpu.make_async_copy(
            table.at[pl.ds(y * half + h * (half // 2) + u * strip, strip)],
            rows_buf.at[u % 2, pl.ds(h * strip, strip)], rows_sem.at[u % 2, h])

    def more_copy(u):
        return pltpu.make_async_copy(
            table.at[pl.ds((1 - y) * half + u * unit, unit)], more_buf.at[u % 2], more_sem.at[u % 2])

    def part_copy(h, u):
        return pltpu.make_async_copy(
            stage.at[pl.ds(h * strip, strip)], part.at[pl.ds(h * (half // 2) + u * strip, strip)], part_sem.at[h])

    unit_iota = lax.broadcasted_iota(jnp.int32, (unit, 1), 0)

    def grads(table_rows, row_ids, at):
        logits = jnp.dot(table_rows, x_t[:, at], preferred_element_type=jnp.float32)
        hit = row_ids == label[:, at]
        probs = jnp.where(row_ids + first_row < VOCAB, jnp.exp(logits - lse[:, at]), 0.0)
        q = ((probs - jnp.where(hit, 1.0, 0.0)) * scale[:, at]).astype(jnp.bfloat16)
        return q, jnp.where(hit, logits, 0.0)

    def add_dx(table_rows, q, t):
        dx_t[t] = dx_t[t] + lax.dot_general(
            table_rows, q, (((0,), (0,)), ((), ())), preferred_element_type=jnp.float32)

    def main_tile(u, t):
        slot = u % 2
        at = tile_at(t)
        mine = y * half + u * strip + unit_iota
        row_ids = jnp.where(unit_iota < strip, mine, mine + (half // 2 - strip))
        q, hits = grads(rows_buf[slot], row_ids, at)
        q_t[:, at] = q
        target[:, at] = target[:, at] + jnp.sum(hits, axis=0, keepdims=True)
        if t < own // TILE:
            add_dx(rows_buf[slot], q, t)

    def table_tile(n):
        at = slice(n * COLUMNS, (n + 1) * COLUMNS)
        stage[:, at] = jnp.dot(q_t[...], x[:, at], preferred_element_type=jnp.float32)

    def more_tile(u, t):
        theirs = (1 - y) * half + u * unit + unit_iota
        q, _ = grads(more_buf[u % 2], theirs, tile_at(t))
        add_dx(more_buf[u % 2], q, t)

    few = (all_tiles - own_tiles) // 4

    def compute_0(u):
        for h in range(2):
            rows_copy(h, u).wait()

        @pl.when(u + 1 < units)
        def _():
            for h in range(2):
                rows_copy(h, u + 1).start()

        for t in list(range(own_tiles // 2)) + list(range(own_tiles, own_tiles + few)):
            main_tile(u, t)

    def compute_1(u):
        for t in list(range(own_tiles // 2, own_tiles)) + list(range(own_tiles + few, own_tiles + 2 * few)):
            main_tile(u, t)

    def compute_2(u):
        for t in range(own_tiles + 2 * few, all_tiles):
            main_tile(u, t)
        for n in range(columns):
            table_tile(n)
        for h in range(2):
            part_copy(h, u).start()

    def compute_3(u):
        more_copy(u).wait()

        @pl.when(u + 1 < units)
        def _():
            more_copy(u + 1).start()

        for t in range(own_tiles // 2):
            more_tile(u, t)

    def compute_4(u):
        for t in range(own_tiles // 2, own_tiles):
            more_tile(u, t)

    def settle(u):
        for h in range(2):
            part_copy(h, u).wait()

    def send_reduced(h, c, src):
        @pl.when(c >= SLOTS)
        def _():
            pl.semaphore_wait(credit.at[h], 1)
        reduce_copy(h, c, src).start()

    def free_slot(h, c):
        @pl.when(c + SLOTS < chunks)
        def _():
            pl.semaphore_signal(credit.at[h], inc=1, device_id={'dp': back[h]}, device_id_type=MESH)

    def reduce_phase(s):
        for h in range(2):
            p = place[h]
            c = s - p
            here = (c >= 0) & (c < chunks)

            @pl.when(here & (p == 0))
            def _():
                @pl.when(c >= 2)
                def _():
                    reduce_copy(h, c - 2, part_rows(h, c - 2)).wait_send()
                send_reduced(h, c, part_rows(h, c))

            @pl.when(here & (p > 0))
            def _():
                slot = c % SLOTS
                reduce_copy(h, c, red.at[h, slot]).wait_recv()
                fetch(h, c).wait()
                red[h, slot] = red[h, slot] + loc[h, c % 2]

                @pl.when(p < Z - 1)
                def _():
                    @pl.when(c >= 2)
                    def _():
                        reduce_copy(h, c - 2, red.at[h, (c - 2) % SLOTS]).wait_send()
                        free_slot(h, c - 2)
                    send_reduced(h, c, red.at[h, slot])

                @pl.when(p == Z - 1)
                def _():
                    own_copy(h, c).start()

            @pl.when((p > 0) & (c >= -1) & (c + 1 < chunks))
            def _():
                fetch(h, c + 1).start()

    def spread_phase(s):
        for h in range(2):
            p = place[h]
            c = s - 2 * (Z - 1) + p

            @pl.when((c >= 0) & (c < chunks))
            def _():
                @pl.when(p == Z - 1)
                def _():
                    own_copy(h, c).wait()
                    free_slot(h, c)

                @pl.when(p < Z - 1)
                def _():
                    spread_copy(h, c).wait_recv()

                @pl.when(p > 0)
                def _():
                    spread_copy(h, c).start()

                mate_copy(h, c).start()

    def swap_copy(i):
        return remote(dx_t.at[2 * i + 1 - core], from_core.at[i], swap_sem.at[0, i], swap_sem.at[1, i], tp=partner)

    def cross_copy():
        return remote(dx_t.at[beside], from_x, cross_sem.at[0], cross_sem.at[1], tp=beside)

    def share_copy(i):
        return remote(send_q, got.at[tp], share_send.at[i], share_recv.at[i], tp=others[i])

    def pass_copy():
        return remote(got.at[beside], got.at[beside], share_send.at[2], share_recv.at[2], tp=partner)

    def round_dh(q, ref):
        at = aligned(q * quarter, quarter)
        x[at, :] = ref.astype(jnp.bfloat16)

    def dh_relay():
        share_copy(1).wait_recv()
        pass_copy().start()
        round_dh(beside, got[beside])
        share_copy(0).wait_recv()
        round_dh(partner, got[partner])
        round_dh(tp, send_q[...])

    def dh_copy():
        return pltpu.make_async_copy(x.at[pl.ds(0, own)], dh, hidden_sem.at[0])

    def dh_finish():
        pass_copy().wait_recv()
        round_dh(across, got[across])
        dh_copy().start()

    slab = 128

    def add_into(j, ref):
        def body(i, carry):
            at = aligned(i * slab, slab)
            dx_t[j, at] = dx_t[j, at] + ref[at]
            return carry
        lax.fori_loop(0, width // slab, body, 0)

    def dx_start():
        for i in range(2):
            swap_copy(i).start()

    def dx_middle():
        for i in range(2):
            swap_copy(i).wait_recv()
            add_into(2 * i + core, from_core.at[i])
        cross_copy().start()

    def dx_finish():
        cross_copy().wait_recv()
        add_into(tp, from_x)
        for i in range(width // slab):
            at = pl.ds(i * slab, slab)
            send_q[:, at] = dx_t[tp, at].T

        levels[0] = jnp.zeros(levels.shape[1:], jnp.float32)
        own_loss = weight[:, :own] * lse[:, :own] * (1.0 / n_tp) - weight[:, :own] * target[:, :own]
        loss_part = own_loss - weight[:, own:] * target[:, own:]
        levels[0, 2:3] = sum(loss_part[:, i * width:(i + 1) * width] for i in range(own // width))
        step = min(64, quarter)

        def token_block(i, carry):
            at = aligned(i * step, step)
            grad = send_q[at, :]
            x_hat = hat[at, :]
            levels[0, 0:1] = levels[0, 0:1] + jnp.sum(grad * x_hat, axis=0, keepdims=True)
            levels[0, 1:2] = levels[0, 1:2] + jnp.sum(grad, axis=0, keepdims=True)
            grad_hat = grad * row_of(gain)
            mean_grad = jnp.mean(grad_hat, axis=-1, keepdims=True)
            mean_proj = jnp.mean(grad_hat * x_hat, axis=-1, keepdims=True)
            send_q[at, :] = inv[at, 0:1] * (grad_hat - mean_grad - x_hat * mean_proj)
            return carry

        lax.fori_loop(0, quarter // step, token_block, 0)
        level_copy(0).start()
        for i in range(2):
            share_copy(i).start()

    level_peers = ({'tp': beside}, {'tp': partner}, {'dp': mate}, {'dp': z_mate}, {'dp': z_far})

    def level_copy(i):
        return remote(levels.at[i], arrived.at[i], level_sem.at[0, i], level_sem.at[1, i], **level_peers[i])

    def level_next(i):
        level_copy(i).wait_recv()
        merged = levels[i] + arrived[i]
        if i + 1 < len(level_peers):
            levels[i + 1] = merged
            level_copy(i + 1).start()
        else:
            sums[...] = merged
            sums[2:3] = jnp.broadcast_to(jnp.sum(merged[2:3], axis=-1, keepdims=True) / tokens_counted(), (1, width))

    def tokens_counted():
        return sum(counts[j, 0:1, 0:1] for j in range(n_dp))

    for j in range(n_tp):
        hidden_copy(j).start()
    block_copy(0).start()
    for h in range(2):
        rows_copy(h, 0).start()
    more_copy(0).start()
    hidden_copy(0).wait()
    lax.fori_loop(0, PIECES, first_piece, 0)
    lax.fori_loop(0, (n_tp - 1) * PIECES, next_piece, 0)
    counts[dp] = jnp.full(counts.shape[1:], jnp.sum(loss_mask[...].astype(jnp.float32)), jnp.float32)
    pl.semaphore_wait(barrier, n_dp - 1 + 2 * len(others))
    for k in range(PIECES):
        y_copy(k).start()
    for i in range(2):
        ids_copy(i).start()
    for j in range(n_dp - 1):
        count_copy(j).start()

    top[...] = jnp.full_like(top, jnp.finfo(jnp.float32).min)
    total[...] = jnp.zeros_like(total)
    held[...] = jnp.full_like(held, -jnp.inf)
    target[...] = jnp.zeros_like(target)

    def clear(t, carry):
        dx_t[t] = jnp.zeros(dx_t.shape[1:], jnp.float32)
        return carry

    lax.fori_loop(0, own // TILE, clear, 0)
    assert blocks >= 6 + 3 * PIECES
    lax.fori_loop(0, blocks, block, 0)
    fold(held[...], tile_at(own_tiles - 1))

    best = jnp.max(top[...], axis=0, keepdims=True)
    stats[0, tp, 0:1] = best
    stats[0, tp, 1:2] = jnp.sum(total[...] * jnp.exp(top[...] - best), axis=0, keepdims=True)
    for copy in stat_copies():
        copy.start()

    relay_copy(last).wait_recv()
    convert(across, last)
    for i in range(2):
        ids_copy(i).wait()
    for j in range(n_dp - 1):
        count_arrival(j).wait_recv()
    for i in range(batch):
        for side, (rows_of, marks) in enumerate(((labels, loss_mask), (ids.at[0], ids.at[1]))):
            at = slice(side * own + i * seq, side * own + (i + 1) * seq)
            label[:, at] = rows_of[i:i + 1, :] - first_row
            weight[:, at] = marks[i:i + 1, :].astype(jnp.float32)
    scale[...] = weight[...] / tokens_counted()
    for k in range(PIECES):
        for copy in (y_copy(k), beside_copy(k), core_copy(k), relay_copy(k)):
            copy.wait_send()
    for j in range(n_dp - 1):
        count_copy(j).wait_send()
    for other in others:
        stat_arrival(0, other).wait_recv()
    for other in (tp,) + others:
        stat_arrival(1, other).wait_recv()
    for side in range(Y):
        tops = [stats[side, j, 0:1] for j in range(n_tp)]
        best = functools.reduce(jnp.maximum, tops)
        mass = sum(stats[side, j, 1:2] * jnp.exp(tops[j] - best) for j in range(n_tp))
        lse[:, side * own:(side + 1) * own] = best + jnp.log(mass)

    computes = (compute_0, compute_1, compute_2, compute_3, compute_4)
    beats = len(computes)
    start = beats - 2
    done = beats * units - 1
    ticks = start + 2 * (chunks + 2 * (Z - 1))
    assert done + 38 < ticks

    def tick(i, carry):
        u = i // beats
        kind = i % beats
        since = jnp.maximum(i - start, 0)

        @pl.when(i == start)
        def _():
            settle(0)

        @pl.when((i >= start) & (since % 2 == 0))
        def _():
            reduce_phase(since // 2)

        @pl.when((i >= start) & (since % 2 == 1))
        def _():
            spread_phase(since // 2)

        @pl.when((i > start) & (kind == start) & (u < units))
        def _():
            settle(u)

        for j, compute in enumerate(computes):
            pl.when((kind == j) & (u < units))(functools.partial(compute, u))

        events = ((1, dx_start), (5, dx_middle), (22, dx_finish), (24, lambda: level_next(0)), (26, lambda: level_next(1)),
                  (33, lambda: level_next(2)), (37, lambda: level_next(3)), (38, dh_relay))
        for after, event in events:
            pl.when(i == done + after)(event)
        return carry

    lax.fori_loop(0, ticks, tick, 0)
    level_next(4)
    dh_finish()

    for h in range(2):
        p = place[h]
        mine = out.at[pl.ds(y * half + h * (half // 2), half // 2)]
        theirs = out.at[pl.ds((1 - y) * half + h * (half // 2), half // 2)]

        @pl.when(p < Z - 1)
        def _():
            for c in (chunks - 2, chunks - 1):
                reduce_copy(h, c, red.at[h, c % SLOTS]).wait_send()

        @pl.when(p > 0)
        def _():
            pltpu.make_async_copy(mine, mine, bc_send.at[h]).wait()

        pltpu.make_async_copy(mine, mine, mate_send.at[h]).wait()
        pltpu.make_async_copy(theirs, theirs, mate_recv.at[h]).wait()
    for copy in stat_copies():
        copy.wait_send()
    for i in range(2):
        swap_copy(i).wait_send()
    cross_copy().wait_send()
    for i in range(2):
        share_copy(i).wait_send()
    pass_copy().wait_send()
    dh_copy().wait()
    for i in range(len(level_peers)):
        level_copy(i).wait_send()


def head_step(table, hidden, gain, bias, labels, loss_mask, n_dp, n_tp):
    own, width = hidden.shape
    tokens = Y * own
    shard = table.shape[0]
    half = shard // Y
    size = half // (2 * UNITS * PER_UNIT)
    unit = 2 * size * PER_UNIT
    chunks = UNITS * PER_UNIT
    quarter = own // n_tp
    assert size * 2 * chunks == half and size % 8 == 0 and unit % 32 == 0 and quarter == TILE
    assert shard % FORWARD_ROWS == 0
    f32 = jnp.float32
    b16 = jnp.bfloat16
    i32 = jnp.int32
    lanes = 128
    dma = pltpu.SemaphoreType.DMA
    vmem = pl.BlockSpec(memory_space=pltpu.VMEM)
    hbm = pl.BlockSpec(memory_space=pl.ANY)
    flops = 2 * width * (own * shard + half * (2 * tokens + 3 * own))
    return pl.pallas_call(
        functools.partial(head_kernel, n_dp, n_tp),
        out_shape=(
            jax.ShapeDtypeStruct((shard, width), f32),
            jax.ShapeDtypeStruct((half, width), f32),
            jax.ShapeDtypeStruct((own, width), b16),
            jax.ShapeDtypeStruct((8, width), f32)),
        in_specs=[hbm, hbm, vmem, vmem, vmem, vmem],
        out_specs=(hbm, hbm, hbm, vmem),
        scratch_shapes=[
            pltpu.VMEM((tokens, width), b16), pltpu.VMEM((width, tokens), b16),
            pltpu.VMEM((1, tokens), f32), pltpu.VMEM((1, tokens), f32), pltpu.VMEM((1, tokens), f32),
            pltpu.VMEM((1, tokens), i32), pltpu.VMEM((1, tokens), f32),
            pltpu.VMEM((quarter, width), f32), pltpu.VMEM((quarter, lanes), f32), pltpu.VMEM((quarter, width), f32),
            pltpu.VMEM((n_tp, quarter, width), f32), pltpu.VMEM((2, FORWARD_ROWS, width), b16),
            pltpu.VMEM((FORWARD_ROWS, TILE), f32),
            pltpu.VMEM((8, own), f32), pltpu.VMEM((8, own), f32),
            pltpu.VMEM((Y, n_tp, 2, own), f32), pltpu.VMEM((n_dp, 8, lanes), f32),
            pltpu.VMEM((2,) + labels.shape, i32),
            pltpu.VMEM((2, SLOTS, size, width), f32), pltpu.VMEM((2, 2, size, width), f32),
            pltpu.VMEM((unit, tokens), b16),
            pltpu.VMEM((2, unit, width), b16), pltpu.VMEM((2, unit, width), b16),
            pltpu.VMEM((unit, width), f32),
            pltpu.VMEM((n_tp, width, quarter), f32),
            pltpu.VMEM((2, width, quarter), f32), pltpu.VMEM((width, quarter), f32),
            pltpu.VMEM((5, 8, width), f32), pltpu.VMEM((5, 8, width), f32),
            dma((n_tp,)), dma((2,)), dma((2, PIECES)), dma((2, PIECES)), dma((2, PIECES)), dma((2, PIECES)),
            dma((2 * n_tp - 1,)), dma((Y, n_tp)), dma((n_dp - 1,)), dma((n_dp,)),
            dma((2, 2)),
            dma((2, SLOTS)), dma((2, SLOTS)), pltpu.SemaphoreType.REGULAR((2,)),
            dma((2,)), dma((2, chunks)), dma((2,)), dma((2,)),
            dma((2, 2)), dma((2,)), dma((2,)), dma((2, 2)), dma((2,)),
            dma((2, 2)), dma((2,)), dma((3,)), dma((3,)), dma((2, 5)),
        ],
        compiler_params=pltpu.CompilerParams(
            collective_id=0, has_side_effects=True, vmem_limit_bytes=VMEM_BYTES),
        cost_estimate=pl.CostEstimate(flops=flops, bytes_accessed=12 * half * width, transcendentals=half * tokens),
    )(table, hidden, gain, bias, labels, loss_mask)


def place_kernel(table_in, dh_in, sums, table_out, dh_out, loss, gain_out, bias_out, buf, dh_buf, in_sem, out_sem, dh_sem):
    size = buf.shape[1]
    count = table_in.shape[0] // size
    lag = PLACE_SLOTS // 2

    def read(i):
        return pltpu.make_async_copy(table_in.at[pl.ds(i * size, size)], buf.at[i % PLACE_SLOTS], in_sem.at[i % PLACE_SLOTS])

    def write(i):
        return pltpu.make_async_copy(buf.at[i % PLACE_SLOTS], table_out.at[pl.ds(i * size, size)], out_sem.at[i % PLACE_SLOTS])

    dh_read = pltpu.make_async_copy(dh_in, dh_buf, dh_sem.at[0])
    dh_write = pltpu.make_async_copy(dh_buf, dh_out, dh_sem.at[1])
    for i in range(count + lag):
        if i < count:
            if i >= PLACE_SLOTS:
                write(i - PLACE_SLOTS).wait()
            read(i).start()
        if i == 0:
            dh_read.start()
            loss[...] = sums[2:3, 0:1]
            gain_out[...] = sums[0:1, :]
            bias_out[...] = sums[1:2, :]
        if i == lag:
            dh_read.wait()
            dh_write.start()
        if i >= lag:
            read(i - lag).wait()
            write(i - lag).start()
    for i in range(count - PLACE_SLOTS, count):
        write(i).wait()
    dh_write.wait()


def place(table, dh, sums):
    f32 = jnp.float32
    dma = pltpu.SemaphoreType.DMA
    vmem = pl.BlockSpec(memory_space=pltpu.VMEM)
    hbm = pl.BlockSpec(memory_space=pltpu.HBM)
    width = table.shape[1]
    assert table.shape[0] % PLACE_ROWS == 0
    return pl.pallas_call(
        place_kernel,
        out_shape=(
            jax.ShapeDtypeStruct(table.shape, f32), jax.ShapeDtypeStruct(dh.shape, dh.dtype),
            jax.ShapeDtypeStruct((1, 1), f32), jax.ShapeDtypeStruct((1, width), f32), jax.ShapeDtypeStruct((1, width), f32)),
        in_specs=[hbm, hbm, vmem],
        out_specs=(hbm, hbm, vmem, vmem, vmem),
        scratch_shapes=[
            pltpu.VMEM((PLACE_SLOTS, PLACE_ROWS, width), f32), pltpu.VMEM(dh.shape, dh.dtype),
            dma((PLACE_SLOTS,)), dma((PLACE_SLOTS,)), dma((2,))],
        compiler_params=pltpu.CompilerParams(vmem_limit_bytes=VMEM_BYTES),
        cost_estimate=pl.CostEstimate(flops=0, bytes_accessed=8 * table.size + 4 * dh.size, transcendentals=0),
    )(table, dh, sums)


def solution(mesh):
    n_dp = mesh.shape['dp']
    n_tp = mesh.shape['tp']

    def device_step(hidden, table, labels, loss_mask, ln_gain, ln_bias):
        batch, seq, width = hidden.shape
        grad_table, _, grad_hidden, sums = head_step(
            table, hidden.reshape(batch * seq, width), ln_gain, ln_bias, labels, loss_mask, n_dp, n_tp)
        grad_table, grad_hidden, loss, grad_gain, grad_bias = place(grad_table, grad_hidden, sums)
        return (loss.reshape(()), grad_hidden.reshape(batch, seq, width), grad_table,
                grad_gain.reshape(width), grad_bias.reshape(width))

    specs_in = (P('dp', None, None), P('tp', None), P('dp', None), P('dp', None), P(None), P(None))
    specs_out = (P(), P('dp', None, None), P('tp', None), P(None), P(None))
    return jax.shard_map(device_step, mesh=mesh, in_specs=specs_in, out_specs=specs_out, check_vma=False)
```

```python
import functools

import jax
import jax.numpy as jnp
from jax import lax
from jax.experimental import pallas as pl
from jax.experimental.pallas import tpu as pltpu
from jax.sharding import PartitionSpec as P

LN_EPS = 1e-5
VOCAB = 50257
Z = 4
Y = 2
UNITS = 33
PER_UNIT = 3
SLOTS = 16
TILE = 512
PIECES = 4
PARCELS = 8
FORWARD_ROWS = 704
PLACE_ROWS = 528
PLACE_SLOTS = 16
COLUMNS = 256
VMEM_BYTES = 67043328
MESH = pl.DeviceIdType.MESH


def signal(barrier, **where):
    pl.semaphore_signal(barrier, inc=1, device_id=where, device_id_type=MESH)


def remote(src, dst, send_sem, recv_sem, **where):
    return pltpu.make_async_remote_copy(
        src_ref=src, dst_ref=dst, send_sem=send_sem, recv_sem=recv_sem, device_id=where, device_id_type=MESH)


def neighbours(tp):
    core = tp % 2
    partner = tp + 1 - 2 * core
    beside = tp + 2 - 4 * (tp // 2)
    return partner, beside, beside + 1 - 2 * core


def tile_at(t):
    return slice(t * TILE, (t + 1) * TILE)


def aligned(start, size):
    return pl.ds(pl.multiple_of(start, size), size)


def head_kernel(
        n_dp, n_tp, table, hidden, gain, bias, labels, loss_mask,
        out, part, dh, sums,
        x, x_t, lse, scale, weight, label, target, hat, inv, send_q,
        got, block_buf, held, top, total, stats, counts, ids,
        red, loc, q_t, rows_buf, more_buf, stage, dx_t, from_core, from_x, levels, arrived,
        hidden_sem, block_sem, y_sem, beside_sem, core_sem, relay_sem, stat_send, stat_recv, count_send, count_recv,
        ids_sem,
        red_send, red_recv, credit, bc_send, bc_recv, mate_send, mate_recv, loc_sem, own_sem, part_sem, rows_sem, more_sem,
        swap_sem, cross_sem, share_send, share_recv, level_sem):
    own, width = hidden.shape
    tokens = Y * own
    shard = table.shape[0]
    half = shard // Y
    quarter = own // n_tp
    piece = quarter // PIECES
    batch, seq = labels.shape
    size = red.shape[2]
    chunks = half // (2 * size)
    strip = size * PER_UNIT
    units = chunks // PER_UNIT
    unit = 2 * strip
    block_rows = block_buf.shape[1]
    blocks = shard // block_rows
    last = PARCELS - 1
    parcel = quarter // PARCELS
    own_tiles, all_tiles, columns = own // TILE, tokens // TILE, width // COLUMNS

    dp = lax.axis_index('dp')
    tp = lax.axis_index('tp')
    y = dp % Y
    z = dp // Y
    core = tp % 2
    mate = dp + 1 - 2 * y
    partner, beside, across = neighbours(tp)
    others = (partner, beside, across)
    dp_others = [lax.rem(dp + j, n_dp) for j in range(1, n_dp)]
    z_mate = dp + Y - 2 * Y * (z % 2)
    z_far = dp + 2 * Y - 4 * Y * (z // 2)
    place = (Z - 1 - z, z)
    onward = (dp - Y, dp + Y)
    back = (dp + Y, dp - Y)
    first_row = tp * shard

    barrier = pltpu.get_barrier_semaphore()
    for other in dp_others:
        signal(barrier, dp=other)
    for other in others:
        signal(barrier, tp=other)
        signal(barrier, dp=mate, tp=other)

    def hidden_copy(j):
        q = lax.rem(tp + j, n_tp)
        at = aligned(q * quarter, quarter)
        return pltpu.make_async_copy(hidden.at[at], x.at[at], hidden_sem.at[j])

    def block_copy(b):
        return pltpu.make_async_copy(
            table.at[pl.ds(b * block_rows, block_rows)], block_buf.at[b % 2], block_sem.at[b % 2])

    def got_piece(q, k):
        return got.at[q, pl.ds(k * parcel, parcel)]

    def y_copy(k):
        return remote(send_q.at[pl.ds(k * parcel, parcel)], got_piece(tp, k), y_sem.at[0, k], y_sem.at[1, k], dp=mate)

    def beside_copy(k):
        return remote(got_piece(tp, k), got_piece(tp, k), beside_sem.at[0, k], beside_sem.at[1, k], tp=beside)

    def core_copy(k):
        return remote(got_piece(tp, k), got_piece(tp, k), core_sem.at[0, k], core_sem.at[1, k], tp=partner)

    def relay_copy(k):
        return remote(got_piece(beside, k), got_piece(beside, k), relay_sem.at[0, k], relay_sem.at[1, k], tp=partner)

    def count_copy(j):
        return remote(counts.at[dp], counts.at[dp], count_send.at[j], count_recv.at[dp], dp=dp_others[j])

    def count_arrival(j):
        other = dp_others[j]
        return remote(counts.at[other], counts.at[other], count_send.at[j], count_recv.at[other], dp=other)

    def ids_copy(i):
        return remote((labels, loss_mask)[i], ids.at[i], ids_sem.at[0, i], ids_sem.at[1, i], dp=mate)

    def row_of(ref):
        return ref[...].astype(jnp.float32)[None, :]

    def block_of(q, k):
        return aligned(q * quarter + k * piece, piece)

    def normalize(at):
        h = x[at, :].astype(jnp.float32)
        mean = jnp.mean(h, axis=-1, keepdims=True)
        centred = h - mean
        variance = jnp.mean(centred * centred, axis=-1, keepdims=True)
        inv_std = lax.rsqrt(variance + LN_EPS)
        x_hat = centred * inv_std
        normed = (x_hat * row_of(gain) + row_of(bias)).astype(jnp.bfloat16)
        wide = normed.astype(jnp.float32)
        x[at, :] = normed
        x_t[:, at] = wide.T.astype(jnp.bfloat16)
        return x_hat, inv_std, wide

    def first_piece(k, carry):
        x_hat, inv_std, wide = normalize(block_of(tp, k))
        at = aligned(k * piece, piece)
        send_q[at, :] = wide
        hat[at, :] = x_hat
        inv[at, :] = jnp.broadcast_to(inv_std, (piece, inv.shape[1]))
        return carry

    def next_piece(j, carry):
        k = j % PIECES

        @pl.when(k == 0)
        def _():
            hidden_copy(1 + j // PIECES).wait()
        normalize(block_of(lax.rem(tp + 1 + j // PIECES, n_tp), k))
        return carry

    def convert(q, k):
        wide = got[q, aligned(k * piece, piece)]
        at = aligned(own + q * quarter + k * piece, piece)
        x[at, :] = wide.astype(jnp.bfloat16)
        x_t[:, at] = wide.T.astype(jnp.bfloat16)

    def fold(logits, at):
        logits = logits.reshape(block_rows // 8, 8, TILE)
        before = top[:, at]
        now = jnp.maximum(before, jnp.max(logits, axis=0))
        total[:, at] = total[:, at] * jnp.exp(before - now) + jnp.sum(jnp.exp(logits - now[None]), axis=0)
        top[:, at] = now

    def block(b, carry):
        block_copy(b).wait()

        @pl.when(b + 1 < blocks)
        def _():
            block_copy(b + 1).start()

        def paced(first, count):
            d = jnp.maximum(b - first, 0)
            beat = d % 5
            k = 3 * (d // 5) + (beat + 1) // 2
            return (b >= first) & ((beat < 2) | (beat == 3)) & (k < count), jnp.minimum(k, PARCELS - 1)

        due, k_y = paced(3, PARCELS)

        @pl.when(due)
        def _():
            with jax.named_scope('wait_y'):
                y_copy(k_y).wait_recv()
            beside_copy(k_y).start()
            core_copy(k_y).start()
            pl.when(k_y % 2 == 1)(lambda: convert(tp, k_y // 2))

        due, k_core = paced(4, PARCELS)

        @pl.when(due)
        def _():
            with jax.named_scope('wait_core'):
                core_copy(k_core).wait_recv()
            pl.when(k_core % 2 == 1)(lambda: convert(partner, k_core // 2))

        due, k_x = paced(6, PARCELS)

        @pl.when(due)
        def _():
            with jax.named_scope('wait_x'):
                beside_copy(k_x).wait_recv()
            relay_copy(k_x).start()
            pl.when(k_x % 2 == 1)(lambda: convert(beside, k_x // 2))

        due, k_relay = paced(7, PARCELS - 1)

        @pl.when(due)
        def _():
            with jax.named_scope('wait_relay'):
                relay_copy(k_relay).wait_recv()
            pl.when(k_relay % 2 == 1)(lambda: convert(across, k_relay // 2))

        slot = b % 2
        row_ids = first_row + b * block_rows + lax.broadcasted_iota(jnp.int32, (block_rows, 1), 0)
        fold(held[...], tile_at(own_tiles - 1))
        for t in range(own_tiles):
            at = tile_at(t)
            logits = jnp.dot(block_buf[slot], x_t[:, at], preferred_element_type=jnp.float32)
            logits = jnp.where(row_ids < VOCAB, logits, -jnp.inf)
            if t + 1 < own_tiles:
                fold(logits, at)
            else:
                held[...] = logits
        return carry

    def stat_copies():
        where = [{'tp': other} for other in others] + [{'dp': mate}] + [{'dp': mate, 'tp': other} for other in others]
        return [remote(stats.at[0, tp], stats.at[int(i >= n_tp - 1), tp], stat_send.at[i], stat_recv.at[int(i >= n_tp - 1), tp],
                       **w) for i, w in enumerate(where)]

    def stat_arrival(side, other):
        return remote(stats.at[side, other], stats.at[side, other], stat_send.at[0], stat_recv.at[side, other], tp=partner)

    def part_rows(h, c):
        return part.at[pl.ds(h * (half // 2) + c * size, size)]

    def out_rows(side, h, c):
        return out.at[pl.ds(side * half + h * (half // 2) + c * size, size)]

    def fetch(h, c):
        return pltpu.make_async_copy(part_rows(h, c), loc.at[h, c % 2], loc_sem.at[h, c % 2])

    def reduce_copy(h, c, src):
        slot = c % SLOTS
        return remote(src, red.at[h, slot], red_send.at[h, slot], red_recv.at[h, slot], dp=onward[h])

    def spread_copy(h, c):
        return remote(out_rows(y, h, c), out_rows(y, h, c), bc_send.at[h], bc_recv.at[h, c], dp=back[h])

    def mate_copy(h, c):
        return remote(out_rows(y, h, c), out_rows(y, h, c), mate_send.at[h], mate_recv.at[h], dp=mate)

    def own_copy(h, c):
        return pltpu.make_async_copy(red.at[h, c % SLOTS], out_rows(y, h, c), own_sem.at[h])

    def rows_copy(h, u):
        return pltpu.make_async_copy(
            table.at[pl.ds(y * half + h * (half // 2) + u * strip, strip)],
            rows_buf.at[u % 2, pl.ds(h * strip, strip)], rows_sem.at[u % 2, h])

    def more_copy(u):
        return pltpu.make_async_copy(
            table.at[pl.ds((1 - y) * half + u * unit, unit)], more_buf.at[u % 2], more_sem.at[u % 2])

    def part_copy(h, u):
        return pltpu.make_async_copy(
            stage.at[pl.ds(h * strip, strip)], part.at[pl.ds(h * (half // 2) + u * strip, strip)], part_sem.at[h])

    unit_iota = lax.broadcasted_iota(jnp.int32, (unit, 1), 0)

    def grads(table_rows, row_ids, at):
        logits = jnp.dot(table_rows, x_t[:, at], preferred_element_type=jnp.float32)
        hit = row_ids == label[:, at]
        probs = jnp.where(row_ids + first_row < VOCAB, jnp.exp(logits - lse[:, at]), 0.0)
        q = ((probs - jnp.where(hit, 1.0, 0.0)) * scale[:, at]).astype(jnp.bfloat16)
        return q, jnp.where(hit, logits, 0.0)

    def add_dx(table_rows, q, t):
        dx_t[t] = dx_t[t] + lax.dot_general(
            table_rows, q, (((0,), (0,)), ((), ())), preferred_element_type=jnp.float32)

    def main_tile(u, t):
        slot = u % 2
        at = tile_at(t)
        mine = y * half + u * strip + unit_iota
        row_ids = jnp.where(unit_iota < strip, mine, mine + (half // 2 - strip))
        q, hits = grads(rows_buf[slot], row_ids, at)
        q_t[:, at] = q
        target[:, at] = target[:, at] + jnp.sum(hits, axis=0, keepdims=True)
        if t < own // TILE:
            add_dx(rows_buf[slot], q, t)

    def table_tile(n):
        at = slice(n * COLUMNS, (n + 1) * COLUMNS)
        stage[:, at] = jnp.dot(q_t[...], x[:, at], preferred_element_type=jnp.float32)

    def more_tile(u, t):
        theirs = (1 - y) * half + u * unit + unit_iota
        q, _ = grads(more_buf[u % 2], theirs, tile_at(t))
        add_dx(more_buf[u % 2], q, t)

    few = (all_tiles - own_tiles) // 4

    def compute_0(u):
        for h in range(2):
            rows_copy(h, u).wait()

        @pl.when(u + 1 < units)
        def _():
            for h in range(2):
                rows_copy(h, u + 1).start()

        for t in list(range(own_tiles // 2)) + list(range(own_tiles, own_tiles + few)):
            main_tile(u, t)

    def compute_1(u):
        for t in list(range(own_tiles // 2, own_tiles)) + list(range(own_tiles + few, own_tiles + 2 * few)):
            main_tile(u, t)

    def compute_2(u):
        for t in range(own_tiles + 2 * few, all_tiles):
            main_tile(u, t)
        for n in range(columns):
            table_tile(n)
        for h in range(2):
            part_copy(h, u).start()

    def compute_3(u):
        more_copy(u).wait()

        @pl.when(u + 1 < units)
        def _():
            more_copy(u + 1).start()

        for t in range(own_tiles // 2):
            more_tile(u, t)

    def compute_4(u):
        for t in range(own_tiles // 2, own_tiles):
            more_tile(u, t)

    def settle(u):
        for h in range(2):
            part_copy(h, u).wait()

    def send_reduced(h, c, src):
        @pl.when(c >= SLOTS)
        def _():
            pl.semaphore_wait(credit.at[h], 1)
        reduce_copy(h, c, src).start()

    def free_slot(h, c):
        @pl.when(c + SLOTS < chunks)
        def _():
            pl.semaphore_signal(credit.at[h], inc=1, device_id={'dp': back[h]}, device_id_type=MESH)

    def reduce_phase(s):
        for h in range(2):
            p = place[h]
            c = s - p
            here = (c >= 0) & (c < chunks)

            @pl.when(here & (p == 0))
            def _():
                @pl.when(c >= 2)
                def _():
                    reduce_copy(h, c - 2, part_rows(h, c - 2)).wait_send()
                send_reduced(h, c, part_rows(h, c))

            @pl.when(here & (p > 0))
            def _():
                slot = c % SLOTS
                reduce_copy(h, c, red.at[h, slot]).wait_recv()
                fetch(h, c).wait()
                red[h, slot] = red[h, slot] + loc[h, c % 2]

                @pl.when(p < Z - 1)
                def _():
                    @pl.when(c >= 2)
                    def _():
                        reduce_copy(h, c - 2, red.at[h, (c - 2) % SLOTS]).wait_send()
                        free_slot(h, c - 2)
                    send_reduced(h, c, red.at[h, slot])

                @pl.when(p == Z - 1)
                def _():
                    own_copy(h, c).start()

            @pl.when((p > 0) & (c >= -1) & (c + 1 < chunks))
            def _():
                fetch(h, c + 1).start()

    def spread_phase(s):
        for h in range(2):
            p = place[h]
            c = s - 2 * (Z - 1) + p

            @pl.when((c >= 0) & (c < chunks))
            def _():
                @pl.when(p == Z - 1)
                def _():
                    own_copy(h, c).wait()
                    free_slot(h, c)

                @pl.when(p < Z - 1)
                def _():
                    spread_copy(h, c).wait_recv()

                @pl.when(p > 0)
                def _():
                    spread_copy(h, c).start()

                mate_copy(h, c).start()

    def swap_copy(i):
        return remote(dx_t.at[2 * i + 1 - core], from_core.at[i], swap_sem.at[0, i], swap_sem.at[1, i], tp=partner)

    def cross_copy():
        return remote(dx_t.at[beside], from_x, cross_sem.at[0], cross_sem.at[1], tp=beside)

    def share_copy(i):
        return remote(send_q, got.at[tp], share_send.at[i], share_recv.at[i], tp=others[i])

    def pass_copy():
        return remote(got.at[beside], got.at[beside], share_send.at[2], share_recv.at[2], tp=partner)

    def round_dh(q, ref):
        at = aligned(q * quarter, quarter)
        x[at, :] = ref.astype(jnp.bfloat16)

    def dh_relay():
        share_copy(1).wait_recv()
        pass_copy().start()
        round_dh(beside, got[beside])
        share_copy(0).wait_recv()
        round_dh(partner, got[partner])
        round_dh(tp, send_q[...])

    def dh_copy():
        return pltpu.make_async_copy(x.at[pl.ds(0, own)], dh, hidden_sem.at[0])

    def dh_finish():
        pass_copy().wait_recv()
        round_dh(across, got[across])
        dh_copy().start()

    slab = 128

    def add_into(j, ref):
        def body(i, carry):
            at = aligned(i * slab, slab)
            dx_t[j, at] = dx_t[j, at] + ref[at]
            return carry
        lax.fori_loop(0, width // slab, body, 0)

    def dx_start():
        for i in range(2):
            swap_copy(i).start()

    def dx_middle():
        for i in range(2):
            swap_copy(i).wait_recv()
            add_into(2 * i + core, from_core.at[i])
        cross_copy().start()

    def dx_finish():
        cross_copy().wait_recv()
        add_into(tp, from_x)
        for i in range(width // slab):
            at = pl.ds(i * slab, slab)
            send_q[:, at] = dx_t[tp, at].T

        levels[0] = jnp.zeros(levels.shape[1:], jnp.float32)
        own_loss = weight[:, :own] * lse[:, :own] * (1.0 / n_tp) - weight[:, :own] * target[:, :own]
        loss_part = own_loss - weight[:, own:] * target[:, own:]
        levels[0, 2:3] = sum(loss_part[:, i * width:(i + 1) * width] for i in range(own // width))
        step = min(64, quarter)

        def token_block(i, carry):
            at = aligned(i * step, step)
            grad = send_q[at, :]
            x_hat = hat[at, :]
            levels[0, 0:1] = levels[0, 0:1] + jnp.sum(grad * x_hat, axis=0, keepdims=True)
            levels[0, 1:2] = levels[0, 1:2] + jnp.sum(grad, axis=0, keepdims=True)
            grad_hat = grad * row_of(gain)
            mean_grad = jnp.mean(grad_hat, axis=-1, keepdims=True)
            mean_proj = jnp.mean(grad_hat * x_hat, axis=-1, keepdims=True)
            send_q[at, :] = inv[at, 0:1] * (grad_hat - mean_grad - x_hat * mean_proj)
            return carry

        lax.fori_loop(0, quarter // step, token_block, 0)
        level_copy(0).start()
        for i in range(2):
            share_copy(i).start()

    level_peers = ({'tp': beside}, {'tp': partner}, {'dp': mate}, {'dp': z_mate}, {'dp': z_far})

    def level_copy(i):
        return remote(levels.at[i], arrived.at[i], level_sem.at[0, i], level_sem.at[1, i], **level_peers[i])

    def level_next(i):
        level_copy(i).wait_recv()
        merged = levels[i] + arrived[i]
        if i + 1 < len(level_peers):
            levels[i + 1] = merged
            level_copy(i + 1).start()
        else:
            sums[...] = merged
            sums[2:3] = jnp.broadcast_to(jnp.sum(merged[2:3], axis=-1, keepdims=True) / tokens_counted(), (1, width))

    def tokens_counted():
        return sum(counts[j, 0:1, 0:1] for j in range(n_dp))

    for j in range(n_tp):
        hidden_copy(j).start()
    block_copy(0).start()
    for h in range(2):
        rows_copy(h, 0).start()
    more_copy(0).start()
    hidden_copy(0).wait()
    with jax.named_scope('lnfirst'):
        lax.fori_loop(0, PIECES, first_piece, 0)
    with jax.named_scope('lnrest'):
        lax.fori_loop(0, (n_tp - 1) * PIECES, next_piece, 0)
    counts[dp] = jnp.full(counts.shape[1:], jnp.sum(loss_mask[...].astype(jnp.float32)), jnp.float32)
    with jax.named_scope('entry'):
        pl.semaphore_wait(barrier, n_dp - 1 + 2 * len(others))
    for k in range(PARCELS):
        y_copy(k).start()
    for i in range(2):
        ids_copy(i).start()
    for j in range(n_dp - 1):
        count_copy(j).start()

    top[...] = jnp.full_like(top, jnp.finfo(jnp.float32).min)
    total[...] = jnp.zeros_like(total)
    held[...] = jnp.full_like(held, -jnp.inf)
    target[...] = jnp.zeros_like(target)

    def clear(t, carry):
        dx_t[t] = jnp.zeros(dx_t.shape[1:], jnp.float32)
        return carry

    lax.fori_loop(0, own // TILE, clear, 0)
    assert blocks > 6 + 5 * (PARCELS - 1) // 3 and PARCELS == 2 * PIECES
    with jax.named_scope('blocks'):
        lax.fori_loop(0, blocks, block, 0)
    fold(held[...], tile_at(own_tiles - 1))

    best = jnp.max(top[...], axis=0, keepdims=True)
    stats[0, tp, 0:1] = best
    stats[0, tp, 1:2] = jnp.sum(total[...] * jnp.exp(top[...] - best), axis=0, keepdims=True)
    for copy in stat_copies():
        copy.start()

    with jax.named_scope('lastrelay'):
        relay_copy(last).wait_recv()
    convert(across, PIECES - 1)
    for i in range(2):
        ids_copy(i).wait()
    for j in range(n_dp - 1):
        count_arrival(j).wait_recv()
    for i in range(batch):
        for side, (rows_of, marks) in enumerate(((labels, loss_mask), (ids.at[0], ids.at[1]))):
            at = slice(side * own + i * seq, side * own + (i + 1) * seq)
            label[:, at] = rows_of[i:i + 1, :] - first_row
            weight[:, at] = marks[i:i + 1, :].astype(jnp.float32)
    scale[...] = weight[...] / tokens_counted()
    for k in range(PARCELS):
        for copy in (y_copy(k), beside_copy(k), core_copy(k), relay_copy(k)):
            copy.wait_send()
    for j in range(n_dp - 1):
        count_copy(j).wait_send()
    with jax.named_scope('statwait'):
        for other in others:
            stat_arrival(0, other).wait_recv()
        for other in (tp,) + others:
            stat_arrival(1, other).wait_recv()
    for side in range(Y):
        tops = [stats[side, j, 0:1] for j in range(n_tp)]
        best = functools.reduce(jnp.maximum, tops)
        mass = sum(stats[side, j, 1:2] * jnp.exp(tops[j] - best) for j in range(n_tp))
        lse[:, side * own:(side + 1) * own] = best + jnp.log(mass)

    computes = (compute_0, compute_1, compute_2, compute_3, compute_4)
    beats = len(computes)
    start = beats - 2
    done = beats * units - 1
    ticks = start + 2 * (chunks + 2 * (Z - 1))
    assert done + 38 < ticks

    def tick(i, carry):
        u = i // beats
        kind = i % beats
        since = jnp.maximum(i - start, 0)

        @pl.when(i == start)
        def _():
            settle(0)

        @pl.when((i >= start) & (since % 2 == 0))
        def _():
            with jax.named_scope('red'):
                reduce_phase(since // 2)

        @pl.when((i >= start) & (since % 2 == 1))
        def _():
            with jax.named_scope('spread'):
                spread_phase(since // 2)

        @pl.when((i > start) & (kind == start) & (u < units))
        def _():
            settle(u)

        for j, compute in enumerate(computes):
            def scoped(compute=compute, j=j):
                with jax.named_scope(f'calc{j}'):
                    compute(u)
            pl.when((kind == j) & (u < units))(scoped)

        events = ((1, dx_start), (5, dx_middle), (22, dx_finish), (24, lambda: level_next(0)), (26, lambda: level_next(1)),
                  (33, lambda: level_next(2)), (37, lambda: level_next(3)), (38, dh_relay))
        for after, event in events:
            pl.when(i == done + after)(event)
        return carry

    lax.fori_loop(0, ticks, tick, 0)
    with jax.named_scope('finallevel'):
        level_next(4)
    with jax.named_scope('dhfinish'):
        dh_finish()

    for h in range(2):
        p = place[h]
        mine = out.at[pl.ds(y * half + h * (half // 2), half // 2)]
        theirs = out.at[pl.ds((1 - y) * half + h * (half // 2), half // 2)]

        @pl.when(p < Z - 1)
        def _():
            for c in (chunks - 2, chunks - 1):
                reduce_copy(h, c, red.at[h, c % SLOTS]).wait_send()

        @pl.when(p > 0)
        def _():
            pltpu.make_async_copy(mine, mine, bc_send.at[h]).wait()

        with jax.named_scope('matewait'):
            pltpu.make_async_copy(mine, mine, mate_send.at[h]).wait()
            pltpu.make_async_copy(theirs, theirs, mate_recv.at[h]).wait()
    for copy in stat_copies():
        copy.wait_send()
    for i in range(2):
        swap_copy(i).wait_send()
    cross_copy().wait_send()
    for i in range(2):
        share_copy(i).wait_send()
    pass_copy().wait_send()
    dh_copy().wait()
    for i in range(len(level_peers)):
        level_copy(i).wait_send()


def head_step(table, hidden, gain, bias, labels, loss_mask, n_dp, n_tp):
    own, width = hidden.shape
    tokens = Y * own
    shard = table.shape[0]
    half = shard // Y
    size = half // (2 * UNITS * PER_UNIT)
    unit = 2 * size * PER_UNIT
    chunks = UNITS * PER_UNIT
    quarter = own // n_tp
    assert size * 2 * chunks == half and size % 8 == 0 and unit % 32 == 0 and quarter == TILE
    assert shard % FORWARD_ROWS == 0
    f32 = jnp.float32
    b16 = jnp.bfloat16
    i32 = jnp.int32
    lanes = 128
    dma = pltpu.SemaphoreType.DMA
    vmem = pl.BlockSpec(memory_space=pltpu.VMEM)
    hbm = pl.BlockSpec(memory_space=pl.ANY)
    flops = 2 * width * (own * shard + half * (2 * tokens + 3 * own))
    return pl.pallas_call(
        functools.partial(head_kernel, n_dp, n_tp),
        out_shape=(
            jax.ShapeDtypeStruct((shard, width), f32),
            jax.ShapeDtypeStruct((half, width), f32),
            jax.ShapeDtypeStruct((own, width), b16),
            jax.ShapeDtypeStruct((8, width), f32)),
        in_specs=[hbm, hbm, vmem, vmem, vmem, vmem],
        out_specs=(hbm, hbm, hbm, vmem),
        scratch_shapes=[
            pltpu.VMEM((tokens, width), b16), pltpu.VMEM((width, tokens), b16),
            pltpu.VMEM((1, tokens), f32), pltpu.VMEM((1, tokens), f32), pltpu.VMEM((1, tokens), f32),
            pltpu.VMEM((1, tokens), i32), pltpu.VMEM((1, tokens), f32),
            pltpu.VMEM((quarter, width), f32), pltpu.VMEM((quarter, lanes), f32), pltpu.VMEM((quarter, width), f32),
            pltpu.VMEM((n_tp, quarter, width), f32), pltpu.VMEM((2, FORWARD_ROWS, width), b16),
            pltpu.VMEM((FORWARD_ROWS, TILE), f32),
            pltpu.VMEM((8, own), f32), pltpu.VMEM((8, own), f32),
            pltpu.VMEM((Y, n_tp, 2, own), f32), pltpu.VMEM((n_dp, 8, lanes), f32),
            pltpu.VMEM((2,) + labels.shape, i32),
            pltpu.VMEM((2, SLOTS, size, width), f32), pltpu.VMEM((2, 2, size, width), f32),
            pltpu.VMEM((unit, tokens), b16),
            pltpu.VMEM((2, unit, width), b16), pltpu.VMEM((2, unit, width), b16),
            pltpu.VMEM((unit, width), f32),
            pltpu.VMEM((n_tp, width, quarter), f32),
            pltpu.VMEM((2, width, quarter), f32), pltpu.VMEM((width, quarter), f32),
            pltpu.VMEM((5, 8, width), f32), pltpu.VMEM((5, 8, width), f32),
            dma((n_tp,)), dma((2,)), dma((2, PARCELS)), dma((2, PARCELS)), dma((2, PARCELS)), dma((2, PARCELS)),
            dma((2 * n_tp - 1,)), dma((Y, n_tp)), dma((n_dp - 1,)), dma((n_dp,)),
            dma((2, 2)),
            dma((2, SLOTS)), dma((2, SLOTS)), pltpu.SemaphoreType.REGULAR((2,)),
            dma((2,)), dma((2, chunks)), dma((2,)), dma((2,)),
            dma((2, 2)), dma((2,)), dma((2,)), dma((2, 2)), dma((2,)),
            dma((2, 2)), dma((2,)), dma((3,)), dma((3,)), dma((2, 5)),
        ],
        compiler_params=pltpu.CompilerParams(
            collective_id=0, has_side_effects=True, vmem_limit_bytes=VMEM_BYTES),
        cost_estimate=pl.CostEstimate(flops=flops, bytes_accessed=12 * half * width, transcendentals=half * tokens),
    )(table, hidden, gain, bias, labels, loss_mask)


def place_kernel(table_in, dh_in, sums, table_out, dh_out, loss, gain_out, bias_out, buf, dh_buf, in_sem, out_sem, dh_sem):
    size = buf.shape[1]
    count = table_in.shape[0] // size
    lag = PLACE_SLOTS // 2

    def read(i):
        return pltpu.make_async_copy(table_in.at[pl.ds(i * size, size)], buf.at[i % PLACE_SLOTS], in_sem.at[i % PLACE_SLOTS])

    def write(i):
        return pltpu.make_async_copy(buf.at[i % PLACE_SLOTS], table_out.at[pl.ds(i * size, size)], out_sem.at[i % PLACE_SLOTS])

    dh_read = pltpu.make_async_copy(dh_in, dh_buf, dh_sem.at[0])
    dh_write = pltpu.make_async_copy(dh_buf, dh_out, dh_sem.at[1])
    for i in range(count + lag):
        if i < count:
            if i >= PLACE_SLOTS:
                write(i - PLACE_SLOTS).wait()
            read(i).start()
        if i == 0:
            dh_read.start()
            loss[...] = sums[2:3, 0:1]
            gain_out[...] = sums[0:1, :]
            bias_out[...] = sums[1:2, :]
        if i == lag:
            dh_read.wait()
            dh_write.start()
        if i >= lag:
            read(i - lag).wait()
            write(i - lag).start()
    for i in range(count - PLACE_SLOTS, count):
        write(i).wait()
    dh_write.wait()


def place(table, dh, sums):
    f32 = jnp.float32
    dma = pltpu.SemaphoreType.DMA
    vmem = pl.BlockSpec(memory_space=pltpu.VMEM)
    hbm = pl.BlockSpec(memory_space=pltpu.HBM)
    width = table.shape[1]
    assert table.shape[0] % PLACE_ROWS == 0
    return pl.pallas_call(
        place_kernel,
        out_shape=(
            jax.ShapeDtypeStruct(table.shape, f32), jax.ShapeDtypeStruct(dh.shape, dh.dtype),
            jax.ShapeDtypeStruct((1, 1), f32), jax.ShapeDtypeStruct((1, width), f32), jax.ShapeDtypeStruct((1, width), f32)),
        in_specs=[hbm, hbm, vmem],
        out_specs=(hbm, hbm, vmem, vmem, vmem),
        scratch_shapes=[
            pltpu.VMEM((PLACE_SLOTS, PLACE_ROWS, width), f32), pltpu.VMEM(dh.shape, dh.dtype),
            dma((PLACE_SLOTS,)), dma((PLACE_SLOTS,)), dma((2,))],
        compiler_params=pltpu.CompilerParams(vmem_limit_bytes=VMEM_BYTES),
        cost_estimate=pl.CostEstimate(flops=0, bytes_accessed=8 * table.size + 4 * dh.size, transcendentals=0),
    )(table, dh, sums)


def solution(mesh):
    n_dp = mesh.shape['dp']
    n_tp = mesh.shape['tp']

    def device_step(hidden, table, labels, loss_mask, ln_gain, ln_bias):
        batch, seq, width = hidden.shape
        grad_table, _, grad_hidden, sums = head_step(
            table, hidden.reshape(batch * seq, width), ln_gain, ln_bias, labels, loss_mask, n_dp, n_tp)
        grad_table, grad_hidden, loss, grad_gain, grad_bias = place(grad_table, grad_hidden, sums)
        return (loss.reshape(()), grad_hidden.reshape(batch, seq, width), grad_table,
                grad_gain.reshape(width), grad_bias.reshape(width))

    specs_in = (P('dp', None, None), P('tp', None), P('dp', None), P('dp', None), P(None), P(None))
    specs_out = (P(), P('dp', None, None), P('tp', None), P(None), P(None))
    return jax.shard_map(device_step, mesh=mesh, in_specs=specs_in, out_specs=specs_out, check_vma=False)
```

```python
import functools

import jax
import jax.numpy as jnp
from jax import lax
from jax.experimental import pallas as pl
from jax.experimental.pallas import tpu as pltpu
from jax.sharding import PartitionSpec as P

LN_EPS = 1e-5
VOCAB = 50257
Z = 4
Y = 2
UNITS = 33
PER_UNIT = 6
SLOTS = 16
RING = 4
END_LAG = 6
TILE = 512
PIECES = 4
FORWARD_ROWS = 704
PLACE_ROWS = 528
PLACE_SLOTS = 16
COLUMNS = 256
VMEM_BYTES = 67043328
MESH = pl.DeviceIdType.MESH


def signal(barrier, **where):
    pl.semaphore_signal(barrier, inc=1, device_id=where, device_id_type=MESH)


def remote(src, dst, send_sem, recv_sem, **where):
    return pltpu.make_async_remote_copy(
        src_ref=src, dst_ref=dst, send_sem=send_sem, recv_sem=recv_sem, device_id=where, device_id_type=MESH)


def neighbours(tp):
    core = tp % 2
    partner = tp + 1 - 2 * core
    beside = tp + 2 - 4 * (tp // 2)
    return partner, beside, beside + 1 - 2 * core


def tile_at(t):
    return slice(t * TILE, (t + 1) * TILE)


def aligned(start, size):
    return pl.ds(pl.multiple_of(start, size), size)


def head_kernel(
        n_dp, n_tp, table, hidden, gain, bias, labels, loss_mask,
        out, part, dh, sums,
        x, x_t, lse, scale, weight, label, target, hat, inv, send_q,
        got, block_buf, held, top, total, stats, counts, ids,
        red, met, loc, q_t, rows_buf, more_buf, stage, dx_t, from_core, from_x, levels, arrived,
        hidden_sem, block_sem, y_sem, beside_sem, core_sem, relay_sem, stat_send, stat_recv, count_send, count_recv,
        ids_sem,
        up_send, up_recv, meet_send, meet_recv, down_send, down_recv, mate_send, mate_recv, credit,
        loc_sem, own_sem, part_sem, rows_sem, more_sem,
        swap_sem, cross_sem, share_send, share_recv, level_sem):
    own, width = hidden.shape
    tokens = Y * own
    shard = table.shape[0]
    half = shard // Y
    quarter = own // n_tp
    piece = quarter // PIECES
    batch, seq = labels.shape
    size = red.shape[1]
    chunks = half // size
    unit = size * PER_UNIT
    units = chunks // PER_UNIT
    block_rows = block_buf.shape[1]
    blocks = shard // block_rows
    last = PIECES - 1
    own_tiles, all_tiles, columns = own // TILE, tokens // TILE, width // COLUMNS

    dp = lax.axis_index('dp')
    tp = lax.axis_index('tp')
    y = dp % Y
    z = dp // Y
    core = tp % 2
    mate = dp + 1 - 2 * y
    partner, beside, across = neighbours(tp)
    others = (partner, beside, across)
    dp_others = [lax.rem(dp + j, n_dp) for j in range(1, n_dp)]
    z_mate = dp + Y - 2 * Y * (z % 2)
    z_far = dp + 2 * Y - 4 * Y * (z // 2)
    inner = (z == 1) | (z == 2)
    z_cross = dp + Y * (Z - 1 - 2 * z)
    first_row = tp * shard

    barrier = pltpu.get_barrier_semaphore()
    for other in dp_others:
        signal(barrier, dp=other)
    for other in others:
        signal(barrier, tp=other)
        signal(barrier, dp=mate, tp=other)

    def hidden_copy(j):
        q = lax.rem(tp + j, n_tp)
        at = aligned(q * quarter, quarter)
        return pltpu.make_async_copy(hidden.at[at], x.at[at], hidden_sem.at[j])

    def block_copy(b):
        return pltpu.make_async_copy(
            table.at[pl.ds(b * block_rows, block_rows)], block_buf.at[b % 2], block_sem.at[b % 2])

    def got_piece(q, k):
        return got.at[q, pl.ds(k * piece, piece)]

    def y_copy(k):
        return remote(send_q.at[pl.ds(k * piece, piece)], got_piece(tp, k), y_sem.at[0, k], y_sem.at[1, k], dp=mate)

    def beside_copy(k):
        return remote(got_piece(tp, k), got_piece(tp, k), beside_sem.at[0, k], beside_sem.at[1, k], tp=beside)

    def core_copy(k):
        return remote(got_piece(tp, k), got_piece(tp, k), core_sem.at[0, k], core_sem.at[1, k], tp=partner)

    def relay_copy(k):
        return remote(got_piece(beside, k), got_piece(beside, k), relay_sem.at[0, k], relay_sem.at[1, k], tp=partner)

    def count_copy(j):
        return remote(counts.at[dp], counts.at[dp], count_send.at[j], count_recv.at[dp], dp=dp_others[j])

    def count_arrival(j):
        other = dp_others[j]
        return remote(counts.at[other], counts.at[other], count_send.at[j], count_recv.at[other], dp=other)

    def ids_copy(i):
        return remote((labels, loss_mask)[i], ids.at[i], ids_sem.at[0, i], ids_sem.at[1, i], dp=mate)

    def row_of(ref):
        return ref[...].astype(jnp.float32)[None, :]

    def block_of(q, k):
        return aligned(q * quarter + k * piece, piece)

    def normalize(at):
        h = x[at, :].astype(jnp.float32)
        mean = jnp.mean(h, axis=-1, keepdims=True)
        centred = h - mean
        variance = jnp.mean(centred * centred, axis=-1, keepdims=True)
        inv_std = lax.rsqrt(variance + LN_EPS)
        x_hat = centred * inv_std
        normed = (x_hat * row_of(gain) + row_of(bias)).astype(jnp.bfloat16)
        wide = normed.astype(jnp.float32)
        x[at, :] = normed
        x_t[:, at] = wide.T.astype(jnp.bfloat16)
        return x_hat, inv_std, wide

    def first_piece(k, carry):
        x_hat, inv_std, wide = normalize(block_of(tp, k))
        at = aligned(k * piece, piece)
        send_q[at, :] = wide
        hat[at, :] = x_hat
        inv[at, :] = jnp.broadcast_to(inv_std, (piece, inv.shape[1]))
        return carry

    def next_piece(j, carry):
        k = j % PIECES

        @pl.when(k == 0)
        def _():
            hidden_copy(1 + j // PIECES).wait()
        normalize(block_of(lax.rem(tp + 1 + j // PIECES, n_tp), k))
        return carry

    def convert(q, k):
        wide = got[q, aligned(k * piece, piece)]
        at = aligned(own + q * quarter + k * piece, piece)
        x[at, :] = wide.astype(jnp.bfloat16)
        x_t[:, at] = wide.T.astype(jnp.bfloat16)

    def fold(logits, at):
        logits = logits.reshape(block_rows // 8, 8, TILE)
        before = top[:, at]
        now = jnp.maximum(before, jnp.max(logits, axis=0))
        total[:, at] = total[:, at] * jnp.exp(before - now) + jnp.sum(jnp.exp(logits - now[None]), axis=0)
        top[:, at] = now

    def block(b, carry):
        block_copy(b).wait()

        @pl.when(b + 1 < blocks)
        def _():
            block_copy(b + 1).start()

        def every_third(first, count):
            d = b - first
            return (d >= 0) & (d < 3 * count) & (jnp.maximum(d, 0) % 3 == 0), jnp.maximum(d, 0) // 3

        due, k_y = every_third(4, PIECES)

        @pl.when(due)
        def _():
            y_copy(k_y).wait_recv()
            beside_copy(k_y).start()
            core_copy(k_y).start()
            convert(tp, k_y)

        due, k_core = every_third(5, PIECES)

        @pl.when(due)
        def _():
            core_copy(k_core).wait_recv()
            convert(partner, k_core)

        due, k_x = every_third(8, PIECES)

        @pl.when(due)
        def _():
            beside_copy(k_x).wait_recv()
            relay_copy(k_x).start()
            convert(beside, k_x)

        due, k_relay = every_third(9, PIECES - 1)

        @pl.when(due)
        def _():
            relay_copy(k_relay).wait_recv()
            convert(across, k_relay)

        slot = b % 2
        row_ids = first_row + b * block_rows + lax.broadcasted_iota(jnp.int32, (block_rows, 1), 0)
        fold(held[...], tile_at(own_tiles - 1))
        for t in range(own_tiles):
            at = tile_at(t)
            logits = jnp.dot(block_buf[slot], x_t[:, at], preferred_element_type=jnp.float32)
            logits = jnp.where(row_ids < VOCAB, logits, -jnp.inf)
            if t + 1 < own_tiles:
                fold(logits, at)
            else:
                held[...] = logits
        return carry

    def stat_copies():
        where = [{'tp': other} for other in others] + [{'dp': mate}] + [{'dp': mate, 'tp': other} for other in others]
        return [remote(stats.at[0, tp], stats.at[int(i >= n_tp - 1), tp], stat_send.at[i], stat_recv.at[int(i >= n_tp - 1), tp],
                       **w) for i, w in enumerate(where)]

    def stat_arrival(side, other):
        return remote(stats.at[side, other], stats.at[side, other], stat_send.at[0], stat_recv.at[side, other], tp=partner)

    def part_rows(c):
        return part.at[pl.ds(c * size, size)]

    def out_rows(side, c):
        return out.at[pl.ds(side * half + c * size, size)]

    def fetch(c):
        return pltpu.make_async_copy(part_rows(c), loc.at[c % 2], loc_sem.at[c % 2])

    def up_copy(c):
        return remote(part_rows(c), red.at[c % SLOTS], up_send.at[c % RING], up_recv.at[c % SLOTS], dp=z_mate)

    def meet_copy(c):
        return remote(red.at[c % SLOTS], met.at[c % SLOTS], meet_send.at[c % RING], meet_recv.at[c % SLOTS], dp=z_cross)

    def down_copy(c):
        return remote(met.at[c % SLOTS], out_rows(y, c), down_send.at[c % RING], down_recv.at[c % SLOTS], dp=z_mate)

    def mate_copy(c, src):
        return remote(src, out_rows(y, c), mate_send.at[c % RING], mate_recv.at[c // (chunks // 2)], dp=mate)

    def own_copy(c):
        return pltpu.make_async_copy(met.at[c % SLOTS], out_rows(y, c), own_sem.at[c % RING])

    def rows_copy(u):
        return pltpu.make_async_copy(table.at[pl.ds(y * half + u * unit, unit)], rows_buf.at[u % 2], rows_sem.at[u % 2])

    def more_copy(u):
        return pltpu.make_async_copy(
            table.at[pl.ds((1 - y) * half + u * unit, unit)], more_buf.at[u % 2], more_sem.at[u % 2])

    def part_copy(u):
        return pltpu.make_async_copy(stage, part.at[pl.ds(u * unit, unit)], part_sem.at[0])

    unit_iota = lax.broadcasted_iota(jnp.int32, (unit, 1), 0)

    def grads(table_rows, row_ids, at):
        logits = jnp.dot(table_rows, x_t[:, at], preferred_element_type=jnp.float32)
        hit = row_ids == label[:, at]
        probs = jnp.where(row_ids + first_row < VOCAB, jnp.exp(logits - lse[:, at]), 0.0)
        q = ((probs - jnp.where(hit, 1.0, 0.0)) * scale[:, at]).astype(jnp.bfloat16)
        return q, jnp.where(hit, logits, 0.0)

    def add_dx(table_rows, q, t):
        dx_t[t] = dx_t[t] + lax.dot_general(
            table_rows, q, (((0,), (0,)), ((), ())), preferred_element_type=jnp.float32)

    def main_tile(u, t):
        slot = u % 2
        at = tile_at(t)
        row_ids = y * half + u * unit + unit_iota
        q, hits = grads(rows_buf[slot], row_ids, at)
        q_t[:, at] = q
        target[:, at] = target[:, at] + jnp.sum(hits, axis=0, keepdims=True)
        if t < own // TILE:
            add_dx(rows_buf[slot], q, t)

    def table_tile(n):
        at = slice(n * COLUMNS, (n + 1) * COLUMNS)
        stage[:, at] = jnp.dot(q_t[...], x[:, at], preferred_element_type=jnp.float32)

    def more_tile(u, t):
        theirs = (1 - y) * half + u * unit + unit_iota
        q, _ = grads(more_buf[u % 2], theirs, tile_at(t))
        add_dx(more_buf[u % 2], q, t)

    few = (all_tiles - own_tiles) // 4

    def compute_0(u):
        rows_copy(u).wait()

        @pl.when(u + 1 < units)
        def _():
            rows_copy(u + 1).start()

        for t in list(range(own_tiles // 2)) + list(range(own_tiles, own_tiles + few)):
            main_tile(u, t)

    def compute_1(u):
        for t in list(range(own_tiles // 2, own_tiles)) + list(range(own_tiles + few, own_tiles + 2 * few)):
            main_tile(u, t)

    def compute_2(u):
        for t in range(own_tiles + 2 * few, all_tiles):
            main_tile(u, t)
        for n in range(columns):
            table_tile(n)
        part_copy(u).start()

    def compute_3(u):
        more_copy(u).wait()

        @pl.when(u + 1 < units)
        def _():
            more_copy(u + 1).start()

        for t in range(own_tiles // 2):
            more_tile(u, t)

    def compute_4(u):
        for t in range(own_tiles // 2, own_tiles):
            more_tile(u, t)

    def settle(u):
        part_copy(u).wait()

    def within(c):
        return (c >= 0) & (c < chunks)

    def take_credit(i, c):
        @pl.when(c >= SLOTS)
        def _():
            pl.semaphore_wait(credit.at[i], 1)

    def give_credit(i, c, other):
        @pl.when(c + SLOTS < chunks)
        def _():
            pl.semaphore_signal(credit.at[i], inc=1, device_id={'dp': other}, device_id_type=MESH)

    def end_step(t):
        @pl.when(t < chunks)
        def _():
            @pl.when(t >= 2)
            def _():
                up_copy(t - 2).wait_send()
            take_credit(0, t)
            up_copy(t).start()

        c = t - END_LAG

        @pl.when(within(c))
        def _():
            down_copy(c).wait_recv()

            @pl.when(c >= RING)
            def _():
                mate_copy(c - RING, out_rows(y, c - RING)).wait_send()
            mate_copy(c, out_rows(y, c)).start()

    def inner_step(t):
        c = t - 2

        @pl.when(within(c))
        def _():
            slot = c % SLOTS
            up_copy(c).wait_recv()
            fetch(c).wait()
            red[slot] = red[slot] + loc[c % 2]
            take_credit(1, c)
            meet_copy(c).start()

        @pl.when(within(c + 1))
        def _():
            fetch(c + 1).start()

        c_met = t - 4

        @pl.when(within(c_met))
        def _():
            slot = c_met % SLOTS
            meet_copy(c_met).wait_recv()
            met[slot] = red[slot] + met[slot]
            down_copy(c_met).start()
            mate_copy(c_met, met.at[slot]).start()
            own_copy(c_met).start()
            meet_copy(c_met).wait_send()
            give_credit(0, c_met, z_mate)

        c_gone = t - 6

        @pl.when(within(c_gone))
        def _():
            own_copy(c_gone).wait()
            down_copy(c_gone).wait_send()
            mate_copy(c_gone, met.at[c_gone % SLOTS]).wait_send()
            give_credit(1, c_gone, z_cross)

    def swap_copy(i):
        return remote(dx_t.at[2 * i + 1 - core], from_core.at[i], swap_sem.at[0, i], swap_sem.at[1, i], tp=partner)

    def cross_copy():
        return remote(dx_t.at[beside], from_x, cross_sem.at[0], cross_sem.at[1], tp=beside)

    def share_copy(i):
        return remote(send_q, got.at[tp], share_send.at[i], share_recv.at[i], tp=others[i])

    def pass_copy():
        return remote(got.at[beside], got.at[beside], share_send.at[2], share_recv.at[2], tp=partner)

    def round_dh(q, ref):
        at = aligned(q * quarter, quarter)
        x[at, :] = ref.astype(jnp.bfloat16)

    def dh_relay():
        share_copy(1).wait_recv()
        pass_copy().start()
        round_dh(beside, got[beside])
        share_copy(0).wait_recv()
        round_dh(partner, got[partner])
        round_dh(tp, send_q[...])

    def dh_copy():
        return pltpu.make_async_copy(x.at[pl.ds(0, own)], dh, hidden_sem.at[0])

    def dh_finish():
        pass_copy().wait_recv()
        round_dh(across, got[across])
        dh_copy().start()

    slab = 128

    def add_into(j, ref):
        def body(i, carry):
            at = aligned(i * slab, slab)
            dx_t[j, at] = dx_t[j, at] + ref[at]
            return carry
        lax.fori_loop(0, width // slab, body, 0)

    def dx_start():
        for i in range(2):
            swap_copy(i).start()

    def dx_middle():
        for i in range(2):
            swap_copy(i).wait_recv()
            add_into(2 * i + core, from_core.at[i])
        cross_copy().start()

    def dx_finish():
        cross_copy().wait_recv()
        add_into(tp, from_x)
        for i in range(width // slab):
            at = pl.ds(i * slab, slab)
            send_q[:, at] = dx_t[tp, at].T

        levels[0] = jnp.zeros(levels.shape[1:], jnp.float32)
        own_loss = weight[:, :own] * lse[:, :own] * (1.0 / n_tp) - weight[:, :own] * target[:, :own]
        loss_part = own_loss - weight[:, own:] * target[:, own:]
        levels[0, 2:3] = sum(loss_part[:, i * width:(i + 1) * width] for i in range(own // width))
        step = min(64, quarter)

        def token_block(i, carry):
            at = aligned(i * step, step)
            grad = send_q[at, :]
            x_hat = hat[at, :]
            levels[0, 0:1] = levels[0, 0:1] + jnp.sum(grad * x_hat, axis=0, keepdims=True)
            levels[0, 1:2] = levels[0, 1:2] + jnp.sum(grad, axis=0, keepdims=True)
            grad_hat = grad * row_of(gain)
            mean_grad = jnp.mean(grad_hat, axis=-1, keepdims=True)
            mean_proj = jnp.mean(grad_hat * x_hat, axis=-1, keepdims=True)
            send_q[at, :] = inv[at, 0:1] * (grad_hat - mean_grad - x_hat * mean_proj)
            return carry

        lax.fori_loop(0, quarter // step, token_block, 0)
        level_copy(0).start()
        for i in range(2):
            share_copy(i).start()

    level_peers = ({'tp': beside}, {'tp': partner}, {'dp': mate}, {'dp': z_mate}, {'dp': z_far})

    def level_copy(i):
        return remote(levels.at[i], arrived.at[i], level_sem.at[0, i], level_sem.at[1, i], **level_peers[i])

    def level_next(i):
        level_copy(i).wait_recv()
        merged = levels[i] + arrived[i]
        if i + 1 < len(level_peers):
            levels[i + 1] = merged
            level_copy(i + 1).start()
        else:
            sums[...] = merged
            sums[2:3] = jnp.broadcast_to(jnp.sum(merged[2:3], axis=-1, keepdims=True) / tokens_counted(), (1, width))

    def tokens_counted():
        return sum(counts[j, 0:1, 0:1] for j in range(n_dp))

    for j in range(n_tp):
        hidden_copy(j).start()
    block_copy(0).start()
    rows_copy(0).start()
    more_copy(0).start()
    hidden_copy(0).wait()
    lax.fori_loop(0, PIECES, first_piece, 0)
    with jax.named_scope('lnrest'):
        lax.fori_loop(0, (n_tp - 1) * PIECES, next_piece, 0)
    counts[dp] = jnp.full(counts.shape[1:], jnp.sum(loss_mask[...].astype(jnp.float32)), jnp.float32)
    pl.semaphore_wait(barrier, n_dp - 1 + 2 * len(others))
    for k in range(PIECES):
        y_copy(k).start()
    for i in range(2):
        ids_copy(i).start()
    for j in range(n_dp - 1):
        count_copy(j).start()

    top[...] = jnp.full_like(top, jnp.finfo(jnp.float32).min)
    total[...] = jnp.zeros_like(total)
    held[...] = jnp.full_like(held, -jnp.inf)
    target[...] = jnp.zeros_like(target)

    def clear(t, carry):
        dx_t[t] = jnp.zeros(dx_t.shape[1:], jnp.float32)
        return carry

    lax.fori_loop(0, own // TILE, clear, 0)
    assert blocks >= 6 + 3 * PIECES
    with jax.named_scope('blocks'):
        lax.fori_loop(0, blocks, block, 0)
    fold(held[...], tile_at(own_tiles - 1))

    best = jnp.max(top[...], axis=0, keepdims=True)
    stats[0, tp, 0:1] = best
    stats[0, tp, 1:2] = jnp.sum(total[...] * jnp.exp(top[...] - best), axis=0, keepdims=True)
    for copy in stat_copies():
        copy.start()

    with jax.named_scope('lastrelay'):
        relay_copy(last).wait_recv()
    convert(across, last)
    for i in range(2):
        ids_copy(i).wait()
    for j in range(n_dp - 1):
        count_arrival(j).wait_recv()
    for i in range(batch):
        for side, (rows_of, marks) in enumerate(((labels, loss_mask), (ids.at[0], ids.at[1]))):
            at = slice(side * own + i * seq, side * own + (i + 1) * seq)
            label[:, at] = rows_of[i:i + 1, :] - first_row
            weight[:, at] = marks[i:i + 1, :].astype(jnp.float32)
    scale[...] = weight[...] / tokens_counted()
    for k in range(PIECES):
        for copy in (y_copy(k), beside_copy(k), core_copy(k), relay_copy(k)):
            copy.wait_send()
    for j in range(n_dp - 1):
        count_copy(j).wait_send()
    with jax.named_scope('statwait'):
        for other in others:
            stat_arrival(0, other).wait_recv()
        for other in (tp,) + others:
            stat_arrival(1, other).wait_recv()
    for side in range(Y):
        tops = [stats[side, j, 0:1] for j in range(n_tp)]
        best = functools.reduce(jnp.maximum, tops)
        mass = sum(stats[side, j, 1:2] * jnp.exp(tops[j] - best) for j in range(n_tp))
        lse[:, side * own:(side + 1) * own] = best + jnp.log(mass)

    computes = (compute_0, compute_1, compute_2, compute_3, compute_4)
    beats = len(computes)
    start = beats - 2
    done = beats * units - 1
    ticks = start + chunks + END_LAG
    assert done + 38 < ticks

    def tick(i, carry):
        u = i // beats
        kind = i % beats

        @pl.when(i == start)
        def _():
            settle(0)

        @pl.when((i >= start) & jnp.logical_not(inner))
        def _():
            with jax.named_scope('red'):
                end_step(jnp.maximum(i - start, 0))

        @pl.when((i >= start) & inner)
        def _():
            with jax.named_scope('red'):
                inner_step(jnp.maximum(i - start, 0))

        @pl.when((i > start) & (kind == start) & (u < units))
        def _():
            settle(u)

        for j, compute in enumerate(computes):
            def scoped(compute=compute, j=j):
                with jax.named_scope(f'calc{j}'):
                    compute(u)
            pl.when((kind == j) & (u < units))(scoped)

        events = ((1, dx_start), (5, dx_middle), (22, dx_finish), (24, lambda: level_next(0)), (26, lambda: level_next(1)),
                  (31, lambda: level_next(2)), (36, lambda: level_next(3)), (38, dh_relay))
        for after, event in events:
            def noted(event=event, after=after):
                with jax.named_scope(f'event{after}'):
                    event()
            pl.when(i == done + after)(noted)
        return carry

    lax.fori_loop(0, ticks, tick, 0)
    with jax.named_scope('finallevel'):
        level_next(4)
    with jax.named_scope('dhfinish'):
        dh_finish()

    @pl.when(jnp.logical_not(inner))
    def _():
        for c in range(chunks - 2, chunks):
            up_copy(c).wait_send()
        for c in range(chunks - RING, chunks):
            mate_copy(c, out_rows(y, c)).wait_send()

    for i in range(2):
        theirs = out.at[pl.ds((1 - y) * half + i * (half // 2), half // 2)]
        with jax.named_scope('matewait'):
            pltpu.make_async_copy(theirs, theirs, mate_recv.at[i]).wait()
    for copy in stat_copies():
        copy.wait_send()
    for i in range(2):
        swap_copy(i).wait_send()
    cross_copy().wait_send()
    for i in range(2):
        share_copy(i).wait_send()
    pass_copy().wait_send()
    dh_copy().wait()
    for i in range(len(level_peers)):
        level_copy(i).wait_send()


def head_step(table, hidden, gain, bias, labels, loss_mask, n_dp, n_tp):
    own, width = hidden.shape
    tokens = Y * own
    shard = table.shape[0]
    half = shard // Y
    size = half // (UNITS * PER_UNIT)
    unit = size * PER_UNIT
    quarter = own // n_tp
    assert unit * UNITS == half and size % 8 == 0 and unit % 32 == 0 and quarter == TILE
    assert shard % FORWARD_ROWS == 0
    f32 = jnp.float32
    b16 = jnp.bfloat16
    i32 = jnp.int32
    lanes = 128
    dma = pltpu.SemaphoreType.DMA
    vmem = pl.BlockSpec(memory_space=pltpu.VMEM)
    hbm = pl.BlockSpec(memory_space=pl.ANY)
    flops = 2 * width * (own * shard + half * (2 * tokens + 3 * own))
    return pl.pallas_call(
        functools.partial(head_kernel, n_dp, n_tp),
        out_shape=(
            jax.ShapeDtypeStruct((shard, width), f32),
            jax.ShapeDtypeStruct((half, width), f32),
            jax.ShapeDtypeStruct((own, width), b16),
            jax.ShapeDtypeStruct((8, width), f32)),
        in_specs=[hbm, hbm, vmem, vmem, vmem, vmem],
        out_specs=(hbm, hbm, hbm, vmem),
        scratch_shapes=[
            pltpu.VMEM((tokens, width), b16), pltpu.VMEM((width, tokens), b16),
            pltpu.VMEM((1, tokens), f32), pltpu.VMEM((1, tokens), f32), pltpu.VMEM((1, tokens), f32),
            pltpu.VMEM((1, tokens), i32), pltpu.VMEM((1, tokens), f32),
            pltpu.VMEM((quarter, width), f32), pltpu.VMEM((quarter, lanes), f32), pltpu.VMEM((quarter, width), f32),
            pltpu.VMEM((n_tp, quarter, width), f32), pltpu.VMEM((2, FORWARD_ROWS, width), b16),
            pltpu.VMEM((FORWARD_ROWS, TILE), f32),
            pltpu.VMEM((8, own), f32), pltpu.VMEM((8, own), f32),
            pltpu.VMEM((Y, n_tp, 2, own), f32), pltpu.VMEM((n_dp, 8, lanes), f32),
            pltpu.VMEM((2,) + labels.shape, i32),
            pltpu.VMEM((SLOTS, size, width), f32), pltpu.VMEM((SLOTS, size, width), f32), pltpu.VMEM((2, size, width), f32),
            pltpu.VMEM((unit, tokens), b16),
            pltpu.VMEM((2, unit, width), b16), pltpu.VMEM((2, unit, width), b16),
            pltpu.VMEM((unit, width), f32),
            pltpu.VMEM((n_tp, width, quarter), f32),
            pltpu.VMEM((2, width, quarter), f32), pltpu.VMEM((width, quarter), f32),
            pltpu.VMEM((5, 8, width), f32), pltpu.VMEM((5, 8, width), f32),
            dma((n_tp,)), dma((2,)), dma((2, PIECES)), dma((2, PIECES)), dma((2, PIECES)), dma((2, PIECES)),
            dma((2 * n_tp - 1,)), dma((Y, n_tp)), dma((n_dp - 1,)), dma((n_dp,)),
            dma((2, 2)),
            dma((RING,)), dma((SLOTS,)), dma((RING,)), dma((SLOTS,)), dma((RING,)), dma((SLOTS,)), dma((RING,)), dma((2,)),
            pltpu.SemaphoreType.REGULAR((2,)),
            dma((2,)), dma((RING,)), dma((1,)), dma((2,)), dma((2,)),
            dma((2, 2)), dma((2,)), dma((3,)), dma((3,)), dma((2, 5)),
        ],
        compiler_params=pltpu.CompilerParams(
            collective_id=0, has_side_effects=True, vmem_limit_bytes=VMEM_BYTES),
        cost_estimate=pl.CostEstimate(flops=flops, bytes_accessed=12 * half * width, transcendentals=half * tokens),
    )(table, hidden, gain, bias, labels, loss_mask)


def place_kernel(table_in, dh_in, sums, table_out, dh_out, loss, gain_out, bias_out, buf, dh_buf, in_sem, out_sem, dh_sem):
    size = buf.shape[1]
    count = table_in.shape[0] // size
    lag = PLACE_SLOTS // 2

    def read(i):
        return pltpu.make_async_copy(table_in.at[pl.ds(i * size, size)], buf.at[i % PLACE_SLOTS], in_sem.at[i % PLACE_SLOTS])

    def write(i):
        return pltpu.make_async_copy(buf.at[i % PLACE_SLOTS], table_out.at[pl.ds(i * size, size)], out_sem.at[i % PLACE_SLOTS])

    dh_read = pltpu.make_async_copy(dh_in, dh_buf, dh_sem.at[0])
    dh_write = pltpu.make_async_copy(dh_buf, dh_out, dh_sem.at[1])
    for i in range(count + lag):
        if i < count:
            if i >= PLACE_SLOTS:
                write(i - PLACE_SLOTS).wait()
            read(i).start()
        if i == 0:
            dh_read.start()
            loss[...] = sums[2:3, 0:1]
            gain_out[...] = sums[0:1, :]
            bias_out[...] = sums[1:2, :]
        if i == lag:
            dh_read.wait()
            dh_write.start()
        if i >= lag:
            read(i - lag).wait()
            write(i - lag).start()
    for i in range(count - PLACE_SLOTS, count):
        write(i).wait()
    dh_write.wait()


def place(table, dh, sums):
    f32 = jnp.float32
    dma = pltpu.SemaphoreType.DMA
    vmem = pl.BlockSpec(memory_space=pltpu.VMEM)
    hbm = pl.BlockSpec(memory_space=pltpu.HBM)
    width = table.shape[1]
    assert table.shape[0] % PLACE_ROWS == 0
    return pl.pallas_call(
        place_kernel,
        out_shape=(
            jax.ShapeDtypeStruct(table.shape, f32), jax.ShapeDtypeStruct(dh.shape, dh.dtype),
            jax.ShapeDtypeStruct((1, 1), f32), jax.ShapeDtypeStruct((1, width), f32), jax.ShapeDtypeStruct((1, width), f32)),
        in_specs=[hbm, hbm, vmem],
        out_specs=(hbm, hbm, vmem, vmem, vmem),
        scratch_shapes=[
            pltpu.VMEM((PLACE_SLOTS, PLACE_ROWS, width), f32), pltpu.VMEM(dh.shape, dh.dtype),
            dma((PLACE_SLOTS,)), dma((PLACE_SLOTS,)), dma((2,))],
        compiler_params=pltpu.CompilerParams(vmem_limit_bytes=VMEM_BYTES),
        cost_estimate=pl.CostEstimate(flops=0, bytes_accessed=8 * table.size + 4 * dh.size, transcendentals=0),
    )(table, dh, sums)


def solution(mesh):
    n_dp = mesh.shape['dp']
    n_tp = mesh.shape['tp']

    def device_step(hidden, table, labels, loss_mask, ln_gain, ln_bias):
        batch, seq, width = hidden.shape
        grad_table, _, grad_hidden, sums = head_step(
            table, hidden.reshape(batch * seq, width), ln_gain, ln_bias, labels, loss_mask, n_dp, n_tp)
        grad_table, grad_hidden, loss, grad_gain, grad_bias = place(grad_table, grad_hidden, sums)
        return (loss.reshape(()), grad_hidden.reshape(batch, seq, width), grad_table,
                grad_gain.reshape(width), grad_bias.reshape(width))

    specs_in = (P('dp', None, None), P('tp', None), P('dp', None), P('dp', None), P(None), P(None))
    specs_out = (P(), P('dp', None, None), P('tp', None), P(None), P(None))
    return jax.shard_map(device_step, mesh=mesh, in_specs=specs_in, out_specs=specs_out, check_vma=False)
```

```python
import functools

import jax
import jax.numpy as jnp
from jax import lax
from jax.experimental import pallas as pl
from jax.experimental.pallas import tpu as pltpu
from jax.sharding import PartitionSpec as P

LN_EPS = 1e-5
VOCAB = 50257
Z = 4
Y = 2
UNITS = 33
PER_UNIT = 6
SLOTS = 16
RING = 4
END_LAG = 6
TILE = 512
PIECES = 4
FORWARD_ROWS = 1056
PLACE_ROWS = 1056
PLACE_SLOTS = 12
COLUMNS = 256
VMEM_BYTES = 67043328
MESH = pl.DeviceIdType.MESH


def signal(barrier, **where):
    pl.semaphore_signal(barrier, inc=1, device_id=where, device_id_type=MESH)


def remote(src, dst, send_sem, recv_sem, **where):
    return pltpu.make_async_remote_copy(
        src_ref=src, dst_ref=dst, send_sem=send_sem, recv_sem=recv_sem, device_id=where, device_id_type=MESH)


def neighbours(tp):
    core = tp % 2
    partner = tp + 1 - 2 * core
    beside = tp + 2 - 4 * (tp // 2)
    return partner, beside, beside + 1 - 2 * core


def tile_at(t):
    return slice(t * TILE, (t + 1) * TILE)


def aligned(start, size):
    return pl.ds(pl.multiple_of(start, size), size)


def head_kernel(
        n_dp, n_tp, table, hidden, gain, bias, labels, loss_mask,
        out, part, dh, sums,
        x, x_t, lse, scale, weight, label, target, hat, inv, send_q,
        got, block_buf, held, top, total, stats, counts, ids,
        red, met, loc, q_t, rows_buf, more_buf, stage, dx_t, from_core, from_x, levels, arrived,
        hidden_sem, block_sem, y_sem, beside_sem, core_sem, relay_sem, stat_send, stat_recv, count_send, count_recv,
        ids_sem,
        up_send, up_recv, meet_send, meet_recv, down_send, down_recv, mate_send, mate_recv, credit,
        loc_sem, own_sem, part_sem, rows_sem, more_sem,
        swap_sem, cross_sem, share_send, share_recv, level_sem):
    own, width = hidden.shape
    tokens = Y * own
    shard = table.shape[0]
    half = shard // Y
    quarter = own // n_tp
    piece = quarter // PIECES
    batch, seq = labels.shape
    size = red.shape[1]
    chunks = half // size
    unit = size * PER_UNIT
    units = chunks // PER_UNIT
    block_rows = block_buf.shape[1]
    blocks = shard // block_rows
    last = PIECES - 1
    own_tiles, all_tiles, columns = own // TILE, tokens // TILE, width // COLUMNS

    dp = lax.axis_index('dp')
    tp = lax.axis_index('tp')
    y = dp % Y
    z = dp // Y
    core = tp % 2
    mate = dp + 1 - 2 * y
    partner, beside, across = neighbours(tp)
    others = (partner, beside, across)
    dp_others = [lax.rem(dp + j, n_dp) for j in range(1, n_dp)]
    z_mate = dp + Y - 2 * Y * (z % 2)
    z_far = dp + 2 * Y - 4 * Y * (z // 2)
    inner = (z == 1) | (z == 2)
    z_cross = dp + Y * (Z - 1 - 2 * z)
    first_row = tp * shard

    barrier = pltpu.get_barrier_semaphore()
    for other in dp_others:
        signal(barrier, dp=other)
    for other in others:
        signal(barrier, tp=other)
        signal(barrier, dp=mate, tp=other)

    def hidden_copy(j):
        q = lax.rem(tp + j, n_tp)
        at = aligned(q * quarter, quarter)
        return pltpu.make_async_copy(hidden.at[at], x.at[at], hidden_sem.at[j])

    def block_copy(b):
        return pltpu.make_async_copy(
            table.at[pl.ds(b * block_rows, block_rows)], block_buf.at[b % 2], block_sem.at[b % 2])

    def got_piece(q, k):
        return got.at[q, pl.ds(k * piece, piece)]

    def y_copy(k):
        return remote(send_q.at[pl.ds(k * piece, piece)], got_piece(tp, k), y_sem.at[0, k], y_sem.at[1, k], dp=mate)

    def beside_copy(k):
        return remote(got_piece(tp, k), got_piece(tp, k), beside_sem.at[0, k], beside_sem.at[1, k], tp=beside)

    def core_copy(k):
        return remote(got_piece(tp, k), got_piece(tp, k), core_sem.at[0, k], core_sem.at[1, k], tp=partner)

    def relay_copy(k):
        return remote(got_piece(beside, k), got_piece(beside, k), relay_sem.at[0, k], relay_sem.at[1, k], tp=partner)

    def count_copy(j):
        return remote(counts.at[dp], counts.at[dp], count_send.at[j], count_recv.at[dp], dp=dp_others[j])

    def count_arrival(j):
        other = dp_others[j]
        return remote(counts.at[other], counts.at[other], count_send.at[j], count_recv.at[other], dp=other)

    def ids_copy(i):
        return remote((labels, loss_mask)[i], ids.at[i], ids_sem.at[0, i], ids_sem.at[1, i], dp=mate)

    def row_of(ref):
        return ref[...].astype(jnp.float32)[None, :]

    def block_of(q, k):
        return aligned(q * quarter + k * piece, piece)

    def normalize(at):
        h = x[at, :].astype(jnp.float32)
        mean = jnp.mean(h, axis=-1, keepdims=True)
        centred = h - mean
        variance = jnp.mean(centred * centred, axis=-1, keepdims=True)
        inv_std = lax.rsqrt(variance + LN_EPS)
        x_hat = centred * inv_std
        normed = (x_hat * row_of(gain) + row_of(bias)).astype(jnp.bfloat16)
        x[at, :] = normed
        x_t[:, at] = normed.T
        return x_hat, inv_std, normed

    def first_piece(k):
        x_hat, inv_std, normed = normalize(block_of(tp, k))
        at = slice(k * piece, (k + 1) * piece)
        send_q[at, :] = normed.astype(jnp.float32)
        hat[at, :] = x_hat
        inv[at, :] = jnp.broadcast_to(inv_std, (piece, inv.shape[1]))

    def next_quarter(j, carry):
        hidden_copy(j).wait()
        for k in range(PIECES):
            normalize(block_of(lax.rem(tp + j, n_tp), k))
        return carry

    def convert(q, k):
        wide = got[q, aligned(k * piece, piece)]
        at = aligned(own + q * quarter + k * piece, piece)
        narrow = wide.astype(jnp.bfloat16)
        x[at, :] = narrow
        x_t[:, at] = narrow.T

    def fold(logits, at):
        logits = logits.reshape(block_rows // 8, 8, TILE)
        before = top[:, at]
        now = jnp.maximum(before, jnp.max(logits, axis=0))
        total[:, at] = total[:, at] * jnp.exp(before - now) + jnp.sum(jnp.exp(logits - now[None]), axis=0)
        top[:, at] = now

    def block(b, carry):
        block_copy(b).wait()

        @pl.when(b + 1 < blocks)
        def _():
            block_copy(b + 1).start()

        def spaced(first, count):
            d = jnp.maximum(b - first, 0)
            return (b >= first) & ((d < 2) | (d == 3) | (d == 5)) & (d < 2 * count - 1), jnp.minimum((d + 1) // 2, last)

        due, k_y = spaced(3, PIECES)

        @pl.when(due)
        def _():
            with jax.named_scope('wait_y'):
                y_copy(k_y).wait_recv()
            beside_copy(k_y).start()
            core_copy(k_y).start()
            convert(tp, k_y)

        due, k_core = spaced(4, PIECES)

        @pl.when(due)
        def _():
            core_copy(k_core).wait_recv()
            convert(partner, k_core)

        due, k_x = spaced(6, PIECES)

        @pl.when(due)
        def _():
            with jax.named_scope('wait_x'):
                beside_copy(k_x).wait_recv()
            relay_copy(k_x).start()
            convert(beside, k_x)

        due, k_relay = spaced(7, PIECES - 1)

        @pl.when(due)
        def _():
            relay_copy(k_relay).wait_recv()
            convert(across, k_relay)

        slot = b % 2
        row_ids = first_row + b * block_rows + lax.broadcasted_iota(jnp.int32, (block_rows, 1), 0)
        fold(held[...], tile_at(own_tiles - 1))
        for t in range(own_tiles):
            at = tile_at(t)
            logits = jnp.dot(block_buf[slot], x_t[:, at], preferred_element_type=jnp.float32)
            logits = jnp.where(row_ids < VOCAB, logits, -jnp.inf)
            if t + 1 < own_tiles:
                fold(logits, at)
            else:
                held[...] = logits
        return carry

    def stat_copies():
        where = [{'tp': other} for other in others] + [{'dp': mate}] + [{'dp': mate, 'tp': other} for other in others]
        return [remote(stats.at[0, tp], stats.at[int(i >= n_tp - 1), tp], stat_send.at[i], stat_recv.at[int(i >= n_tp - 1), tp],
                       **w) for i, w in enumerate(where)]

    def stat_arrival(side, other):
        return remote(stats.at[side, other], stats.at[side, other], stat_send.at[0], stat_recv.at[side, other], tp=partner)

    def part_rows(c):
        return part.at[pl.ds(c * size, size)]

    def out_rows(side, c):
        return out.at[pl.ds(side * half + c * size, size)]

    def fetch(c):
        return pltpu.make_async_copy(part_rows(c), loc.at[c % 2], loc_sem.at[c % 2])

    def up_copy(c):
        return remote(part_rows(c), red.at[c % SLOTS], up_send.at[c % RING], up_recv.at[c % SLOTS], dp=z_mate)

    def meet_copy(c):
        return remote(red.at[c % SLOTS], met.at[c % SLOTS], meet_send.at[c % RING], meet_recv.at[c % SLOTS], dp=z_cross)

    def down_copy(c):
        return remote(met.at[c % SLOTS], out_rows(y, c), down_send.at[c % RING], down_recv.at[c % SLOTS], dp=z_mate)

    def mate_copy(c, src):
        return remote(src, out_rows(y, c), mate_send.at[c % RING], mate_recv.at[c // (chunks // 2)], dp=mate)

    def own_copy(c):
        return pltpu.make_async_copy(met.at[c % SLOTS], out_rows(y, c), own_sem.at[c % RING])

    def rows_copy(u):
        return pltpu.make_async_copy(table.at[pl.ds(y * half + u * unit, unit)], rows_buf.at[u % 2], rows_sem.at[u % 2])

    def more_copy(u):
        return pltpu.make_async_copy(
            table.at[pl.ds((1 - y) * half + u * unit, unit)], more_buf.at[u % 2], more_sem.at[u % 2])

    def part_copy(u):
        return pltpu.make_async_copy(stage, part.at[pl.ds(u * unit, unit)], part_sem.at[0])

    unit_iota = lax.broadcasted_iota(jnp.int32, (unit, 1), 0)

    def logits_of(table_rows, at):
        return jnp.dot(table_rows, x_t[:, at], preferred_element_type=jnp.float32)

    def grads(logits, row_ids, at):
        hit = row_ids == label[:, at]
        probs = jnp.where(row_ids + first_row < VOCAB, jnp.exp(logits - lse[:, at]), 0.0)
        q = ((probs - jnp.where(hit, 1.0, 0.0)) * scale[:, at]).astype(jnp.bfloat16)
        return q, jnp.where(hit, logits, 0.0)

    def add_dx(table_rows, q, t):
        dx_t[t] = dx_t[t] + lax.dot_general(
            table_rows, q, (((0,), (0,)), ((), ())), preferred_element_type=jnp.float32)

    def main_tile(u, t, logits=None):
        slot = u % 2
        at = tile_at(t)
        row_ids = y * half + u * unit + unit_iota
        if logits is None:
            logits = logits_of(rows_buf[slot], at)
        q, hits = grads(logits, row_ids, at)
        q_t[:, at] = q
        target[:, at] = target[:, at] + jnp.sum(hits, axis=0, keepdims=True)
        if t < own // TILE:
            add_dx(rows_buf[slot], q, t)

    def table_tile(n):
        at = slice(n * COLUMNS, (n + 1) * COLUMNS)
        stage[:, at] = jnp.dot(q_t[...], x[:, at], preferred_element_type=jnp.float32)

    def more_tile(u, t):
        theirs = (1 - y) * half + u * unit + unit_iota
        q, _ = grads(logits_of(more_buf[u % 2], tile_at(t)), theirs, tile_at(t))
        add_dx(more_buf[u % 2], q, t)

    few = (all_tiles - own_tiles) // 4

    def compute_0(u):
        rows_copy(u).wait()

        @pl.when(u + 1 < units)
        def _():
            rows_copy(u + 1).start()

        for t in list(range(own_tiles // 2)) + list(range(own_tiles, own_tiles + few)):
            main_tile(u, t)

    def compute_1(u):
        for t in list(range(own_tiles // 2, own_tiles)) + list(range(own_tiles + few, own_tiles + 2 * few)):
            main_tile(u, t)

    def compute_2(u):
        for t in range(own_tiles + 2 * few, all_tiles):
            main_tile(u, t)
        for n in range(columns):
            table_tile(n)
        part_copy(u).start()

    def early(t):
        return got.at[t // 2, pl.ds(0, unit), pl.ds(t % 2 * TILE, TILE)]

    def first_logits():
        rows_copy(0).wait()
        rows_copy(1).start()
        for t in range(all_tiles):
            early(t)[...] = logits_of(rows_buf[0], tile_at(t))

    def first_unit():
        for t in range(all_tiles):
            main_tile(0, t, early(t)[...])
        for n in range(columns):
            table_tile(n)
        part_copy(0).start()

    def compute_3(u):
        more_copy(u).wait()

        @pl.when(u + 1 < units)
        def _():
            more_copy(u + 1).start()

        for t in range(own_tiles // 2):
            more_tile(u, t)

    def compute_4(u):
        for t in range(own_tiles // 2, own_tiles):
            more_tile(u, t)

    def settle(u):
        part_copy(u).wait()

    def within(c):
        return (c >= 0) & (c < chunks)

    def take_credit(i, c):
        @pl.when(c >= SLOTS)
        def _():
            pl.semaphore_wait(credit.at[i], 1)

    def give_credit(i, c, other):
        @pl.when(c + SLOTS < chunks)
        def _():
            pl.semaphore_signal(credit.at[i], inc=1, device_id={'dp': other}, device_id_type=MESH)

    def end_step(t):
        @pl.when(t < chunks)
        def _():
            @pl.when(t >= 2)
            def _():
                up_copy(t - 2).wait_send()
            take_credit(0, t)
            up_copy(t).start()

        c = t - END_LAG

        @pl.when(within(c))
        def _():
            down_copy(c).wait_recv()

            @pl.when(c >= RING)
            def _():
                mate_copy(c - RING, out_rows(y, c - RING)).wait_send()
            mate_copy(c, out_rows(y, c)).start()

    def inner_step(t):
        c = t - 2

        @pl.when(within(c))
        def _():
            slot = c % SLOTS
            up_copy(c).wait_recv()
            fetch(c).wait()
            red[slot] = red[slot] + loc[c % 2]
            take_credit(1, c)
            meet_copy(c).start()

        @pl.when(within(c + 1))
        def _():
            fetch(c + 1).start()

        c_met = t - 4

        @pl.when(within(c_met))
        def _():
            slot = c_met % SLOTS
            meet_copy(c_met).wait_recv()
            met[slot] = red[slot] + met[slot]
            down_copy(c_met).start()
            mate_copy(c_met, met.at[slot]).start()
            own_copy(c_met).start()
            meet_copy(c_met).wait_send()
            give_credit(0, c_met, z_mate)

        c_gone = t - 6

        @pl.when(within(c_gone))
        def _():
            own_copy(c_gone).wait()
            down_copy(c_gone).wait_send()
            mate_copy(c_gone, met.at[c_gone % SLOTS]).wait_send()
            give_credit(1, c_gone, z_cross)

    def swap_copy(i):
        return remote(dx_t.at[2 * i + 1 - core], from_core.at[i], swap_sem.at[0, i], swap_sem.at[1, i], tp=partner)

    def cross_copy():
        return remote(dx_t.at[beside], from_x, cross_sem.at[0], cross_sem.at[1], tp=beside)

    def share_copy(i):
        return remote(send_q, got.at[tp], share_send.at[i], share_recv.at[i], tp=others[i])

    def pass_copy():
        return remote(got.at[beside], got.at[beside], share_send.at[2], share_recv.at[2], tp=partner)

    def round_dh(q, ref):
        at = aligned(q * quarter, quarter)
        x[at, :] = ref.astype(jnp.bfloat16)

    def dh_relay():
        share_copy(1).wait_recv()
        pass_copy().start()
        round_dh(beside, got[beside])
        share_copy(0).wait_recv()
        round_dh(partner, got[partner])
        round_dh(tp, send_q[...])

    def dh_copy():
        return pltpu.make_async_copy(x.at[pl.ds(0, own)], dh, hidden_sem.at[0])

    def dh_finish():
        pass_copy().wait_recv()
        round_dh(across, got[across])
        dh_copy().start()

    slab = 128

    def add_into(j, ref):
        def body(i, carry):
            at = aligned(i * slab, slab)
            dx_t[j, at] = dx_t[j, at] + ref[at]
            return carry
        lax.fori_loop(0, width // slab, body, 0)

    def dx_start():
        for i in range(2):
            swap_copy(i).start()

    def dx_middle():
        for i in range(2):
            swap_copy(i).wait_recv()
            add_into(2 * i + core, from_core.at[i])
        cross_copy().start()

    def dx_finish():
        cross_copy().wait_recv()
        add_into(tp, from_x)
        for i in range(width // slab):
            at = pl.ds(i * slab, slab)
            send_q[:, at] = dx_t[tp, at].T

        levels[0] = jnp.zeros(levels.shape[1:], jnp.float32)
        own_loss = weight[:, :own] * lse[:, :own] * (1.0 / n_tp) - weight[:, :own] * target[:, :own]
        loss_part = own_loss - weight[:, own:] * target[:, own:]
        levels[0, 2:3] = sum(loss_part[:, i * width:(i + 1) * width] for i in range(own // width))
        step = min(64, quarter)

        def token_block(i, carry):
            at = aligned(i * step, step)
            grad = send_q[at, :]
            x_hat = hat[at, :]
            levels[0, 0:1] = levels[0, 0:1] + jnp.sum(grad * x_hat, axis=0, keepdims=True)
            levels[0, 1:2] = levels[0, 1:2] + jnp.sum(grad, axis=0, keepdims=True)
            grad_hat = grad * row_of(gain)
            mean_grad = jnp.mean(grad_hat, axis=-1, keepdims=True)
            mean_proj = jnp.mean(grad_hat * x_hat, axis=-1, keepdims=True)
            send_q[at, :] = inv[at, 0:1] * (grad_hat - mean_grad - x_hat * mean_proj)
            return carry

        lax.fori_loop(0, quarter // step, token_block, 0)
        level_copy(0).start()
        for i in range(2):
            share_copy(i).start()

    level_peers = ({'tp': beside}, {'tp': partner}, {'dp': mate}, {'dp': z_mate}, {'dp': z_far})

    def level_copy(i):
        return remote(levels.at[i], arrived.at[i], level_sem.at[0, i], level_sem.at[1, i], **level_peers[i])

    def level_next(i):
        level_copy(i).wait_recv()
        merged = levels[i] + arrived[i]
        if i + 1 < len(level_peers):
            levels[i + 1] = merged
            level_copy(i + 1).start()
        else:
            sums[...] = merged
            sums[2:3] = jnp.broadcast_to(jnp.sum(merged[2:3], axis=-1, keepdims=True) / tokens_counted(), (1, width))

    def tokens_counted():
        return sum(counts[j, 0:1, 0:1] for j in range(n_dp))

    for j in range(n_tp):
        hidden_copy(j).start()
    block_copy(0).start()
    rows_copy(0).start()
    more_copy(0).start()
    hidden_copy(0).wait()
    for k in range(PIECES):
        first_piece(k)
    with jax.named_scope('lnrest'):
        lax.fori_loop(1, n_tp, next_quarter, 0)
    counts[dp] = jnp.full(counts.shape[1:], jnp.sum(loss_mask[...].astype(jnp.float32)), jnp.float32)
    pl.semaphore_wait(barrier, n_dp - 1 + 2 * len(others))
    for k in range(PIECES):
        y_copy(k).start()
    for i in range(2):
        ids_copy(i).start()
    for j in range(n_dp - 1):
        count_copy(j).start()

    top[...] = jnp.full_like(top, jnp.finfo(jnp.float32).min)
    total[...] = jnp.zeros_like(total)
    held[...] = jnp.full_like(held, -jnp.inf)
    target[...] = jnp.zeros_like(target)

    def clear(t, carry):
        dx_t[t] = jnp.zeros(dx_t.shape[1:], jnp.float32)
        return carry

    lax.fori_loop(0, own // TILE, clear, 0)
    assert blocks > 11 and PIECES == 4
    with jax.named_scope('blocks'):
        lax.fori_loop(0, blocks, block, 0)
    fold(held[...], tile_at(own_tiles - 1))

    best = jnp.max(top[...], axis=0, keepdims=True)
    stats[0, tp, 0:1] = best
    stats[0, tp, 1:2] = jnp.sum(total[...] * jnp.exp(top[...] - best), axis=0, keepdims=True)
    for copy in stat_copies():
        copy.start()

    with jax.named_scope('lastrelay'):
        relay_copy(last).wait_recv()
    convert(across, last)
    for i in range(2):
        ids_copy(i).wait()
    for j in range(n_dp - 1):
        count_arrival(j).wait_recv()
    for i in range(batch):
        for side, (rows_of, marks) in enumerate(((labels, loss_mask), (ids.at[0], ids.at[1]))):
            at = slice(side * own + i * seq, side * own + (i + 1) * seq)
            label[:, at] = rows_of[i:i + 1, :] - first_row
            weight[:, at] = marks[i:i + 1, :].astype(jnp.float32)
    scale[...] = weight[...] / tokens_counted()
    for k in range(PIECES):
        for copy in (y_copy(k), beside_copy(k), core_copy(k), relay_copy(k)):
            copy.wait_send()
    for j in range(n_dp - 1):
        count_copy(j).wait_send()
    with jax.named_scope('early'):
        first_logits()
    with jax.named_scope('statwait'):
        for other in others:
            stat_arrival(0, other).wait_recv()
        for other in (tp,) + others:
            stat_arrival(1, other).wait_recv()
    for side in range(Y):
        tops = [stats[side, j, 0:1] for j in range(n_tp)]
        best = functools.reduce(jnp.maximum, tops)
        mass = sum(stats[side, j, 1:2] * jnp.exp(tops[j] - best) for j in range(n_tp))
        lse[:, side * own:(side + 1) * own] = best + jnp.log(mass)

    with jax.named_scope('first'):
        first_unit()

    computes = (compute_0, compute_1, compute_2, compute_3, compute_4)
    beats = len(computes)
    start = beats - 2
    done = beats * units - 1
    ticks = start + chunks + END_LAG
    assert done + 38 < ticks

    def tick(i, carry):
        u = i // beats
        kind = i % beats

        @pl.when(i == start)
        def _():
            settle(0)

        @pl.when(jnp.logical_not(inner))
        def _():
            with jax.named_scope('red'):
                end_step(jnp.maximum(i - start, 0))

        @pl.when(inner)
        def _():
            with jax.named_scope('red'):
                inner_step(jnp.maximum(i - start, 0))

        @pl.when((i > start) & (kind == start) & (u < units))
        def _():
            settle(u)

        for j, compute in enumerate(computes):
            def scoped(compute=compute, j=j):
                with jax.named_scope(f'calc{j}'):
                    compute(u)
            pl.when((kind == j) & (u < units))(scoped)

        events = ((1, dx_start), (5, dx_middle), (22, dx_finish), (24, lambda: level_next(0)), (26, lambda: level_next(1)),
                  (31, lambda: level_next(2)), (36, lambda: level_next(3)), (38, dh_relay))
        for after, event in events:
            pl.when(i == done + after)(event)
        return carry

    lax.fori_loop(start, ticks, tick, 0)
    level_next(4)
    dh_finish()

    @pl.when(jnp.logical_not(inner))
    def _():
        for c in range(chunks - 2, chunks):
            up_copy(c).wait_send()
        for c in range(chunks - RING, chunks):
            mate_copy(c, out_rows(y, c)).wait_send()

    for i in range(2):
        theirs = out.at[pl.ds((1 - y) * half + i * (half // 2), half // 2)]
        with jax.named_scope('matewait'):
            pltpu.make_async_copy(theirs, theirs, mate_recv.at[i]).wait()
    for copy in stat_copies():
        copy.wait_send()
    for i in range(2):
        swap_copy(i).wait_send()
    cross_copy().wait_send()
    for i in range(2):
        share_copy(i).wait_send()
    pass_copy().wait_send()
    dh_copy().wait()
    for i in range(len(level_peers)):
        level_copy(i).wait_send()


def head_step(table, hidden, gain, bias, labels, loss_mask, n_dp, n_tp):
    own, width = hidden.shape
    tokens = Y * own
    shard = table.shape[0]
    half = shard // Y
    size = half // (UNITS * PER_UNIT)
    unit = size * PER_UNIT
    quarter = own // n_tp
    assert unit <= quarter and 2 * TILE <= width and unit * UNITS == half and size % 8 == 0 and unit % 32 == 0 and quarter == TILE
    assert shard % FORWARD_ROWS == 0
    f32 = jnp.float32
    b16 = jnp.bfloat16
    i32 = jnp.int32
    lanes = 128
    dma = pltpu.SemaphoreType.DMA
    vmem = pl.BlockSpec(memory_space=pltpu.VMEM)
    hbm = pl.BlockSpec(memory_space=pl.ANY)
    flops = 2 * width * (own * shard + half * (2 * tokens + 3 * own))
    return pl.pallas_call(
        functools.partial(head_kernel, n_dp, n_tp),
        out_shape=(
            jax.ShapeDtypeStruct((shard, width), f32),
            jax.ShapeDtypeStruct((half, width), f32),
            jax.ShapeDtypeStruct((own, width), b16),
            jax.ShapeDtypeStruct((8, width), f32)),
        in_specs=[hbm, hbm, vmem, vmem, vmem, vmem],
        out_specs=(hbm, hbm, hbm, vmem),
        scratch_shapes=[
            pltpu.VMEM((tokens, width), b16), pltpu.VMEM((width, tokens), b16),
            pltpu.VMEM((1, tokens), f32), pltpu.VMEM((1, tokens), f32), pltpu.VMEM((1, tokens), f32),
            pltpu.VMEM((1, tokens), i32), pltpu.VMEM((1, tokens), f32),
            pltpu.VMEM((quarter, width), f32), pltpu.VMEM((quarter, lanes), f32), pltpu.VMEM((quarter, width), f32),
            pltpu.VMEM((n_tp, quarter, width), f32), pltpu.VMEM((2, FORWARD_ROWS, width), b16),
            pltpu.VMEM((FORWARD_ROWS, TILE), f32),
            pltpu.VMEM((8, own), f32), pltpu.VMEM((8, own), f32),
            pltpu.VMEM((Y, n_tp, 2, own), f32), pltpu.VMEM((n_dp, 8, lanes), f32),
            pltpu.VMEM((2,) + labels.shape, i32),
            pltpu.VMEM((SLOTS, size, width), f32), pltpu.VMEM((SLOTS, size, width), f32), pltpu.VMEM((2, size, width), f32),
            pltpu.VMEM((unit, tokens), b16),
            pltpu.VMEM((2, unit, width), b16), pltpu.VMEM((2, unit, width), b16),
            pltpu.VMEM((unit, width), f32),
            pltpu.VMEM((n_tp, width, quarter), f32),
            pltpu.VMEM((2, width, quarter), f32), pltpu.VMEM((width, quarter), f32),
            pltpu.VMEM((5, 8, width), f32), pltpu.VMEM((5, 8, width), f32),
            dma((n_tp,)), dma((2,)), dma((2, PIECES)), dma((2, PIECES)), dma((2, PIECES)), dma((2, PIECES)),
            dma((2 * n_tp - 1,)), dma((Y, n_tp)), dma((n_dp - 1,)), dma((n_dp,)),
            dma((2, 2)),
            dma((RING,)), dma((SLOTS,)), dma((RING,)), dma((SLOTS,)), dma((RING,)), dma((SLOTS,)), dma((RING,)), dma((2,)),
            pltpu.SemaphoreType.REGULAR((2,)),
            dma((2,)), dma((RING,)), dma((1,)), dma((2,)), dma((2,)),
            dma((2, 2)), dma((2,)), dma((3,)), dma((3,)), dma((2, 5)),
        ],
        compiler_params=pltpu.CompilerParams(
            collective_id=0, has_side_effects=True, vmem_limit_bytes=VMEM_BYTES),
        cost_estimate=pl.CostEstimate(flops=flops, bytes_accessed=12 * half * width, transcendentals=half * tokens),
    )(table, hidden, gain, bias, labels, loss_mask)


def place_kernel(table_in, dh_in, sums, table_out, dh_out, loss, gain_out, bias_out, buf, dh_buf, in_sem, out_sem, dh_sem):
    size = buf.shape[1]
    count = table_in.shape[0] // size
    lag = PLACE_SLOTS // 2

    def read(i):
        return pltpu.make_async_copy(table_in.at[pl.ds(i * size, size)], buf.at[i % PLACE_SLOTS], in_sem.at[i % PLACE_SLOTS])

    def write(i):
        return pltpu.make_async_copy(buf.at[i % PLACE_SLOTS], table_out.at[pl.ds(i * size, size)], out_sem.at[i % PLACE_SLOTS])

    dh_read = pltpu.make_async_copy(dh_in, dh_buf, dh_sem.at[0])
    dh_write = pltpu.make_async_copy(dh_buf, dh_out, dh_sem.at[1])
    for i in range(count + lag):
        if i < count:
            if i >= PLACE_SLOTS:
                write(i - PLACE_SLOTS).wait()
            read(i).start()
        if i == 0:
            dh_read.start()
            loss[...] = sums[2:3, 0:1]
            gain_out[...] = sums[0:1, :]
            bias_out[...] = sums[1:2, :]
        if i == lag:
            dh_read.wait()
            dh_write.start()
        if i >= lag:
            read(i - lag).wait()
            write(i - lag).start()
    for i in range(count - PLACE_SLOTS, count):
        write(i).wait()
    dh_write.wait()


def place(table, dh, sums):
    f32 = jnp.float32
    dma = pltpu.SemaphoreType.DMA
    vmem = pl.BlockSpec(memory_space=pltpu.VMEM)
    hbm = pl.BlockSpec(memory_space=pltpu.HBM)
    width = table.shape[1]
    assert table.shape[0] % PLACE_ROWS == 0
    return pl.pallas_call(
        place_kernel,
        out_shape=(
            jax.ShapeDtypeStruct(table.shape, f32), jax.ShapeDtypeStruct(dh.shape, dh.dtype),
            jax.ShapeDtypeStruct((1, 1), f32), jax.ShapeDtypeStruct((1, width), f32), jax.ShapeDtypeStruct((1, width), f32)),
        in_specs=[hbm, hbm, vmem],
        out_specs=(hbm, hbm, vmem, vmem, vmem),
        scratch_shapes=[
            pltpu.VMEM((PLACE_SLOTS, PLACE_ROWS, width), f32), pltpu.VMEM(dh.shape, dh.dtype),
            dma((PLACE_SLOTS,)), dma((PLACE_SLOTS,)), dma((2,))],
        compiler_params=pltpu.CompilerParams(vmem_limit_bytes=VMEM_BYTES),
        cost_estimate=pl.CostEstimate(flops=0, bytes_accessed=8 * table.size + 4 * dh.size, transcendentals=0),
    )(table, dh, sums)


def solution(mesh):
    n_dp = mesh.shape['dp']
    n_tp = mesh.shape['tp']

    def device_step(hidden, table, labels, loss_mask, ln_gain, ln_bias):
        batch, seq, width = hidden.shape
        grad_table, _, grad_hidden, sums = head_step(
            table, hidden.reshape(batch * seq, width), ln_gain, ln_bias, labels, loss_mask, n_dp, n_tp)
        grad_table, grad_hidden, loss, grad_gain, grad_bias = place(grad_table, grad_hidden, sums)
        return (loss.reshape(()), grad_hidden.reshape(batch, seq, width), grad_table,
                grad_gain.reshape(width), grad_bias.reshape(width))

    specs_in = (P('dp', None, None), P('tp', None), P('dp', None), P('dp', None), P(None), P(None))
    specs_out = (P(), P('dp', None, None), P('tp', None), P(None), P(None))
    return jax.shard_map(device_step, mesh=mesh, in_specs=specs_in, out_specs=specs_out, check_vma=False)
```

```python
import functools

import jax
import jax.numpy as jnp
from jax import lax
from jax.experimental import pallas as pl
from jax.experimental.pallas import tpu as pltpu
from jax.sharding import PartitionSpec as P

LN_EPS = 1e-5
VOCAB = 50257
Z = 4
Y = 2
UNITS = 33
PER_UNIT = 6
SLOTS = 8
RING = 4
END_LAG = 6
TILE = 512
PIECES = 4
FORWARD_ROWS = 1056
PLACE_ROWS = 1056
PLACE_SLOTS = 12
COLUMNS = 256
VMEM_BYTES = 67043328
MESH = pl.DeviceIdType.MESH


def signal(barrier, **where):
    pl.semaphore_signal(barrier, inc=1, device_id=where, device_id_type=MESH)


def remote(src, dst, send_sem, recv_sem, **where):
    return pltpu.make_async_remote_copy(
        src_ref=src, dst_ref=dst, send_sem=send_sem, recv_sem=recv_sem, device_id=where, device_id_type=MESH)


def neighbours(tp):
    core = tp % 2
    partner = tp + 1 - 2 * core
    beside = tp + 2 - 4 * (tp // 2)
    return partner, beside, beside + 1 - 2 * core


def tile_at(t):
    return slice(t * TILE, (t + 1) * TILE)


def aligned(start, size):
    return pl.ds(pl.multiple_of(start, size), size)


def head_kernel(
        n_dp, n_tp, table, hidden, gain, bias, labels, loss_mask,
        out, part, dh, sums,
        x, x_t, lse, scale, weight, label, target, hat, inv, send_q,
        got, block_buf, held, top, total, stats, counts, ids,
        red, met, loc, q_t, rows_buf, more_buf, stage, dx_t, from_core, from_x, levels, arrived,
        hidden_sem, block_sem, y_sem, beside_sem, core_sem, relay_sem, stat_send, stat_recv, count_send, count_recv,
        ids_sem,
        up_send, up_recv, meet_send, meet_recv, down_send, down_recv, mate_send, mate_recv, credit,
        loc_sem, own_sem, part_sem, rows_sem, more_sem,
        swap_sem, cross_sem, share_send, share_recv, level_sem):
    own, width = hidden.shape
    tokens = Y * own
    shard = table.shape[0]
    half = shard // Y
    quarter = own // n_tp
    piece = quarter // PIECES
    batch, seq = labels.shape
    size = red.shape[1]
    chunks = half // size
    unit = size * PER_UNIT
    units = chunks // PER_UNIT
    block_rows = block_buf.shape[1]
    blocks = shard // block_rows
    last = PIECES - 1
    own_tiles, all_tiles, columns = own // TILE, tokens // TILE, width // COLUMNS

    dp = lax.axis_index('dp')
    tp = lax.axis_index('tp')
    y = dp % Y
    z = dp // Y
    core = tp % 2
    mate = dp + 1 - 2 * y
    partner, beside, across = neighbours(tp)
    others = (partner, beside, across)
    dp_others = [lax.rem(dp + j, n_dp) for j in range(1, n_dp)]
    z_mate = dp + Y - 2 * Y * (z % 2)
    z_far = dp + 2 * Y - 4 * Y * (z // 2)
    inner = (z == 1) | (z == 2)
    z_cross = dp + Y * (Z - 1 - 2 * z)
    first_row = tp * shard

    barrier = pltpu.get_barrier_semaphore()
    for other in dp_others:
        signal(barrier, dp=other)
    for other in others:
        signal(barrier, tp=other)
        signal(barrier, dp=mate, tp=other)

    def hidden_copy(j):
        q = lax.rem(tp + j, n_tp)
        at = aligned(q * quarter, quarter)
        return pltpu.make_async_copy(hidden.at[at], x.at[at], hidden_sem.at[j])

    def block_copy(b):
        return pltpu.make_async_copy(
            table.at[pl.ds(b * block_rows, block_rows)], block_buf.at[b % 2], block_sem.at[b % 2])

    def got_piece(q, k):
        return got.at[q, pl.ds(k * piece, piece)]

    def y_copy(k):
        return remote(send_q.at[pl.ds(k * piece, piece)], got_piece(tp, k), y_sem.at[0, k], y_sem.at[1, k], dp=mate)

    def beside_copy(k):
        return remote(got_piece(tp, k), got_piece(tp, k), beside_sem.at[0, k], beside_sem.at[1, k], tp=beside)

    def core_copy(k):
        return remote(got_piece(tp, k), got_piece(tp, k), core_sem.at[0, k], core_sem.at[1, k], tp=partner)

    def relay_copy(k):
        return remote(got_piece(beside, k), got_piece(beside, k), relay_sem.at[0, k], relay_sem.at[1, k], tp=partner)

    def count_copy(j):
        return remote(counts.at[dp], counts.at[dp], count_send.at[j], count_recv.at[dp], dp=dp_others[j])

    def count_arrival(j):
        other = dp_others[j]
        return remote(counts.at[other], counts.at[other], count_send.at[j], count_recv.at[other], dp=other)

    def ids_copy(i):
        return remote((labels, loss_mask)[i], ids.at[i], ids_sem.at[0, i], ids_sem.at[1, i], dp=mate)

    def row_of(ref):
        return ref[...].astype(jnp.float32)[None, :]

    def block_of(q, k):
        return aligned(q * quarter + k * piece, piece)

    def normalize(at):
        h = x[at, :].astype(jnp.float32)
        mean = jnp.mean(h, axis=-1, keepdims=True)
        centred = h - mean
        variance = jnp.mean(centred * centred, axis=-1, keepdims=True)
        inv_std = lax.rsqrt(variance + LN_EPS)
        x_hat = centred * inv_std
        normed = (x_hat * row_of(gain) + row_of(bias)).astype(jnp.bfloat16)
        x[at, :] = normed
        x_t[:, at] = normed.T
        return x_hat, inv_std, normed

    def first_piece(k):
        x_hat, inv_std, normed = normalize(block_of(tp, k))
        at = slice(k * piece, (k + 1) * piece)
        send_q[at, :] = normed.astype(jnp.float32)
        hat[at, :] = x_hat
        inv[at, :] = jnp.broadcast_to(inv_std, (piece, inv.shape[1]))

    def next_quarter(j, carry):
        hidden_copy(j).wait()
        for k in range(PIECES):
            normalize(block_of(lax.rem(tp + j, n_tp), k))
        return carry

    def convert(q, k):
        wide = got[q, aligned(k * piece, piece)]
        at = aligned(own + q * quarter + k * piece, piece)
        narrow = wide.astype(jnp.bfloat16)
        x[at, :] = narrow
        x_t[:, at] = narrow.T

    def fold(logits, at):
        logits = logits.reshape(block_rows // 8, 8, TILE)
        before = top[:, at]
        now = jnp.maximum(before, jnp.max(logits, axis=0))
        total[:, at] = total[:, at] * jnp.exp(before - now) + jnp.sum(jnp.exp(logits - now[None]), axis=0)
        top[:, at] = now

    def block(b, carry):
        block_copy(b).wait()

        @pl.when(b + 1 < blocks)
        def _():
            block_copy(b + 1).start()

        def spaced(first, count):
            d = jnp.maximum(b - first, 0)
            return (b >= first) & ((d < 2) | (d == 3) | (d == 5)) & (d < 2 * count - 1), jnp.minimum((d + 1) // 2, last)

        due, k_y = spaced(3, PIECES)

        @pl.when(due)
        def _():
            y_copy(k_y).wait_recv()
            beside_copy(k_y).start()
            core_copy(k_y).start()
            convert(tp, k_y)

        due, k_core = spaced(4, PIECES)

        @pl.when(due)
        def _():
            core_copy(k_core).wait_recv()
            convert(partner, k_core)

        due, k_x = spaced(6, PIECES)

        @pl.when(due)
        def _():
            beside_copy(k_x).wait_recv()
            relay_copy(k_x).start()
            convert(beside, k_x)

        due, k_relay = spaced(7, PIECES - 1)

        @pl.when(due)
        def _():
            relay_copy(k_relay).wait_recv()
            convert(across, k_relay)

        slot = b % 2
        row_ids = first_row + b * block_rows + lax.broadcasted_iota(jnp.int32, (block_rows, 1), 0)
        fold(held[...], tile_at(own_tiles - 1))
        for t in range(own_tiles):
            at = tile_at(t)
            logits = jnp.dot(block_buf[slot], x_t[:, at], preferred_element_type=jnp.float32)
            logits = jnp.where(row_ids < VOCAB, logits, -jnp.inf)
            if t + 1 < own_tiles:
                fold(logits, at)
            else:
                held[...] = logits
        return carry

    def stat_copies():
        where = [{'tp': other} for other in others] + [{'dp': mate}] + [{'dp': mate, 'tp': other} for other in others]
        return [remote(stats.at[0, tp], stats.at[int(i >= n_tp - 1), tp], stat_send.at[i], stat_recv.at[int(i >= n_tp - 1), tp],
                       **w) for i, w in enumerate(where)]

    def stat_arrival(side, other):
        return remote(stats.at[side, other], stats.at[side, other], stat_send.at[0], stat_recv.at[side, other], tp=partner)

    def part_rows(c):
        return part.at[pl.ds(c * size, size)]

    def out_rows(side, c):
        return out.at[pl.ds(side * half + c * size, size)]

    def fetch(c):
        return pltpu.make_async_copy(part_rows(c), loc.at[c % 2], loc_sem.at[c % 2])

    def up_copy(c):
        return remote(part_rows(c), red.at[c % SLOTS], up_send.at[c % RING], up_recv.at[c % SLOTS], dp=z_mate)

    def meet_copy(c):
        return remote(red.at[c % SLOTS], met.at[c % SLOTS], meet_send.at[c % RING], meet_recv.at[c % SLOTS], dp=z_cross)

    def down_copy(c):
        return remote(met.at[c % SLOTS], out_rows(y, c), down_send.at[c % RING], down_recv.at[c % SLOTS], dp=z_mate)

    def mate_copy(c, src):
        return remote(src, out_rows(y, c), mate_send.at[c % RING], mate_recv.at[c // (chunks // 2)], dp=mate)

    def own_copy(c):
        return pltpu.make_async_copy(met.at[c % SLOTS], out_rows(y, c), own_sem.at[c % RING])

    def rows_copy(u):
        return pltpu.make_async_copy(table.at[pl.ds(y * half + u * unit, unit)], rows_buf.at[u % 2], rows_sem.at[u % 2])

    def more_copy(u):
        return pltpu.make_async_copy(
            table.at[pl.ds((1 - y) * half + u * unit, unit)], more_buf.at[u % 2], more_sem.at[u % 2])

    def part_copy(u):
        return pltpu.make_async_copy(stage, part.at[pl.ds(u * unit, unit)], part_sem.at[0])

    unit_iota = lax.broadcasted_iota(jnp.int32, (unit, 1), 0)

    def logits_of(table_rows, at):
        return jnp.dot(table_rows, x_t[:, at], preferred_element_type=jnp.float32)

    def grads(logits, row_ids, at):
        hit = row_ids == label[:, at]
        probs = jnp.where(row_ids + first_row < VOCAB, jnp.exp(logits - lse[:, at]), 0.0)
        q = ((probs - jnp.where(hit, 1.0, 0.0)) * scale[:, at]).astype(jnp.bfloat16)
        return q, jnp.where(hit, logits, 0.0)

    def dx_of(table_rows, q):
        return lax.dot_general(table_rows, q, (((0,), (0,)), ((), ())), preferred_element_type=jnp.float32)

    def add_dx(table_rows, q, t):
        dx_t[t] = dx_t[t] + dx_of(table_rows, q)

    def main_tile(u, t, logits=None):
        slot = u % 2
        at = tile_at(t)
        row_ids = y * half + u * unit + unit_iota
        is_first = logits is not None
        if not is_first:
            logits = logits_of(rows_buf[slot], at)
        q, hits = grads(logits, row_ids, at)
        q_t[:, at] = q
        target[:, at] = target[:, at] + jnp.sum(hits, axis=0, keepdims=True)
        if t < own_tiles and is_first:
            dx_t[t] = dx_of(rows_buf[slot], q)
        elif t < own_tiles:
            add_dx(rows_buf[slot], q, t)

    def table_tile(n):
        at = slice(n * COLUMNS, (n + 1) * COLUMNS)
        stage[:, at] = jnp.dot(q_t[...], x[:, at], preferred_element_type=jnp.float32)

    def more_tile(u, t):
        theirs = (1 - y) * half + u * unit + unit_iota
        q, _ = grads(logits_of(more_buf[u % 2], tile_at(t)), theirs, tile_at(t))
        add_dx(more_buf[u % 2], q, t)

    few = (all_tiles - own_tiles) // 4

    def compute_0(u):
        rows_copy(u).wait()

        @pl.when(u + 1 < units)
        def _():
            rows_copy(u + 1).start()

        for t in list(range(own_tiles // 2)) + list(range(own_tiles, own_tiles + few)):
            main_tile(u, t)

    def compute_1(u):
        for t in list(range(own_tiles // 2, own_tiles)) + list(range(own_tiles + few, own_tiles + 2 * few)):
            main_tile(u, t)

    def compute_2(u):
        for t in range(own_tiles + 2 * few, all_tiles):
            main_tile(u, t)
        for n in range(columns):
            table_tile(n)
        part_copy(u).start()

    def early(t):
        return got.at[t // 2, pl.ds(0, unit), pl.ds(t % 2 * TILE, TILE)]

    def first_logits():
        rows_copy(0).wait()
        rows_copy(1).start()
        for t in range(all_tiles):
            early(t)[...] = logits_of(rows_buf[0], tile_at(t))

    def first_unit():
        for t in range(all_tiles):
            main_tile(0, t, early(t)[...])
        for n in range(columns):
            table_tile(n)
        part_copy(0).start()

    def compute_3(u):
        more_copy(u).wait()

        @pl.when(u + 1 < units)
        def _():
            more_copy(u + 1).start()

        for t in range(own_tiles // 2):
            more_tile(u, t)

    def compute_4(u):
        for t in range(own_tiles // 2, own_tiles):
            more_tile(u, t)

    def settle(u):
        part_copy(u).wait()

    def within(c):
        return (c >= 0) & (c < chunks)

    def take_credit(i, c):
        @pl.when(c >= SLOTS)
        def _():
            pl.semaphore_wait(credit.at[i], 1)

    def give_credit(i, c, other):
        @pl.when(c + SLOTS < chunks)
        def _():
            pl.semaphore_signal(credit.at[i], inc=1, device_id={'dp': other}, device_id_type=MESH)

    def end_step(t):
        @pl.when(t < chunks)
        def _():
            @pl.when(t >= 2)
            def _():
                up_copy(t - 2).wait_send()
            take_credit(0, t)
            up_copy(t).start()

        c = t - END_LAG

        @pl.when(within(c))
        def _():
            down_copy(c).wait_recv()

            @pl.when(c >= RING)
            def _():
                mate_copy(c - RING, out_rows(y, c - RING)).wait_send()
            mate_copy(c, out_rows(y, c)).start()

    def inner_step(t):
        c = t - 2

        @pl.when(within(c))
        def _():
            slot = c % SLOTS
            up_copy(c).wait_recv()
            fetch(c).wait()
            red[slot] = red[slot] + loc[c % 2]
            take_credit(1, c)
            meet_copy(c).start()

        @pl.when(within(c + 1))
        def _():
            fetch(c + 1).start()

        c_met = t - 4

        @pl.when(within(c_met))
        def _():
            slot = c_met % SLOTS
            meet_copy(c_met).wait_recv()
            met[slot] = red[slot] + met[slot]
            down_copy(c_met).start()
            mate_copy(c_met, met.at[slot]).start()
            own_copy(c_met).start()
            meet_copy(c_met).wait_send()
            give_credit(0, c_met, z_mate)

        c_gone = t - 6

        @pl.when(within(c_gone))
        def _():
            own_copy(c_gone).wait()
            down_copy(c_gone).wait_send()
            mate_copy(c_gone, met.at[c_gone % SLOTS]).wait_send()
            give_credit(1, c_gone, z_cross)

    def swap_copy(i):
        return remote(dx_t.at[2 * i + 1 - core], from_core.at[i], swap_sem.at[0, i], swap_sem.at[1, i], tp=partner)

    def cross_copy():
        return remote(dx_t.at[beside], from_x, cross_sem.at[0], cross_sem.at[1], tp=beside)

    def share_copy(i):
        return remote(send_q, got.at[tp], share_send.at[i], share_recv.at[i], tp=others[i])

    def pass_copy():
        return remote(got.at[beside], got.at[beside], share_send.at[2], share_recv.at[2], tp=partner)

    def round_dh(q, ref):
        at = aligned(q * quarter, quarter)
        x[at, :] = ref.astype(jnp.bfloat16)

    def dh_own():
        round_dh(tp, send_q[...])

    def dh_partner():
        share_copy(0).wait_recv()
        round_dh(partner, got[partner])

    def dh_relay():
        share_copy(1).wait_recv()
        pass_copy().start()

    def dh_copy():
        return pltpu.make_async_copy(x.at[pl.ds(0, own)], dh, hidden_sem.at[0])

    def dh_finish():
        round_dh(beside, got[beside])
        pass_copy().wait_recv()
        round_dh(across, got[across])
        dh_copy().start()

    slab = 128

    def add_into(j, ref):
        def body(i, carry):
            at = aligned(i * slab, slab)
            dx_t[j, at] = dx_t[j, at] + ref[at]
            return carry
        lax.fori_loop(0, width // slab, body, 0)

    def dx_start():
        for i in range(2):
            swap_copy(i).start()

    def dx_middle():
        for i in range(2):
            swap_copy(i).wait_recv()
            add_into(2 * i + core, from_core.at[i])
        cross_copy().start()

    def dx_finish():
        cross_copy().wait_recv()
        add_into(tp, from_x)
        for i in range(width // slab):
            at = pl.ds(i * slab, slab)
            send_q[:, at] = dx_t[tp, at].T

        levels[0] = jnp.zeros(levels.shape[1:], jnp.float32)
        own_loss = weight[:, :own] * lse[:, :own] * (1.0 / n_tp) - weight[:, :own] * target[:, :own]
        loss_part = own_loss - weight[:, own:] * target[:, own:]
        levels[0, 2:3] = sum(loss_part[:, i * width:(i + 1) * width] for i in range(own // width))
        step = min(64, quarter)

        def token_block(i, carry):
            at = aligned(i * step, step)
            grad = send_q[at, :]
            x_hat = hat[at, :]
            levels[0, 0:1] = levels[0, 0:1] + jnp.sum(grad * x_hat, axis=0, keepdims=True)
            levels[0, 1:2] = levels[0, 1:2] + jnp.sum(grad, axis=0, keepdims=True)
            grad_hat = grad * row_of(gain)
            mean_grad = jnp.mean(grad_hat, axis=-1, keepdims=True)
            mean_proj = jnp.mean(grad_hat * x_hat, axis=-1, keepdims=True)
            send_q[at, :] = inv[at, 0:1] * (grad_hat - mean_grad - x_hat * mean_proj)
            return carry

        lax.fori_loop(0, quarter // step, token_block, 0)
        level_copy(0).start()
        for i in range(2):
            share_copy(i).start()

    level_peers = ({'tp': beside}, {'tp': partner}, {'dp': mate}, {'dp': z_mate}, {'dp': z_far})

    def level_copy(i):
        return remote(levels.at[i], arrived.at[i], level_sem.at[0, i], level_sem.at[1, i], **level_peers[i])

    def level_next(i):
        level_copy(i).wait_recv()
        merged = levels[i] + arrived[i]
        if i + 1 < len(level_peers):
            levels[i + 1] = merged
            level_copy(i + 1).start()
        else:
            sums[...] = merged
            sums[2:3] = jnp.broadcast_to(jnp.sum(merged[2:3], axis=-1, keepdims=True) / tokens_counted(), (1, width))

    def tokens_counted():
        return sum(counts[j, 0:1, 0:1] for j in range(n_dp))

    for j in range(n_tp):
        hidden_copy(j).start()
    block_copy(0).start()
    rows_copy(0).start()
    more_copy(0).start()
    hidden_copy(0).wait()
    for k in range(PIECES):
        first_piece(k)
    lax.fori_loop(1, n_tp, next_quarter, 0)
    counts[dp] = jnp.full(counts.shape[1:], jnp.sum(loss_mask[...].astype(jnp.float32)), jnp.float32)
    pl.semaphore_wait(barrier, n_dp - 1 + 2 * len(others))
    for k in range(PIECES):
        y_copy(k).start()
    for i in range(2):
        ids_copy(i).start()
    for j in range(n_dp - 1):
        count_copy(j).start()

    top[...] = jnp.full_like(top, jnp.finfo(jnp.float32).min)
    total[...] = jnp.zeros_like(total)
    held[...] = jnp.full_like(held, -jnp.inf)
    target[...] = jnp.zeros_like(target)

    assert blocks > 11 and PIECES == 4
    lax.fori_loop(0, blocks, block, 0)
    fold(held[...], tile_at(own_tiles - 1))

    best = jnp.max(top[...], axis=0, keepdims=True)
    stats[0, tp, 0:1] = best
    stats[0, tp, 1:2] = jnp.sum(total[...] * jnp.exp(top[...] - best), axis=0, keepdims=True)
    for copy in stat_copies():
        copy.start()

    relay_copy(last).wait_recv()
    convert(across, last)
    for i in range(2):
        ids_copy(i).wait()
    for j in range(n_dp - 1):
        count_arrival(j).wait_recv()
    for i in range(batch):
        for side, (rows_of, marks) in enumerate(((labels, loss_mask), (ids.at[0], ids.at[1]))):
            at = slice(side * own + i * seq, side * own + (i + 1) * seq)
            label[:, at] = rows_of[i:i + 1, :] - first_row
            weight[:, at] = marks[i:i + 1, :].astype(jnp.float32)
    scale[...] = weight[...] / tokens_counted()
    for k in range(PIECES):
        for copy in (y_copy(k), beside_copy(k), core_copy(k), relay_copy(k)):
            copy.wait_send()
    for j in range(n_dp - 1):
        count_copy(j).wait_send()
    first_logits()
    for other in others:
        stat_arrival(0, other).wait_recv()
    for other in (tp,) + others:
        stat_arrival(1, other).wait_recv()
    for side in range(Y):
        tops = [stats[side, j, 0:1] for j in range(n_tp)]
        best = functools.reduce(jnp.maximum, tops)
        mass = sum(stats[side, j, 1:2] * jnp.exp(tops[j] - best) for j in range(n_tp))
        lse[:, side * own:(side + 1) * own] = best + jnp.log(mass)

    first_unit()

    computes = (compute_0, compute_1, compute_2, compute_3, compute_4)
    beats = len(computes)
    start = beats - 2
    done = beats * units - 1
    ticks = start + chunks + END_LAG
    assert done + 39 < ticks

    def tick(i, carry):
        u = i // beats
        kind = i % beats

        @pl.when(i == start)
        def _():
            settle(0)

        @pl.when(jnp.logical_not(inner))
        def _():
            end_step(jnp.maximum(i - start, 0))

        @pl.when(inner)
        def _():
            inner_step(jnp.maximum(i - start, 0))

        @pl.when((i > start) & (kind == start) & (u < units))
        def _():
            settle(u)

        for j, compute in enumerate(computes):
            pl.when((kind == j) & (u < units))(functools.partial(compute, u))

        events = ((1, dx_start), (5, dx_middle), (22, dx_finish), (24, lambda: level_next(0)), (26, lambda: level_next(1)),
                  (28, dh_own), (30, dh_partner), (32, lambda: level_next(2)), (36, lambda: level_next(3)), (39, dh_relay))
        for after, event in events:
            pl.when(i == done + after)(event)
        return carry

    lax.fori_loop(start, ticks, tick, 0)
    level_next(4)
    dh_finish()

    @pl.when(jnp.logical_not(inner))
    def _():
        for c in range(chunks - 2, chunks):
            up_copy(c).wait_send()
        for c in range(chunks - RING, chunks):
            mate_copy(c, out_rows(y, c)).wait_send()

    for i in range(2):
        theirs = out.at[pl.ds((1 - y) * half + i * (half // 2), half // 2)]
        pltpu.make_async_copy(theirs, theirs, mate_recv.at[i]).wait()
    for copy in stat_copies():
        copy.wait_send()
    for i in range(2):
        swap_copy(i).wait_send()
    cross_copy().wait_send()
    for i in range(2):
        share_copy(i).wait_send()
    pass_copy().wait_send()
    dh_copy().wait()
    for i in range(len(level_peers)):
        level_copy(i).wait_send()


def head_step(table, hidden, gain, bias, labels, loss_mask, n_dp, n_tp):
    own, width = hidden.shape
    tokens = Y * own
    shard = table.shape[0]
    half = shard // Y
    size = half // (UNITS * PER_UNIT)
    unit = size * PER_UNIT
    quarter = own // n_tp
    assert unit <= quarter and 2 * TILE <= width and unit * UNITS == half and size % 8 == 0 and unit % 32 == 0 and quarter == TILE
    assert shard % FORWARD_ROWS == 0
    f32 = jnp.float32
    b16 = jnp.bfloat16
    i32 = jnp.int32
    lanes = 128
    dma = pltpu.SemaphoreType.DMA
    vmem = pl.BlockSpec(memory_space=pltpu.VMEM)
    hbm = pl.BlockSpec(memory_space=pl.ANY)
    flops = 2 * width * (own * shard + half * (2 * tokens + 3 * own))
    return pl.pallas_call(
        functools.partial(head_kernel, n_dp, n_tp),
        out_shape=(
            jax.ShapeDtypeStruct((shard, width), f32),
            jax.ShapeDtypeStruct((half, width), f32),
            jax.ShapeDtypeStruct((own, width), b16),
            jax.ShapeDtypeStruct((8, width), f32)),
        in_specs=[hbm, hbm, vmem, vmem, vmem, vmem],
        out_specs=(hbm, hbm, hbm, vmem),
        scratch_shapes=[
            pltpu.VMEM((tokens, width), b16), pltpu.VMEM((width, tokens), b16),
            pltpu.VMEM((1, tokens), f32), pltpu.VMEM((1, tokens), f32), pltpu.VMEM((1, tokens), f32),
            pltpu.VMEM((1, tokens), i32), pltpu.VMEM((1, tokens), f32),
            pltpu.VMEM((quarter, width), f32), pltpu.VMEM((quarter, lanes), f32), pltpu.VMEM((quarter, width), f32),
            pltpu.VMEM((n_tp, quarter, width), f32), pltpu.VMEM((2, FORWARD_ROWS, width), b16),
            pltpu.VMEM((FORWARD_ROWS, TILE), f32),
            pltpu.VMEM((8, own), f32), pltpu.VMEM((8, own), f32),
            pltpu.VMEM((Y, n_tp, 2, own), f32), pltpu.VMEM((n_dp, 8, lanes), f32),
            pltpu.VMEM((2,) + labels.shape, i32),
            pltpu.VMEM((SLOTS, size, width), f32), pltpu.VMEM((SLOTS, size, width), f32), pltpu.VMEM((2, size, width), f32),
            pltpu.VMEM((unit, tokens), b16),
            pltpu.VMEM((2, unit, width), b16), pltpu.VMEM((2, unit, width), b16),
            pltpu.VMEM((unit, width), f32),
            pltpu.VMEM((n_tp, width, quarter), f32),
            pltpu.VMEM((2, width, quarter), f32), pltpu.VMEM((width, quarter), f32),
            pltpu.VMEM((5, 8, width), f32), pltpu.VMEM((5, 8, width), f32),
            dma((n_tp,)), dma((2,)), dma((2, PIECES)), dma((2, PIECES)), dma((2, PIECES)), dma((2, PIECES)),
            dma((2 * n_tp - 1,)), dma((Y, n_tp)), dma((n_dp - 1,)), dma((n_dp,)),
            dma((2, 2)),
            dma((RING,)), dma((SLOTS,)), dma((RING,)), dma((SLOTS,)), dma((RING,)), dma((SLOTS,)), dma((RING,)), dma((2,)),
            pltpu.SemaphoreType.REGULAR((2,)),
            dma((2,)), dma((RING,)), dma((1,)), dma((2,)), dma((2,)),
            dma((2, 2)), dma((2,)), dma((3,)), dma((3,)), dma((2, 5)),
        ],
        compiler_params=pltpu.CompilerParams(
            collective_id=0, has_side_effects=True, vmem_limit_bytes=VMEM_BYTES),
        cost_estimate=pl.CostEstimate(flops=flops, bytes_accessed=12 * half * width, transcendentals=half * tokens),
    )(table, hidden, gain, bias, labels, loss_mask)


def place_kernel(table_in, dh_in, sums, table_out, dh_out, loss, gain_out, bias_out, buf, dh_buf, in_sem, out_sem, dh_sem):
    size = buf.shape[1]
    count = table_in.shape[0] // size
    lag = PLACE_SLOTS // 2

    def read(i):
        return pltpu.make_async_copy(table_in.at[pl.ds(i * size, size)], buf.at[i % PLACE_SLOTS], in_sem.at[i % PLACE_SLOTS])

    def write(i):
        return pltpu.make_async_copy(buf.at[i % PLACE_SLOTS], table_out.at[pl.ds(i * size, size)], out_sem.at[i % PLACE_SLOTS])

    dh_read = pltpu.make_async_copy(dh_in, dh_buf, dh_sem.at[0])
    dh_write = pltpu.make_async_copy(dh_buf, dh_out, dh_sem.at[1])
    for i in range(count + lag):
        if i < count:
            if i >= PLACE_SLOTS:
                write(i - PLACE_SLOTS).wait()
            read(i).start()
        if i == 0:
            dh_read.start()
            loss[...] = sums[2:3, 0:1]
            gain_out[...] = sums[0:1, :]
            bias_out[...] = sums[1:2, :]
        if i == lag:
            dh_read.wait()
            dh_write.start()
        if i >= lag:
            read(i - lag).wait()
            write(i - lag).start()
    for i in range(count - PLACE_SLOTS, count):
        write(i).wait()
    dh_write.wait()


def place(table, dh, sums):
    f32 = jnp.float32
    dma = pltpu.SemaphoreType.DMA
    vmem = pl.BlockSpec(memory_space=pltpu.VMEM)
    hbm = pl.BlockSpec(memory_space=pltpu.HBM)
    width = table.shape[1]
    assert table.shape[0] % PLACE_ROWS == 0
    return pl.pallas_call(
        place_kernel,
        out_shape=(
            jax.ShapeDtypeStruct(table.shape, f32), jax.ShapeDtypeStruct(dh.shape, dh.dtype),
            jax.ShapeDtypeStruct((1, 1), f32), jax.ShapeDtypeStruct((1, width), f32), jax.ShapeDtypeStruct((1, width), f32)),
        in_specs=[hbm, hbm, vmem],
        out_specs=(hbm, hbm, vmem, vmem, vmem),
        scratch_shapes=[
            pltpu.VMEM((PLACE_SLOTS, PLACE_ROWS, width), f32), pltpu.VMEM(dh.shape, dh.dtype),
            dma((PLACE_SLOTS,)), dma((PLACE_SLOTS,)), dma((2,))],
        compiler_params=pltpu.CompilerParams(vmem_limit_bytes=VMEM_BYTES),
        cost_estimate=pl.CostEstimate(flops=0, bytes_accessed=8 * table.size + 4 * dh.size, transcendentals=0),
    )(table, dh, sums)


def solution(mesh):
    n_dp = mesh.shape['dp']
    n_tp = mesh.shape['tp']

    def device_step(hidden, table, labels, loss_mask, ln_gain, ln_bias):
        batch, seq, width = hidden.shape
        grad_table, _, grad_hidden, sums = head_step(
            table, hidden.reshape(batch * seq, width), ln_gain, ln_bias, labels, loss_mask, n_dp, n_tp)
        grad_table, grad_hidden, loss, grad_gain, grad_bias = place(grad_table, grad_hidden, sums)
        return (loss.reshape(()), grad_hidden.reshape(batch, seq, width), grad_table,
                grad_gain.reshape(width), grad_bias.reshape(width))

    specs_in = (P('dp', None, None), P('tp', None), P('dp', None), P('dp', None), P(None), P(None))
    specs_out = (P(), P('dp', None, None), P('tp', None), P(None), P(None))
    return jax.shard_map(device_step, mesh=mesh, in_specs=specs_in, out_specs=specs_out, check_vma=False)
```

```python
import functools

import jax
import jax.numpy as jnp
from jax import lax
from jax.experimental import pallas as pl
from jax.experimental.pallas import tpu as pltpu
from jax.sharding import PartitionSpec as P

LN_EPS = 1e-5
VOCAB = 50257
Z = 4
Y = 2
UNITS = 33
PER_UNIT = 6
SLOTS = 8
RING = 4
END_LAG = 6
TILE = 512
PIECES = 4
FORWARD_ROWS = 1056
PLACE_ROWS = 1056
PLACE_SLOTS = 12
COLUMNS = 256
VMEM_BYTES = 67043328
MESH = pl.DeviceIdType.MESH


def signal(barrier, **where):
    pl.semaphore_signal(barrier, inc=1, device_id=where, device_id_type=MESH)


def remote(src, dst, send_sem, recv_sem, **where):
    return pltpu.make_async_remote_copy(
        src_ref=src, dst_ref=dst, send_sem=send_sem, recv_sem=recv_sem, device_id=where, device_id_type=MESH)


def neighbours(tp):
    core = tp % 2
    partner = tp + 1 - 2 * core
    beside = tp + 2 - 4 * (tp // 2)
    return partner, beside, beside + 1 - 2 * core


def tile_at(t):
    return slice(t * TILE, (t + 1) * TILE)


def aligned(start, size):
    return pl.ds(pl.multiple_of(start, size), size)


def head_kernel(
        n_dp, n_tp, table, hidden, gain, bias, labels, loss_mask,
        out, part, dh, sums,
        x, x_t, lse, scale, weight, label, target, hat, inv, send_q,
        got, block_buf, held, top, total, stats, counts, ids,
        red, met, loc, q_t, rows_buf, more_buf, stage, dx_t, from_core, from_x, levels, arrived,
        hidden_sem, block_sem, y_sem, beside_sem, core_sem, relay_sem, stat_send, stat_recv, count_send, count_recv,
        ids_sem,
        up_send, up_recv, meet_send, meet_recv, down_send, down_recv, mate_send, mate_recv, credit,
        loc_sem, own_sem, part_sem, rows_sem, more_sem,
        swap_sem, cross_sem, share_send, share_recv, level_sem):
    own, width = hidden.shape
    tokens = Y * own
    shard = table.shape[0]
    half = shard // Y
    quarter = own // n_tp
    piece = quarter // PIECES
    batch, seq = labels.shape
    size = red.shape[1]
    chunks = half // size
    unit = size * PER_UNIT
    units = chunks // PER_UNIT
    block_rows = block_buf.shape[1]
    blocks = shard // block_rows
    last = PIECES - 1
    own_tiles, all_tiles, columns = own // TILE, tokens // TILE, width // COLUMNS

    dp = lax.axis_index('dp')
    tp = lax.axis_index('tp')
    y = dp % Y
    z = dp // Y
    core = tp % 2
    mate = dp + 1 - 2 * y
    partner, beside, across = neighbours(tp)
    others = (partner, beside, across)
    dp_others = [lax.rem(dp + j, n_dp) for j in range(1, n_dp)]
    z_mate = dp + Y - 2 * Y * (z % 2)
    z_far = dp + 2 * Y - 4 * Y * (z // 2)
    inner = (z == 1) | (z == 2)
    z_cross = dp + Y * (Z - 1 - 2 * z)
    first_row = tp * shard

    barrier = pltpu.get_barrier_semaphore()
    for other in dp_others:
        signal(barrier, dp=other)
    for other in others:
        signal(barrier, tp=other)
        signal(barrier, dp=mate, tp=other)

    def hidden_copy(j):
        q = lax.rem(tp + j, n_tp)
        at = aligned(q * quarter, quarter)
        return pltpu.make_async_copy(hidden.at[at], x.at[at], hidden_sem.at[j])

    def block_copy(b):
        return pltpu.make_async_copy(
            table.at[pl.ds(b * block_rows, block_rows)], block_buf.at[b % 2], block_sem.at[b % 2])

    def got_piece(q, k):
        return got.at[q, pl.ds(k * piece, piece)]

    def y_copy(k):
        return remote(send_q.at[pl.ds(k * piece, piece)], got_piece(tp, k), y_sem.at[0, k], y_sem.at[1, k], dp=mate)

    def beside_copy(k):
        return remote(got_piece(tp, k), got_piece(tp, k), beside_sem.at[0, k], beside_sem.at[1, k], tp=beside)

    def core_copy(k):
        return remote(got_piece(tp, k), got_piece(tp, k), core_sem.at[0, k], core_sem.at[1, k], tp=partner)

    def relay_copy(k):
        return remote(got_piece(beside, k), got_piece(beside, k), relay_sem.at[0, k], relay_sem.at[1, k], tp=partner)

    def count_copy(j):
        return remote(counts.at[dp], counts.at[dp], count_send.at[j], count_recv.at[dp], dp=dp_others[j])

    def count_arrival(j):
        other = dp_others[j]
        return remote(counts.at[other], counts.at[other], count_send.at[j], count_recv.at[other], dp=other)

    def ids_copy(i):
        return remote((labels, loss_mask)[i], ids.at[i], ids_sem.at[0, i], ids_sem.at[1, i], dp=mate)

    def row_of(ref):
        return ref[...].astype(jnp.float32)[None, :]

    def block_of(q, k):
        return aligned(q * quarter + k * piece, piece)

    def normalize(at):
        h = x[at, :].astype(jnp.float32)
        mean = jnp.mean(h, axis=-1, keepdims=True)
        centred = h - mean
        variance = jnp.mean(centred * centred, axis=-1, keepdims=True)
        inv_std = lax.rsqrt(variance + LN_EPS)
        x_hat = centred * inv_std
        normed = (x_hat * row_of(gain) + row_of(bias)).astype(jnp.bfloat16)
        x[at, :] = normed
        x_t[:, at] = normed.T
        return x_hat, inv_std, normed

    def first_piece(k):
        x_hat, inv_std, normed = normalize(block_of(tp, k))
        at = slice(k * piece, (k + 1) * piece)
        send_q[at, :] = normed.astype(jnp.float32)
        hat[at, :] = x_hat
        inv[at, :] = jnp.broadcast_to(inv_std, (piece, inv.shape[1]))

    def next_quarter(j, carry):
        hidden_copy(j).wait()
        for k in range(PIECES):
            normalize(block_of(lax.rem(tp + j, n_tp), k))
        return carry

    def convert(q, k):
        wide = got[q, aligned(k * piece, piece)]
        at = aligned(own + q * quarter + k * piece, piece)
        narrow = wide.astype(jnp.bfloat16)
        x[at, :] = narrow
        x_t[:, at] = narrow.T

    def fold(logits, at):
        logits = logits.reshape(block_rows // 8, 8, TILE)
        before = top[:, at]
        now = jnp.maximum(before, jnp.max(logits, axis=0))
        total[:, at] = total[:, at] * jnp.exp(before - now) + jnp.sum(jnp.exp(logits - now[None]), axis=0)
        top[:, at] = now

    def block(b, carry):
        block_copy(b).wait()

        @pl.when(b + 1 < blocks)
        def _():
            block_copy(b + 1).start()

        def spaced(first, count):
            d = jnp.maximum(b - first, 0)
            return (b >= first) & ((d < 2) | (d == 3) | (d == 5)) & (d < 2 * count - 1), jnp.minimum((d + 1) // 2, last)

        due, k_y = spaced(3, PIECES)

        @pl.when(due)
        def _():
            y_copy(k_y).wait_recv()
            beside_copy(k_y).start()
            core_copy(k_y).start()
            convert(tp, k_y)

        due, k_core = spaced(4, PIECES)

        @pl.when(due)
        def _():
            core_copy(k_core).wait_recv()
            convert(partner, k_core)

        due, k_x = spaced(6, PIECES)

        @pl.when(due)
        def _():
            beside_copy(k_x).wait_recv()
            relay_copy(k_x).start()
            convert(beside, k_x)

        due, k_relay = spaced(7, PIECES - 1)

        @pl.when(due)
        def _():
            relay_copy(k_relay).wait_recv()
            convert(across, k_relay)

        slot = b % 2
        row_ids = first_row + b * block_rows + lax.broadcasted_iota(jnp.int32, (block_rows, 1), 0)
        fold(held[...], tile_at(own_tiles - 1))
        for t in range(own_tiles):
            at = tile_at(t)
            logits = jnp.dot(block_buf[slot], x_t[:, at], preferred_element_type=jnp.float32)
            logits = jnp.where(row_ids < VOCAB, logits, -jnp.inf)
            if t + 1 < own_tiles:
                fold(logits, at)
            else:
                held[...] = logits
        return carry

    def stat_copies():
        where = [{'tp': other} for other in others] + [{'dp': mate}] + [{'dp': mate, 'tp': other} for other in others]
        return [remote(stats.at[0, tp], stats.at[int(i >= n_tp - 1), tp], stat_send.at[i], stat_recv.at[int(i >= n_tp - 1), tp],
                       **w) for i, w in enumerate(where)]

    def stat_arrival(side, other):
        return remote(stats.at[side, other], stats.at[side, other], stat_send.at[0], stat_recv.at[side, other], tp=partner)

    def part_rows(c):
        return part.at[pl.ds(c * size, size)]

    def out_rows(side, c):
        return out.at[pl.ds(side * half + c * size, size)]

    def fetch(c):
        return pltpu.make_async_copy(part_rows(c), loc.at[c % 2], loc_sem.at[c % 2])

    def up_copy(c):
        return remote(part_rows(c), red.at[c % SLOTS], up_send.at[c % RING], up_recv.at[c % SLOTS], dp=z_mate)

    def first_up_copy():
        return remote(stage.at[pl.ds(0, size)], red.at[0], up_send.at[0], up_recv.at[0], dp=z_mate)

    def meet_copy(c):
        return remote(red.at[c % SLOTS], met.at[c % SLOTS], meet_send.at[c % RING], meet_recv.at[c % SLOTS], dp=z_cross)

    def down_copy(c):
        return remote(met.at[c % SLOTS], out_rows(y, c), down_send.at[c % RING], down_recv.at[c % SLOTS], dp=z_mate)

    def mate_copy(c, src):
        return remote(src, out_rows(y, c), mate_send.at[c % RING], mate_recv.at[c // (chunks // 2)], dp=mate)

    def own_copy(c):
        return pltpu.make_async_copy(met.at[c % SLOTS], out_rows(y, c), own_sem.at[c % RING])

    def rows_copy(u):
        return pltpu.make_async_copy(table.at[pl.ds(y * half + u * unit, unit)], rows_buf.at[u % 2], rows_sem.at[u % 2])

    def more_copy(u):
        return pltpu.make_async_copy(
            table.at[pl.ds((1 - y) * half + u * unit, unit)], more_buf.at[u % 2], more_sem.at[u % 2])

    def part_copy(u):
        return pltpu.make_async_copy(stage, part.at[pl.ds(u * unit, unit)], part_sem.at[0])

    unit_iota = lax.broadcasted_iota(jnp.int32, (unit, 1), 0)

    def logits_of(table_rows, at):
        return jnp.dot(table_rows, x_t[:, at], preferred_element_type=jnp.float32)

    def grads(logits, row_ids, at):
        hit = row_ids == label[:, at]
        probs = jnp.where(row_ids + first_row < VOCAB, jnp.exp(logits - lse[:, at]), 0.0)
        q = ((probs - jnp.where(hit, 1.0, 0.0)) * scale[:, at]).astype(jnp.bfloat16)
        return q, jnp.where(hit, logits, 0.0)

    def dx_of(table_rows, q):
        return lax.dot_general(table_rows, q, (((0,), (0,)), ((), ())), preferred_element_type=jnp.float32)

    def add_dx(table_rows, q, t):
        dx_t[t] = dx_t[t] + dx_of(table_rows, q)

    def main_tile(u, t, logits=None):
        slot = u % 2
        at = tile_at(t)
        row_ids = y * half + u * unit + unit_iota
        is_first = logits is not None
        if not is_first:
            logits = logits_of(rows_buf[slot], at)
        q, hits = grads(logits, row_ids, at)
        q_t[:, at] = q
        target[:, at] = target[:, at] + jnp.sum(hits, axis=0, keepdims=True)
        if t < own_tiles and not is_first:
            add_dx(rows_buf[slot], q, t)

    def table_tile(n):
        at = slice(n * COLUMNS, (n + 1) * COLUMNS)
        stage[:, at] = jnp.dot(q_t[...], x[:, at], preferred_element_type=jnp.float32)

    def more_tile(u, t):
        theirs = (1 - y) * half + u * unit + unit_iota
        q, _ = grads(logits_of(more_buf[u % 2], tile_at(t)), theirs, tile_at(t))
        add_dx(more_buf[u % 2], q, t)

    few = (all_tiles - own_tiles) // 4

    def compute_0(u):
        rows_copy(u).wait()

        @pl.when(u + 1 < units)
        def _():
            rows_copy(u + 1).start()

        for t in list(range(own_tiles // 2)) + list(range(own_tiles, own_tiles + few)):
            main_tile(u, t)

    def compute_1(u):
        for t in list(range(own_tiles // 2, own_tiles)) + list(range(own_tiles + few, own_tiles + 2 * few)):
            main_tile(u, t)

    def compute_2(u):
        for t in range(own_tiles + 2 * few, all_tiles):
            main_tile(u, t)
        for n in range(columns):
            table_tile(n)
        part_copy(u).start()

    def early(t):
        return got.at[t // 2, pl.ds(0, unit), pl.ds(t % 2 * TILE, TILE)]

    def first_logits():
        rows_copy(0).wait()
        rows_copy(1).start()
        for t in range(all_tiles):
            early(t)[...] = logits_of(rows_buf[0], tile_at(t))

    def first_unit():
        for t in range(all_tiles):
            main_tile(0, t, early(t)[...])
        for n in range(columns):
            table_tile(n)
        part_copy(0).start()

    def first_dx():
        for t in range(own_tiles):
            dx_t[t] = dx_of(rows_buf[0], q_t[:, tile_at(t)])

    def compute_3(u):
        more_copy(u).wait()

        @pl.when(u + 1 < units)
        def _():
            more_copy(u + 1).start()

        for t in range(own_tiles // 2):
            more_tile(u, t)

    def compute_4(u):
        for t in range(own_tiles // 2, own_tiles):
            more_tile(u, t)

    def settle(u):
        part_copy(u).wait()

    def within(c):
        return (c >= 0) & (c < chunks)

    def take_credit(i, c):
        @pl.when(c >= SLOTS)
        def _():
            pl.semaphore_wait(credit.at[i], 1)

    def give_credit(i, c, other):
        @pl.when(c + SLOTS < chunks)
        def _():
            pl.semaphore_signal(credit.at[i], inc=1, device_id={'dp': other}, device_id_type=MESH)

    def end_step(t):
        @pl.when(t < chunks)
        def _():
            @pl.when(t >= 2)
            def _():
                up_copy(t - 2).wait_send()
            take_credit(0, t)

            @pl.when(t == 0)
            def _():
                first_up_copy().start()

            @pl.when(t > 0)
            def _():
                up_copy(t).start()

        c = t - END_LAG

        @pl.when(within(c))
        def _():
            down_copy(c).wait_recv()

            @pl.when(c >= RING)
            def _():
                mate_copy(c - RING, out_rows(y, c - RING)).wait_send()
            mate_copy(c, out_rows(y, c)).start()

    def inner_step(t):
        c = t - 2

        @pl.when(within(c))
        def _():
            slot = c % SLOTS
            up_copy(c).wait_recv()
            fetch(c).wait()
            red[slot] = red[slot] + loc[c % 2]
            take_credit(1, c)
            meet_copy(c).start()

        @pl.when(within(c + 1))
        def _():
            fetch(c + 1).start()

        c_met = t - 4

        @pl.when(within(c_met))
        def _():
            slot = c_met % SLOTS
            meet_copy(c_met).wait_recv()
            met[slot] = red[slot] + met[slot]
            down_copy(c_met).start()
            mate_copy(c_met, met.at[slot]).start()
            own_copy(c_met).start()
            meet_copy(c_met).wait_send()
            give_credit(0, c_met, z_mate)

        c_gone = t - 6

        @pl.when(within(c_gone))
        def _():
            own_copy(c_gone).wait()
            down_copy(c_gone).wait_send()
            mate_copy(c_gone, met.at[c_gone % SLOTS]).wait_send()
            give_credit(1, c_gone, z_cross)

    def swap_copy(i):
        return remote(dx_t.at[2 * i + 1 - core], from_core.at[i], swap_sem.at[0, i], swap_sem.at[1, i], tp=partner)

    def cross_copy():
        return remote(dx_t.at[beside], from_x, cross_sem.at[0], cross_sem.at[1], tp=beside)

    def share_copy(i):
        return remote(send_q, got.at[tp], share_send.at[i], share_recv.at[i], tp=others[i])

    def pass_copy():
        return remote(got.at[beside], got.at[beside], share_send.at[2], share_recv.at[2], tp=partner)

    def round_dh(q, ref):
        at = aligned(q * quarter, quarter)
        x[at, :] = ref.astype(jnp.bfloat16)

    def dh_own():
        round_dh(tp, send_q[...])

    def dh_partner():
        share_copy(0).wait_recv()
        round_dh(partner, got[partner])

    def dh_relay():
        share_copy(1).wait_recv()
        pass_copy().start()

    def dh_copy():
        return pltpu.make_async_copy(x.at[pl.ds(0, own)], dh, hidden_sem.at[0])

    def dh_finish():
        round_dh(beside, got[beside])
        pass_copy().wait_recv()
        round_dh(across, got[across])
        dh_copy().start()

    slab = 128

    def add_into(j, ref):
        def body(i, carry):
            at = aligned(i * slab, slab)
            dx_t[j, at] = dx_t[j, at] + ref[at]
            return carry
        lax.fori_loop(0, width // slab, body, 0)

    def dx_start():
        for i in range(2):
            swap_copy(i).start()

    def dx_middle():
        for i in range(2):
            swap_copy(i).wait_recv()
            add_into(2 * i + core, from_core.at[i])
        cross_copy().start()

    def dx_finish():
        cross_copy().wait_recv()
        add_into(tp, from_x)
        for i in range(width // slab):
            at = pl.ds(i * slab, slab)
            send_q[:, at] = dx_t[tp, at].T

        levels[0] = jnp.zeros(levels.shape[1:], jnp.float32)
        own_loss = weight[:, :own] * lse[:, :own] * (1.0 / n_tp) - weight[:, :own] * target[:, :own]
        loss_part = own_loss - weight[:, own:] * target[:, own:]
        levels[0, 2:3] = sum(loss_part[:, i * width:(i + 1) * width] for i in range(own // width))
        step = min(64, quarter)

        def token_block(i, carry):
            at = aligned(i * step, step)
            grad = send_q[at, :]
            x_hat = hat[at, :]
            levels[0, 0:1] = levels[0, 0:1] + jnp.sum(grad * x_hat, axis=0, keepdims=True)
            levels[0, 1:2] = levels[0, 1:2] + jnp.sum(grad, axis=0, keepdims=True)
            grad_hat = grad * row_of(gain)
            mean_grad = jnp.mean(grad_hat, axis=-1, keepdims=True)
            mean_proj = jnp.mean(grad_hat * x_hat, axis=-1, keepdims=True)
            send_q[at, :] = inv[at, 0:1] * (grad_hat - mean_grad - x_hat * mean_proj)
            return carry

        lax.fori_loop(0, quarter // step, token_block, 0)
        level_copy(0).start()
        for i in range(2):
            share_copy(i).start()

    level_peers = ({'tp': beside}, {'tp': partner}, {'dp': mate}, {'dp': z_mate}, {'dp': z_far})

    def level_copy(i):
        return remote(levels.at[i], arrived.at[i], level_sem.at[0, i], level_sem.at[1, i], **level_peers[i])

    def level_next(i):
        level_copy(i).wait_recv()
        merged = levels[i] + arrived[i]
        if i + 1 < len(level_peers):
            levels[i + 1] = merged
            level_copy(i + 1).start()
        else:
            sums[...] = merged
            sums[2:3] = jnp.broadcast_to(jnp.sum(merged[2:3], axis=-1, keepdims=True) / tokens_counted(), (1, width))

    def tokens_counted():
        return sum(counts[j, 0:1, 0:1] for j in range(n_dp))

    for j in range(n_tp):
        hidden_copy(j).start()
    block_copy(0).start()
    rows_copy(0).start()
    more_copy(0).start()
    hidden_copy(0).wait()
    for k in range(PIECES):
        first_piece(k)
    lax.fori_loop(1, n_tp, next_quarter, 0)
    counts[dp] = jnp.full(counts.shape[1:], jnp.sum(loss_mask[...].astype(jnp.float32)), jnp.float32)
    pl.semaphore_wait(barrier, n_dp - 1 + 2 * len(others))
    for k in range(PIECES):
        y_copy(k).start()
    for i in range(2):
        ids_copy(i).start()
    for j in range(n_dp - 1):
        count_copy(j).start()

    top[...] = jnp.full_like(top, jnp.finfo(jnp.float32).min)
    total[...] = jnp.zeros_like(total)
    held[...] = jnp.full_like(held, -jnp.inf)
    target[...] = jnp.zeros_like(target)

    assert blocks > 11 and PIECES == 4
    lax.fori_loop(0, blocks, block, 0)
    fold(held[...], tile_at(own_tiles - 1))

    best = jnp.max(top[...], axis=0, keepdims=True)
    stats[0, tp, 0:1] = best
    stats[0, tp, 1:2] = jnp.sum(total[...] * jnp.exp(top[...] - best), axis=0, keepdims=True)
    for copy in stat_copies():
        copy.start()

    relay_copy(last).wait_recv()
    convert(across, last)
    for i in range(2):
        ids_copy(i).wait()
    for j in range(n_dp - 1):
        count_arrival(j).wait_recv()
    for i in range(batch):
        for side, (rows_of, marks) in enumerate(((labels, loss_mask), (ids.at[0], ids.at[1]))):
            at = slice(side * own + i * seq, side * own + (i + 1) * seq)
            label[:, at] = rows_of[i:i + 1, :] - first_row
            weight[:, at] = marks[i:i + 1, :].astype(jnp.float32)
    scale[...] = weight[...] / tokens_counted()
    for k in range(PIECES):
        for copy in (y_copy(k), beside_copy(k), core_copy(k), relay_copy(k)):
            copy.wait_send()
    for j in range(n_dp - 1):
        count_copy(j).wait_send()
    first_logits()
    for other in others:
        stat_arrival(0, other).wait_recv()
    for other in (tp,) + others:
        stat_arrival(1, other).wait_recv()
    for side in range(Y):
        tops = [stats[side, j, 0:1] for j in range(n_tp)]
        best = functools.reduce(jnp.maximum, tops)
        mass = sum(stats[side, j, 1:2] * jnp.exp(tops[j] - best) for j in range(n_tp))
        lse[:, side * own:(side + 1) * own] = best + jnp.log(mass)

    first_unit()

    computes = (compute_0, compute_1, compute_2, compute_3, compute_4)
    beats = len(computes)
    start = beats - 2
    done = beats * units - 1
    ticks = start + chunks + END_LAG
    assert done + 39 < ticks

    def tick(i, carry):
        u = i // beats
        kind = i % beats

        @pl.when(i == start + 1)
        def _():
            settle(0)

        @pl.when(jnp.logical_not(inner))
        def _():
            end_step(jnp.maximum(i - start, 0))

        @pl.when(inner)
        def _():
            inner_step(jnp.maximum(i - start, 0))

        @pl.when(i == start)
        def _():
            first_dx()

        @pl.when((i > start) & (kind == start) & (u < units))
        def _():
            settle(u)

        for j, compute in enumerate(computes):
            pl.when((kind == j) & (u < units))(functools.partial(compute, u))

        events = ((1, dx_start), (5, dx_middle), (22, dx_finish), (24, lambda: level_next(0)), (26, lambda: level_next(1)),
                  (28, dh_own), (30, dh_partner), (32, lambda: level_next(2)), (36, lambda: level_next(3)), (39, dh_relay))
        for after, event in events:
            pl.when(i == done + after)(event)
        return carry

    lax.fori_loop(start, ticks, tick, 0)
    level_next(4)
    dh_finish()

    @pl.when(jnp.logical_not(inner))
    def _():
        for c in range(chunks - 2, chunks):
            up_copy(c).wait_send()
        for c in range(chunks - RING, chunks):
            mate_copy(c, out_rows(y, c)).wait_send()

    for i in range(2):
        theirs = out.at[pl.ds((1 - y) * half + i * (half // 2), half // 2)]
        pltpu.make_async_copy(theirs, theirs, mate_recv.at[i]).wait()
    for copy in stat_copies():
        copy.wait_send()
    for i in range(2):
        swap_copy(i).wait_send()
    cross_copy().wait_send()
    for i in range(2):
        share_copy(i).wait_send()
    pass_copy().wait_send()
    dh_copy().wait()
    for i in range(len(level_peers)):
        level_copy(i).wait_send()


def head_step(table, hidden, gain, bias, labels, loss_mask, n_dp, n_tp):
    own, width = hidden.shape
    tokens = Y * own
    shard = table.shape[0]
    half = shard // Y
    size = half // (UNITS * PER_UNIT)
    unit = size * PER_UNIT
    quarter = own // n_tp
    assert unit <= quarter and 2 * TILE <= width and unit * UNITS == half and size % 8 == 0 and unit % 32 == 0 and quarter == TILE
    assert shard % FORWARD_ROWS == 0
    f32 = jnp.float32
    b16 = jnp.bfloat16
    i32 = jnp.int32
    lanes = 128
    dma = pltpu.SemaphoreType.DMA
    vmem = pl.BlockSpec(memory_space=pltpu.VMEM)
    hbm = pl.BlockSpec(memory_space=pl.ANY)
    flops = 2 * width * (own * shard + half * (2 * tokens + 3 * own))
    return pl.pallas_call(
        functools.partial(head_kernel, n_dp, n_tp),
        out_shape=(
            jax.ShapeDtypeStruct((shard, width), f32),
            jax.ShapeDtypeStruct((half, width), f32),
            jax.ShapeDtypeStruct((own, width), b16),
            jax.ShapeDtypeStruct((8, width), f32)),
        in_specs=[hbm, hbm, vmem, vmem, vmem, vmem],
        out_specs=(hbm, hbm, hbm, vmem),
        scratch_shapes=[
            pltpu.VMEM((tokens, width), b16), pltpu.VMEM((width, tokens), b16),
            pltpu.VMEM((1, tokens), f32), pltpu.VMEM((1, tokens), f32), pltpu.VMEM((1, tokens), f32),
            pltpu.VMEM((1, tokens), i32), pltpu.VMEM((1, tokens), f32),
            pltpu.VMEM((quarter, width), f32), pltpu.VMEM((quarter, lanes), f32), pltpu.VMEM((quarter, width), f32),
            pltpu.VMEM((n_tp, quarter, width), f32), pltpu.VMEM((2, FORWARD_ROWS, width), b16),
            pltpu.VMEM((FORWARD_ROWS, TILE), f32),
            pltpu.VMEM((8, own), f32), pltpu.VMEM((8, own), f32),
            pltpu.VMEM((Y, n_tp, 2, own), f32), pltpu.VMEM((n_dp, 8, lanes), f32),
            pltpu.VMEM((2,) + labels.shape, i32),
            pltpu.VMEM((SLOTS, size, width), f32), pltpu.VMEM((SLOTS, size, width), f32), pltpu.VMEM((2, size, width), f32),
            pltpu.VMEM((unit, tokens), b16),
            pltpu.VMEM((2, unit, width), b16), pltpu.VMEM((2, unit, width), b16),
            pltpu.VMEM((unit, width), f32),
            pltpu.VMEM((n_tp, width, quarter), f32),
            pltpu.VMEM((2, width, quarter), f32), pltpu.VMEM((width, quarter), f32),
            pltpu.VMEM((5, 8, width), f32), pltpu.VMEM((5, 8, width), f32),
            dma((n_tp,)), dma((2,)), dma((2, PIECES)), dma((2, PIECES)), dma((2, PIECES)), dma((2, PIECES)),
            dma((2 * n_tp - 1,)), dma((Y, n_tp)), dma((n_dp - 1,)), dma((n_dp,)),
            dma((2, 2)),
            dma((RING,)), dma((SLOTS,)), dma((RING,)), dma((SLOTS,)), dma((RING,)), dma((SLOTS,)), dma((RING,)), dma((2,)),
            pltpu.SemaphoreType.REGULAR((2,)),
            dma((2,)), dma((RING,)), dma((1,)), dma((2,)), dma((2,)),
            dma((2, 2)), dma((2,)), dma((3,)), dma((3,)), dma((2, 5)),
        ],
        compiler_params=pltpu.CompilerParams(
            collective_id=0, has_side_effects=True, vmem_limit_bytes=VMEM_BYTES),
        cost_estimate=pl.CostEstimate(flops=flops, bytes_accessed=12 * half * width, transcendentals=half * tokens),
    )(table, hidden, gain, bias, labels, loss_mask)


def place_kernel(table_in, dh_in, sums, table_out, dh_out, loss, gain_out, bias_out, buf, dh_buf, in_sem, out_sem, dh_sem):
    size = buf.shape[1]
    count = table_in.shape[0] // size
    lag = PLACE_SLOTS // 2

    def read(i):
        return pltpu.make_async_copy(table_in.at[pl.ds(i * size, size)], buf.at[i % PLACE_SLOTS], in_sem.at[i % PLACE_SLOTS])

    def write(i):
        return pltpu.make_async_copy(buf.at[i % PLACE_SLOTS], table_out.at[pl.ds(i * size, size)], out_sem.at[i % PLACE_SLOTS])

    dh_read = pltpu.make_async_copy(dh_in, dh_buf, dh_sem.at[0])
    dh_write = pltpu.make_async_copy(dh_buf, dh_out, dh_sem.at[1])
    for i in range(count + lag):
        if i < count:
            if i >= PLACE_SLOTS:
                write(i - PLACE_SLOTS).wait()
            read(i).start()
        if i == 0:
            dh_read.start()
            loss[...] = sums[2:3, 0:1]
            gain_out[...] = sums[0:1, :]
            bias_out[...] = sums[1:2, :]
        if i == lag:
            dh_read.wait()
            dh_write.start()
        if i >= lag:
            read(i - lag).wait()
            write(i - lag).start()
    for i in range(count - PLACE_SLOTS, count):
        write(i).wait()
    dh_write.wait()


def place(table, dh, sums):
    f32 = jnp.float32
    dma = pltpu.SemaphoreType.DMA
    vmem = pl.BlockSpec(memory_space=pltpu.VMEM)
    hbm = pl.BlockSpec(memory_space=pltpu.HBM)
    width = table.shape[1]
    assert table.shape[0] % PLACE_ROWS == 0
    return pl.pallas_call(
        place_kernel,
        out_shape=(
            jax.ShapeDtypeStruct(table.shape, f32), jax.ShapeDtypeStruct(dh.shape, dh.dtype),
            jax.ShapeDtypeStruct((1, 1), f32), jax.ShapeDtypeStruct((1, width), f32), jax.ShapeDtypeStruct((1, width), f32)),
        in_specs=[hbm, hbm, vmem],
        out_specs=(hbm, hbm, vmem, vmem, vmem),
        scratch_shapes=[
            pltpu.VMEM((PLACE_SLOTS, PLACE_ROWS, width), f32), pltpu.VMEM(dh.shape, dh.dtype),
            dma((PLACE_SLOTS,)), dma((PLACE_SLOTS,)), dma((2,))],
        compiler_params=pltpu.CompilerParams(vmem_limit_bytes=VMEM_BYTES),
        cost_estimate=pl.CostEstimate(flops=0, bytes_accessed=8 * table.size + 4 * dh.size, transcendentals=0),
    )(table, dh, sums)


def solution(mesh):
    n_dp = mesh.shape['dp']
    n_tp = mesh.shape['tp']

    def device_step(hidden, table, labels, loss_mask, ln_gain, ln_bias):
        batch, seq, width = hidden.shape
        grad_table, _, grad_hidden, sums = head_step(
            table, hidden.reshape(batch * seq, width), ln_gain, ln_bias, labels, loss_mask, n_dp, n_tp)
        grad_table, grad_hidden, loss, grad_gain, grad_bias = place(grad_table, grad_hidden, sums)
        return (loss.reshape(()), grad_hidden.reshape(batch, seq, width), grad_table,
                grad_gain.reshape(width), grad_bias.reshape(width))

    specs_in = (P('dp', None, None), P('tp', None), P('dp', None), P('dp', None), P(None), P(None))
    specs_out = (P(), P('dp', None, None), P('tp', None), P(None), P(None))
    return jax.shard_map(device_step, mesh=mesh, in_specs=specs_in, out_specs=specs_out, check_vma=False)
```

```python
import functools

import jax
import jax.numpy as jnp
from jax import lax
from jax.experimental import pallas as pl
from jax.experimental.pallas import tpu as pltpu
from jax.sharding import PartitionSpec as P

LN_EPS = 1e-5
VOCAB = 50257
Z = 4
Y = 2
UNITS = 33
PER_UNIT = 6
SLOTS = 8
RING = 4
END_LAG = 6
TILE = 512
PIECES = 4
FORWARD_ROWS = 1056
PLACE_ROWS = 1056
PLACE_SLOTS = 12
COLUMNS = 256
VMEM_BYTES = 67043328
MESH = pl.DeviceIdType.MESH


def signal(barrier, **where):
    pl.semaphore_signal(barrier, inc=1, device_id=where, device_id_type=MESH)


def remote(src, dst, send_sem, recv_sem, **where):
    return pltpu.make_async_remote_copy(
        src_ref=src, dst_ref=dst, send_sem=send_sem, recv_sem=recv_sem, device_id=where, device_id_type=MESH)


def neighbours(tp):
    core = tp % 2
    partner = tp + 1 - 2 * core
    beside = tp + 2 - 4 * (tp // 2)
    return partner, beside, beside + 1 - 2 * core


def tile_at(t):
    return slice(t * TILE, (t + 1) * TILE)


def aligned(start, size):
    return pl.ds(pl.multiple_of(start, size), size)


def head_kernel(
        n_dp, n_tp, table, hidden, gain_in, bias_in, labels_in, mask_in,
        out, part, dh, sums_out,
        gain, bias, labels, loss_mask, sums,
        x, x_t, lse, scale, weight, label, target, hat, inv, send_q,
        got, block_buf, held, top, total, stats, counts, ids,
        red, met, loc, q_t, rows_buf, more_buf, stage, dx_t, from_core, from_x, levels, arrived,
        small_sem, piece_sem, hidden_sem, block_sem, y_sem, beside_sem, core_sem, relay_sem, stat_send, stat_recv, count_send, count_recv,
        ids_sem,
        up_send, up_recv, meet_send, meet_recv, down_send, down_recv, mate_send, mate_recv, credit,
        loc_sem, own_sem, part_sem, rows_sem, more_sem,
        swap_sem, cross_sem, share_send, share_recv, level_sem):
    own, width = hidden.shape
    tokens = Y * own
    shard = table.shape[0]
    half = shard // Y
    quarter = own // n_tp
    piece = quarter // PIECES
    batch, seq = labels.shape
    size = red.shape[1]
    chunks = half // size
    unit = size * PER_UNIT
    units = chunks // PER_UNIT
    block_rows = block_buf.shape[1]
    blocks = shard // block_rows
    last = PIECES - 1
    own_tiles, all_tiles, columns = own // TILE, tokens // TILE, width // COLUMNS

    dp = lax.axis_index('dp')
    tp = lax.axis_index('tp')
    y = dp % Y
    z = dp // Y
    core = tp % 2
    mate = dp + 1 - 2 * y
    partner, beside, across = neighbours(tp)
    others = (partner, beside, across)
    dp_others = [lax.rem(dp + j, n_dp) for j in range(1, n_dp)]
    z_mate = dp + Y - 2 * Y * (z % 2)
    z_far = dp + 2 * Y - 4 * Y * (z // 2)
    inner = (z == 1) | (z == 2)
    z_cross = dp + Y * (Z - 1 - 2 * z)
    first_row = tp * shard

    barrier = pltpu.get_barrier_semaphore()
    for other in dp_others:
        signal(barrier, dp=other)
    for other in others:
        signal(barrier, tp=other)
        signal(barrier, dp=mate, tp=other)

    small_copies = [pltpu.make_async_copy(src, dst, small_sem.at[i]) for i, (src, dst) in enumerate((
        (gain_in, gain), (bias_in, bias), (labels_in, labels), (mask_in, loss_mask), (sums, sums_out)))]

    def piece_copy(k):
        at = block_of(tp, k)
        return pltpu.make_async_copy(hidden.at[at], x.at[at], piece_sem.at[k])

    def hidden_copy(j):
        q = lax.rem(tp + j, n_tp)
        at = aligned(q * quarter, quarter)
        return pltpu.make_async_copy(hidden.at[at], x.at[at], hidden_sem.at[j])

    def block_copy(b):
        return pltpu.make_async_copy(
            table.at[pl.ds(b * block_rows, block_rows)], block_buf.at[b % 2], block_sem.at[b % 2])

    def got_piece(q, k):
        return got.at[q, pl.ds(k * piece, piece)]

    def y_copy(k):
        return remote(send_q.at[pl.ds(k * piece, piece)], got_piece(tp, k), y_sem.at[0, k], y_sem.at[1, k], dp=mate)

    def beside_copy(k):
        return remote(got_piece(tp, k), got_piece(tp, k), beside_sem.at[0, k], beside_sem.at[1, k], tp=beside)

    def core_copy(k):
        return remote(got_piece(tp, k), got_piece(tp, k), core_sem.at[0, k], core_sem.at[1, k], tp=partner)

    def relay_copy(k):
        return remote(got_piece(beside, k), got_piece(beside, k), relay_sem.at[0, k], relay_sem.at[1, k], tp=partner)

    def count_copy(j):
        return remote(counts.at[dp], counts.at[dp], count_send.at[j], count_recv.at[dp], dp=dp_others[j])

    def count_arrival(j):
        other = dp_others[j]
        return remote(counts.at[other], counts.at[other], count_send.at[j], count_recv.at[other], dp=other)

    def ids_copy(i):
        return remote((labels, loss_mask)[i], ids.at[i], ids_sem.at[0, i], ids_sem.at[1, i], dp=mate)

    def row_of(ref):
        return ref[...].astype(jnp.float32)[None, :]

    def block_of(q, k):
        return aligned(q * quarter + k * piece, piece)

    def normalize(at):
        h = x[at, :].astype(jnp.float32)
        mean = jnp.mean(h, axis=-1, keepdims=True)
        centred = h - mean
        variance = jnp.mean(centred * centred, axis=-1, keepdims=True)
        inv_std = lax.rsqrt(variance + LN_EPS)
        x_hat = centred * inv_std
        normed = (x_hat * row_of(gain) + row_of(bias)).astype(jnp.bfloat16)
        x[at, :] = normed
        x_t[:, at] = normed.T
        return x_hat, inv_std, normed

    def first_piece(k):
        x_hat, inv_std, normed = normalize(block_of(tp, k))
        at = slice(k * piece, (k + 1) * piece)
        send_q[at, :] = normed.astype(jnp.float32)
        hat[at, :] = x_hat
        inv[at, :] = jnp.broadcast_to(inv_std, (piece, inv.shape[1]))

    def next_quarter(j, carry):
        hidden_copy(j).wait()
        for k in range(PIECES):
            normalize(block_of(lax.rem(tp + j, n_tp), k))
        return carry

    def convert(q, k):
        wide = got[q, aligned(k * piece, piece)]
        at = aligned(own + q * quarter + k * piece, piece)
        narrow = wide.astype(jnp.bfloat16)
        x[at, :] = narrow
        x_t[:, at] = narrow.T

    def fold(logits, at):
        logits = logits.reshape(block_rows // 8, 8, TILE)
        before = top[:, at]
        now = jnp.maximum(before, jnp.max(logits, axis=0))
        total[:, at] = total[:, at] * jnp.exp(before - now) + jnp.sum(jnp.exp(logits - now[None]), axis=0)
        top[:, at] = now

    def block(b, carry):
        block_copy(b).wait()

        @pl.when(b + 1 < blocks)
        def _():
            block_copy(b + 1).start()

        def spaced(first, count):
            d = jnp.maximum(b - first, 0)
            return (b >= first) & ((d < 2) | (d == 3) | (d == 5)) & (d < 2 * count - 1), jnp.minimum((d + 1) // 2, last)

        due, k_y = spaced(3, PIECES)

        @pl.when(due)
        def _():
            y_copy(k_y).wait_recv()
            beside_copy(k_y).start()
            core_copy(k_y).start()
            convert(tp, k_y)

        due, k_core = spaced(4, PIECES)

        @pl.when(due)
        def _():
            core_copy(k_core).wait_recv()
            convert(partner, k_core)

        due, k_x = spaced(6, PIECES)

        @pl.when(due)
        def _():
            beside_copy(k_x).wait_recv()
            relay_copy(k_x).start()
            convert(beside, k_x)

        due, k_relay = spaced(7, PIECES - 1)

        @pl.when(due)
        def _():
            relay_copy(k_relay).wait_recv()
            convert(across, k_relay)

        slot = b % 2
        row_ids = first_row + b * block_rows + lax.broadcasted_iota(jnp.int32, (block_rows, 1), 0)
        fold(held[...], tile_at(own_tiles - 1))
        for t in range(own_tiles):
            at = tile_at(t)
            logits = jnp.dot(block_buf[slot], x_t[:, at], preferred_element_type=jnp.float32)
            logits = jnp.where(row_ids < VOCAB, logits, -jnp.inf)
            if t + 1 < own_tiles:
                fold(logits, at)
            else:
                held[...] = logits
        return carry

    def stat_copies():
        where = [{'tp': other} for other in others] + [{'dp': mate}] + [{'dp': mate, 'tp': other} for other in others]
        return [remote(stats.at[0, tp], stats.at[int(i >= n_tp - 1), tp], stat_send.at[i], stat_recv.at[int(i >= n_tp - 1), tp],
                       **w) for i, w in enumerate(where)]

    def stat_arrival(side, other):
        return remote(stats.at[side, other], stats.at[side, other], stat_send.at[0], stat_recv.at[side, other], tp=partner)

    def part_rows(c):
        return part.at[pl.ds(c * size, size)]

    def out_rows(side, c):
        return out.at[pl.ds(side * half + c * size, size)]

    def fetch(c):
        return pltpu.make_async_copy(part_rows(c), loc.at[c % 2], loc_sem.at[c % 2])

    def up_copy(c):
        return remote(part_rows(c), red.at[c % SLOTS], up_send.at[c % RING], up_recv.at[c % SLOTS], dp=z_mate)

    def first_up_copy():
        return remote(stage.at[pl.ds(0, size)], red.at[0], up_send.at[0], up_recv.at[0], dp=z_mate)

    def meet_copy(c):
        return remote(red.at[c % SLOTS], met.at[c % SLOTS], meet_send.at[c % RING], meet_recv.at[c % SLOTS], dp=z_cross)

    def down_copy(c):
        return remote(met.at[c % SLOTS], out_rows(y, c), down_send.at[c % RING], down_recv.at[c % SLOTS], dp=z_mate)

    def mate_copy(c, src):
        return remote(src, out_rows(y, c), mate_send.at[c % RING], mate_recv.at[c // (chunks // 2)], dp=mate)

    def own_copy(c):
        return pltpu.make_async_copy(met.at[c % SLOTS], out_rows(y, c), own_sem.at[c % RING])

    def rows_copy(u):
        return pltpu.make_async_copy(table.at[pl.ds(y * half + u * unit, unit)], rows_buf.at[u % 2], rows_sem.at[u % 2])

    def more_copy(u):
        return pltpu.make_async_copy(
            table.at[pl.ds((1 - y) * half + u * unit, unit)], more_buf.at[u % 2], more_sem.at[u % 2])

    def part_copy(u):
        return pltpu.make_async_copy(stage, part.at[pl.ds(u * unit, unit)], part_sem.at[0])

    unit_iota = lax.broadcasted_iota(jnp.int32, (unit, 1), 0)

    def logits_of(table_rows, at):
        return jnp.dot(table_rows, x_t[:, at], preferred_element_type=jnp.float32)

    def grads(logits, row_ids, at):
        hit = row_ids == label[:, at]
        probs = jnp.where(row_ids + first_row < VOCAB, jnp.exp(logits - lse[:, at]), 0.0)
        q = ((probs - jnp.where(hit, 1.0, 0.0)) * scale[:, at]).astype(jnp.bfloat16)
        return q, jnp.where(hit, logits, 0.0)

    def dx_of(table_rows, q):
        return lax.dot_general(table_rows, q, (((0,), (0,)), ((), ())), preferred_element_type=jnp.float32)

    def add_dx(table_rows, q, t):
        dx_t[t] = dx_t[t] + dx_of(table_rows, q)

    def main_tile(u, t, logits=None):
        slot = u % 2
        at = tile_at(t)
        row_ids = y * half + u * unit + unit_iota
        is_first = logits is not None
        if not is_first:
            logits = logits_of(rows_buf[slot], at)
        q, hits = grads(logits, row_ids, at)
        q_t[:, at] = q
        target[:, at] = target[:, at] + jnp.sum(hits, axis=0, keepdims=True)
        if t < own_tiles and not is_first:
            add_dx(rows_buf[slot], q, t)

    def table_tile(n):
        at = slice(n * COLUMNS, (n + 1) * COLUMNS)
        stage[:, at] = jnp.dot(q_t[...], x[:, at], preferred_element_type=jnp.float32)

    def more_tile(u, t):
        theirs = (1 - y) * half + u * unit + unit_iota
        q, _ = grads(logits_of(more_buf[u % 2], tile_at(t)), theirs, tile_at(t))
        add_dx(more_buf[u % 2], q, t)

    few = (all_tiles - own_tiles) // 4

    def compute_0(u):
        rows_copy(u).wait()

        @pl.when(u + 1 < units)
        def _():
            rows_copy(u + 1).start()

        for t in list(range(own_tiles // 2)) + list(range(own_tiles, own_tiles + few)):
            main_tile(u, t)

    def compute_1(u):
        for t in list(range(own_tiles // 2, own_tiles)) + list(range(own_tiles + few, own_tiles + 2 * few)):
            main_tile(u, t)

    def compute_2(u):
        for t in range(own_tiles + 2 * few, all_tiles):
            main_tile(u, t)
        for n in range(columns):
            table_tile(n)
        part_copy(u).start()

    def early(t):
        return got.at[t // 2, pl.ds(0, unit), pl.ds(t % 2 * TILE, TILE)]

    def first_logits():
        rows_copy(0).wait()
        rows_copy(1).start()
        for t in range(all_tiles):
            early(t)[...] = logits_of(rows_buf[0], tile_at(t))

    def first_unit():
        for t in range(all_tiles):
            main_tile(0, t, early(t)[...])
        for n in range(columns):
            table_tile(n)
        part_copy(0).start()

    def first_dx():
        for t in range(own_tiles):
            dx_t[t] = dx_of(rows_buf[0], q_t[:, tile_at(t)])

    def compute_3(u):
        more_copy(u).wait()

        @pl.when(u + 1 < units)
        def _():
            more_copy(u + 1).start()

        for t in range(own_tiles // 2):
            more_tile(u, t)

    def compute_4(u):
        for t in range(own_tiles // 2, own_tiles):
            more_tile(u, t)

    def settle(u):
        part_copy(u).wait()

    def within(c):
        return (c >= 0) & (c < chunks)

    def take_credit(i, c):
        @pl.when(c >= SLOTS)
        def _():
            pl.semaphore_wait(credit.at[i], 1)

    def give_credit(i, c, other):
        @pl.when(c + SLOTS < chunks)
        def _():
            pl.semaphore_signal(credit.at[i], inc=1, device_id={'dp': other}, device_id_type=MESH)

    def end_step(t):
        @pl.when(t < chunks)
        def _():
            @pl.when(t >= 2)
            def _():
                up_copy(t - 2).wait_send()
            take_credit(0, t)

            @pl.when(t == 0)
            def _():
                first_up_copy().start()

            @pl.when(t > 0)
            def _():
                up_copy(t).start()

        c = t - END_LAG

        @pl.when(within(c))
        def _():
            down_copy(c).wait_recv()

            @pl.when(c >= RING)
            def _():
                mate_copy(c - RING, out_rows(y, c - RING)).wait_send()
            mate_copy(c, out_rows(y, c)).start()

    def inner_step(t):
        c = t - 2

        @pl.when(within(c))
        def _():
            slot = c % SLOTS
            up_copy(c).wait_recv()
            fetch(c).wait()
            red[slot] = red[slot] + loc[c % 2]
            take_credit(1, c)
            meet_copy(c).start()

        @pl.when(within(c + 1))
        def _():
            fetch(c + 1).start()

        c_met = t - 4

        @pl.when(within(c_met))
        def _():
            slot = c_met % SLOTS
            meet_copy(c_met).wait_recv()
            met[slot] = red[slot] + met[slot]
            down_copy(c_met).start()
            mate_copy(c_met, met.at[slot]).start()
            own_copy(c_met).start()
            meet_copy(c_met).wait_send()
            give_credit(0, c_met, z_mate)

        c_gone = t - 6

        @pl.when(within(c_gone))
        def _():
            own_copy(c_gone).wait()
            down_copy(c_gone).wait_send()
            mate_copy(c_gone, met.at[c_gone % SLOTS]).wait_send()
            give_credit(1, c_gone, z_cross)

    def swap_copy(i):
        return remote(dx_t.at[2 * i + 1 - core], from_core.at[i], swap_sem.at[0, i], swap_sem.at[1, i], tp=partner)

    def cross_copy():
        return remote(dx_t.at[beside], from_x, cross_sem.at[0], cross_sem.at[1], tp=beside)

    def share_copy(i):
        return remote(send_q, got.at[tp], share_send.at[i], share_recv.at[i], tp=others[i])

    def pass_copy():
        return remote(got.at[beside], got.at[beside], share_send.at[2], share_recv.at[2], tp=partner)

    def round_dh(q, ref):
        at = aligned(q * quarter, quarter)
        x[at, :] = ref.astype(jnp.bfloat16)

    def dh_own():
        round_dh(tp, send_q[...])

    def dh_partner():
        share_copy(0).wait_recv()
        round_dh(partner, got[partner])

    def dh_relay():
        share_copy(1).wait_recv()
        pass_copy().start()

    def dh_copy():
        return pltpu.make_async_copy(x.at[pl.ds(0, own)], dh, hidden_sem.at[0])

    def dh_finish():
        round_dh(beside, got[beside])
        pass_copy().wait_recv()
        round_dh(across, got[across])
        dh_copy().start()

    slab = 128

    def add_into(j, ref):
        def body(i, carry):
            at = aligned(i * slab, slab)
            dx_t[j, at] = dx_t[j, at] + ref[at]
            return carry
        lax.fori_loop(0, width // slab, body, 0)

    def dx_start():
        for i in range(2):
            swap_copy(i).start()

    def dx_middle():
        for i in range(2):
            swap_copy(i).wait_recv()
            add_into(2 * i + core, from_core.at[i])
        cross_copy().start()

    def dx_finish():
        cross_copy().wait_recv()
        add_into(tp, from_x)
        for i in range(width // slab):
            at = pl.ds(i * slab, slab)
            send_q[:, at] = dx_t[tp, at].T

        levels[0] = jnp.zeros(levels.shape[1:], jnp.float32)
        own_loss = weight[:, :own] * lse[:, :own] * (1.0 / n_tp) - weight[:, :own] * target[:, :own]
        loss_part = own_loss - weight[:, own:] * target[:, own:]
        levels[0, 2:3] = sum(loss_part[:, i * width:(i + 1) * width] for i in range(own // width))
        step = min(64, quarter)

        def token_block(i, carry):
            at = aligned(i * step, step)
            grad = send_q[at, :]
            x_hat = hat[at, :]
            levels[0, 0:1] = levels[0, 0:1] + jnp.sum(grad * x_hat, axis=0, keepdims=True)
            levels[0, 1:2] = levels[0, 1:2] + jnp.sum(grad, axis=0, keepdims=True)
            grad_hat = grad * row_of(gain)
            mean_grad = jnp.mean(grad_hat, axis=-1, keepdims=True)
            mean_proj = jnp.mean(grad_hat * x_hat, axis=-1, keepdims=True)
            send_q[at, :] = inv[at, 0:1] * (grad_hat - mean_grad - x_hat * mean_proj)
            return carry

        lax.fori_loop(0, quarter // step, token_block, 0)
        level_copy(0).start()
        for i in range(2):
            share_copy(i).start()

    level_peers = ({'tp': beside}, {'tp': partner}, {'dp': mate}, {'dp': z_mate}, {'dp': z_far})

    def level_copy(i):
        return remote(levels.at[i], arrived.at[i], level_sem.at[0, i], level_sem.at[1, i], **level_peers[i])

    def level_next(i):
        level_copy(i).wait_recv()
        merged = levels[i] + arrived[i]
        if i + 1 < len(level_peers):
            levels[i + 1] = merged
            level_copy(i + 1).start()
        else:
            sums[...] = merged
            sums[2:3] = jnp.broadcast_to(jnp.sum(merged[2:3], axis=-1, keepdims=True) / tokens_counted(), (1, width))

    def tokens_counted():
        return sum(counts[j, 0:1, 0:1] for j in range(n_dp))

    for k in range(PIECES):
        piece_copy(k).start()
    for copy in small_copies[:4]:
        copy.start()
    for j in range(1, n_tp):
        hidden_copy(j).start()
    block_copy(0).start()
    rows_copy(0).start()
    more_copy(0).start()
    for copy in small_copies[:4]:
        copy.wait()
    for k in range(PIECES):
        piece_copy(k).wait()
        first_piece(k)
    lax.fori_loop(1, n_tp, next_quarter, 0)
    counts[dp] = jnp.full(counts.shape[1:], jnp.sum(loss_mask[...].astype(jnp.float32)), jnp.float32)
    pl.semaphore_wait(barrier, n_dp - 1 + 2 * len(others))
    for k in range(PIECES):
        y_copy(k).start()
    for i in range(2):
        ids_copy(i).start()
    for j in range(n_dp - 1):
        count_copy(j).start()

    top[...] = jnp.full_like(top, jnp.finfo(jnp.float32).min)
    total[...] = jnp.zeros_like(total)
    held[...] = jnp.full_like(held, -jnp.inf)
    target[...] = jnp.zeros_like(target)

    assert blocks > 11 and PIECES == 4
    lax.fori_loop(0, blocks, block, 0)
    fold(held[...], tile_at(own_tiles - 1))

    best = jnp.max(top[...], axis=0, keepdims=True)
    stats[0, tp, 0:1] = best
    stats[0, tp, 1:2] = jnp.sum(total[...] * jnp.exp(top[...] - best), axis=0, keepdims=True)
    for copy in stat_copies():
        copy.start()

    relay_copy(last).wait_recv()
    convert(across, last)
    for i in range(2):
        ids_copy(i).wait()
    for j in range(n_dp - 1):
        count_arrival(j).wait_recv()
    for i in range(batch):
        for side, (rows_of, marks) in enumerate(((labels, loss_mask), (ids.at[0], ids.at[1]))):
            at = slice(side * own + i * seq, side * own + (i + 1) * seq)
            label[:, at] = rows_of[i:i + 1, :] - first_row
            weight[:, at] = marks[i:i + 1, :].astype(jnp.float32)
    scale[...] = weight[...] / tokens_counted()
    for k in range(PIECES):
        for copy in (y_copy(k), beside_copy(k), core_copy(k), relay_copy(k)):
            copy.wait_send()
    for j in range(n_dp - 1):
        count_copy(j).wait_send()
    first_logits()
    for other in others:
        stat_arrival(0, other).wait_recv()
    for other in (tp,) + others:
        stat_arrival(1, other).wait_recv()
    for side in range(Y):
        tops = [stats[side, j, 0:1] for j in range(n_tp)]
        best = functools.reduce(jnp.maximum, tops)
        mass = sum(stats[side, j, 1:2] * jnp.exp(tops[j] - best) for j in range(n_tp))
        lse[:, side * own:(side + 1) * own] = best + jnp.log(mass)

    first_unit()

    computes = (compute_0, compute_1, compute_2, compute_3, compute_4)
    beats = len(computes)
    start = beats - 2
    done = beats * units - 1
    ticks = start + chunks + END_LAG
    assert done + 39 < ticks

    def tick(i, carry):
        u = i // beats
        kind = i % beats

        @pl.when(i == start + 1)
        def _():
            settle(0)

        @pl.when(jnp.logical_not(inner))
        def _():
            end_step(jnp.maximum(i - start, 0))

        @pl.when(inner)
        def _():
            inner_step(jnp.maximum(i - start, 0))

        @pl.when(i == start)
        def _():
            first_dx()

        @pl.when((i > start) & (kind == start) & (u < units))
        def _():
            settle(u)

        for j, compute in enumerate(computes):
            pl.when((kind == j) & (u < units))(functools.partial(compute, u))

        events = ((1, dx_start), (5, dx_middle), (22, dx_finish), (24, lambda: level_next(0)), (26, lambda: level_next(1)),
                  (28, dh_own), (30, dh_partner), (32, lambda: level_next(2)), (36, lambda: level_next(3)), (39, dh_relay))
        for after, event in events:
            pl.when(i == done + after)(event)
        return carry

    lax.fori_loop(start, ticks, tick, 0)
    level_next(4)
    dh_finish()
    small_copies[4].start()

    @pl.when(jnp.logical_not(inner))
    def _():
        for c in range(chunks - 2, chunks):
            up_copy(c).wait_send()
        for c in range(chunks - RING, chunks):
            mate_copy(c, out_rows(y, c)).wait_send()

    for i in range(2):
        theirs = out.at[pl.ds((1 - y) * half + i * (half // 2), half // 2)]
        pltpu.make_async_copy(theirs, theirs, mate_recv.at[i]).wait()
    for copy in stat_copies():
        copy.wait_send()
    for i in range(2):
        swap_copy(i).wait_send()
    cross_copy().wait_send()
    for i in range(2):
        share_copy(i).wait_send()
    pass_copy().wait_send()
    dh_copy().wait()
    small_copies[4].wait()
    for i in range(len(level_peers)):
        level_copy(i).wait_send()


def head_step(table, hidden, gain, bias, labels, loss_mask, n_dp, n_tp):
    own, width = hidden.shape
    tokens = Y * own
    shard = table.shape[0]
    half = shard // Y
    size = half // (UNITS * PER_UNIT)
    unit = size * PER_UNIT
    quarter = own // n_tp
    assert unit <= quarter and 2 * TILE <= width and unit * UNITS == half and size % 8 == 0 and unit % 32 == 0 and quarter == TILE
    assert shard % FORWARD_ROWS == 0
    f32 = jnp.float32
    b16 = jnp.bfloat16
    i32 = jnp.int32
    lanes = 128
    dma = pltpu.SemaphoreType.DMA
    hbm = pl.BlockSpec(memory_space=pl.ANY)
    flops = 2 * width * (own * shard + half * (2 * tokens + 3 * own))
    return pl.pallas_call(
        functools.partial(head_kernel, n_dp, n_tp),
        out_shape=(
            jax.ShapeDtypeStruct((shard, width), f32),
            jax.ShapeDtypeStruct((half, width), f32),
            jax.ShapeDtypeStruct((own, width), b16),
            jax.ShapeDtypeStruct((8, width), f32)),
        in_specs=[hbm] * 6,
        out_specs=(hbm,) * 4,
        scratch_shapes=[
            pltpu.VMEM((width,), b16), pltpu.VMEM((width,), b16), pltpu.VMEM(labels.shape, i32), pltpu.VMEM(labels.shape, i32),
            pltpu.VMEM((8, width), f32),
            pltpu.VMEM((tokens, width), b16), pltpu.VMEM((width, tokens), b16),
            pltpu.VMEM((1, tokens), f32), pltpu.VMEM((1, tokens), f32), pltpu.VMEM((1, tokens), f32),
            pltpu.VMEM((1, tokens), i32), pltpu.VMEM((1, tokens), f32),
            pltpu.VMEM((quarter, width), f32), pltpu.VMEM((quarter, lanes), f32), pltpu.VMEM((quarter, width), f32),
            pltpu.VMEM((n_tp, quarter, width), f32), pltpu.VMEM((2, FORWARD_ROWS, width), b16),
            pltpu.VMEM((FORWARD_ROWS, TILE), f32),
            pltpu.VMEM((8, own), f32), pltpu.VMEM((8, own), f32),
            pltpu.VMEM((Y, n_tp, 2, own), f32), pltpu.VMEM((n_dp, 8, lanes), f32),
            pltpu.VMEM((2,) + labels.shape, i32),
            pltpu.VMEM((SLOTS, size, width), f32), pltpu.VMEM((SLOTS, size, width), f32), pltpu.VMEM((2, size, width), f32),
            pltpu.VMEM((unit, tokens), b16),
            pltpu.VMEM((2, unit, width), b16), pltpu.VMEM((2, unit, width), b16),
            pltpu.VMEM((unit, width), f32),
            pltpu.VMEM((n_tp, width, quarter), f32),
            pltpu.VMEM((2, width, quarter), f32), pltpu.VMEM((width, quarter), f32),
            pltpu.VMEM((5, 8, width), f32), pltpu.VMEM((5, 8, width), f32),
            dma((5,)), dma((PIECES,)), dma((n_tp,)), dma((2,)), dma((2, PIECES)), dma((2, PIECES)), dma((2, PIECES)), dma((2, PIECES)),
            dma((2 * n_tp - 1,)), dma((Y, n_tp)), dma((n_dp - 1,)), dma((n_dp,)),
            dma((2, 2)),
            dma((RING,)), dma((SLOTS,)), dma((RING,)), dma((SLOTS,)), dma((RING,)), dma((SLOTS,)), dma((RING,)), dma((2,)),
            pltpu.SemaphoreType.REGULAR((2,)),
            dma((2,)), dma((RING,)), dma((1,)), dma((2,)), dma((2,)),
            dma((2, 2)), dma((2,)), dma((3,)), dma((3,)), dma((2, 5)),
        ],
        compiler_params=pltpu.CompilerParams(
            collective_id=0, has_side_effects=True, vmem_limit_bytes=VMEM_BYTES),
        cost_estimate=pl.CostEstimate(flops=flops, bytes_accessed=12 * half * width, transcendentals=half * tokens),
    )(table, hidden, gain, bias, labels, loss_mask)


def place_kernel(table_in, dh_in, sums, table_out, dh_out, loss, gain_out, bias_out, buf, dh_buf, in_sem, out_sem, dh_sem):
    size = buf.shape[1]
    count = table_in.shape[0] // size
    lag = PLACE_SLOTS // 2

    def read(i):
        return pltpu.make_async_copy(table_in.at[pl.ds(i * size, size)], buf.at[i % PLACE_SLOTS], in_sem.at[i % PLACE_SLOTS])

    def write(i):
        return pltpu.make_async_copy(buf.at[i % PLACE_SLOTS], table_out.at[pl.ds(i * size, size)], out_sem.at[i % PLACE_SLOTS])

    dh_read = pltpu.make_async_copy(dh_in, dh_buf, dh_sem.at[0])
    dh_write = pltpu.make_async_copy(dh_buf, dh_out, dh_sem.at[1])
    for i in range(count + lag):
        if i < count:
            if i >= PLACE_SLOTS:
                write(i - PLACE_SLOTS).wait()
            read(i).start()
        if i == 0:
            dh_read.start()
            loss[...] = sums[2:3, 0:1]
            gain_out[...] = sums[0:1, :]
            bias_out[...] = sums[1:2, :]
        if i == lag:
            dh_read.wait()
            dh_write.start()
        if i >= lag:
            read(i - lag).wait()
            write(i - lag).start()
    for i in range(count - PLACE_SLOTS, count):
        write(i).wait()
    dh_write.wait()


def place(table, dh, sums):
    f32 = jnp.float32
    dma = pltpu.SemaphoreType.DMA
    vmem = pl.BlockSpec(memory_space=pltpu.VMEM)
    hbm = pl.BlockSpec(memory_space=pltpu.HBM)
    width = table.shape[1]
    assert table.shape[0] % PLACE_ROWS == 0
    return pl.pallas_call(
        place_kernel,
        out_shape=(
            jax.ShapeDtypeStruct(table.shape, f32), jax.ShapeDtypeStruct(dh.shape, dh.dtype),
            jax.ShapeDtypeStruct((1, 1), f32), jax.ShapeDtypeStruct((1, width), f32), jax.ShapeDtypeStruct((1, width), f32)),
        in_specs=[hbm, hbm, vmem],
        out_specs=(hbm, hbm, vmem, vmem, vmem),
        scratch_shapes=[
            pltpu.VMEM((PLACE_SLOTS, PLACE_ROWS, width), f32), pltpu.VMEM(dh.shape, dh.dtype),
            dma((PLACE_SLOTS,)), dma((PLACE_SLOTS,)), dma((2,))],
        compiler_params=pltpu.CompilerParams(vmem_limit_bytes=VMEM_BYTES),
        cost_estimate=pl.CostEstimate(flops=0, bytes_accessed=8 * table.size + 4 * dh.size, transcendentals=0),
    )(table, dh, sums)


def solution(mesh):
    n_dp = mesh.shape['dp']
    n_tp = mesh.shape['tp']

    def device_step(hidden, table, labels, loss_mask, ln_gain, ln_bias):
        batch, seq, width = hidden.shape
        grad_table, _, grad_hidden, sums = head_step(
            table, hidden.reshape(batch * seq, width), ln_gain, ln_bias, labels, loss_mask, n_dp, n_tp)
        grad_table, grad_hidden, loss, grad_gain, grad_bias = place(grad_table, grad_hidden, sums)
        return (loss.reshape(()), grad_hidden.reshape(batch, seq, width), grad_table,
                grad_gain.reshape(width), grad_bias.reshape(width))

    specs_in = (P('dp', None, None), P('tp', None), P('dp', None), P('dp', None), P(None), P(None))
    specs_out = (P(), P('dp', None, None), P('tp', None), P(None), P(None))
    return jax.shard_map(device_step, mesh=mesh, in_specs=specs_in, out_specs=specs_out, check_vma=False)
```
